256 devices in a mesh: block: 8 (over y, core), patch: 32 (over z, x).
Axes of the slice: x: 4, y: 4, z: 8, core: 2. Of those that a mesh axis runs over, the one named last changes fastest.
Arguments:
- samples_in: bfloat16 [16, 32, 2048, 128], P('block', None, 'patch'), may hold values from -6 to 6
- block_order: int32 [32, 16], P('patch'), may hold values from 0 to 15, each once within a row
- seam_link: int32 [32], P('patch'), may hold values from 0 to 1, as said below
- w_in: bfloat16 [16, 32, 256], P('block'), may hold values from -1.5 to 1.5
- w_mid: bfloat16 [16, 2, 256, 256], P('block'), may hold values from -0.5 to 0.5
- w_feat: bfloat16 [16, 256, 64], P('block'), may hold values from -0.375 to 0.375
- w_density: bfloat16 [16, 256], P('block'), may hold values from -0.375 to 0.375
- w_conv: bfloat16 [4, 3, 3, 64, 64], replicated, may hold values from -0.375 to 0.375
- w_color: bfloat16 [3, 64], replicated, may hold values from -0.75 to 0.75
Outputs:
- pixels: float32 [3, 128, 8192], P(None, 'block', 'patch')
The draws below stay inside these ranges and needn't reach their ends.
Inputs may be any that keep to these rules, and one draw needn't show every extreme that they name: Each row of block_order names every one of the 16 blocks once, in the order in which that patch's rays pass them, nearest first. seam_link[p] is 1 where patch p + 1 continues patch p to the right in one image; the entry before last is always 1; the last entry is not read.
All inputs are finite; a program needn't handle non-finite values.
Results may differ from the reference program's by a relative error of at most 0.015.
Values may be sent and summed in bfloat16 or wider, within the bound.
A program may use at most 64 MiB of HBM per device.

```python
import jax
import jax.numpy as jnp
from jax import lax

WIDTH = 256
ENC = 32
FEAT = 64
SAMP = 4
COLS_LO = 64
NB = 16
IMG_ROWS = 32
PATCHES = 32
TOTAL_COLS = 2048
N_PATCH = 32


def draw_seam_link(key, part):
    levels = jax.random.randint(jax.random.fold_in(key, 17), (PATCHES,), 0, 4)
    links = (levels < 3).astype(jnp.int32)
    return links.at[PATCHES - 2].set(1)


def steps_of(own_key, extent, cuts, low, top_value):
    level, own = 1.0, jax.random.fold_in(own_key, 6)
    for dim, shards_of in cuts:
        heights = jnp.exp(jax.random.uniform(jax.random.fold_in(own, dim), (shards_of,), jnp.float32, low / len(cuts), top_value / len(cuts)))
        level = level * jnp.repeat(heights, extent[dim] // shards_of).reshape([-1 if axis == dim else 1 for axis in range(len(extent))])
    return level


def noise(key, dims, spread, bound, split=(), kind=jnp.bfloat16):
    array = jax.random.normal(key, dims, jnp.float32) * spread
    if len(split) > 0:
        array = steps_of(key, dims, split, -0.22, 0.18) * array
    return jnp.clip(array, min=-bound, max=bound).astype(kind)


def setup_inputs(seed: int = 0) -> dict:
    splits = jax.random.split(jax.random.key(seed), 10)
    return {
        "samples_in": noise(splits[0], (NB, IMG_ROWS, TOTAL_COLS, SAMP * ENC), 1.0, 6.0, ((0, 8), (2, 32))),
        "block_order": jax.vmap(lambda own: jax.random.permutation(own, NB))(jax.random.split(splits[1], PATCHES)).reshape((PATCHES, NB)).astype(jnp.int32),
        "seam_link": draw_seam_link(jax.random.fold_in(splits[9], 71), 0),
        "w_in": noise(splits[3], (NB, ENC, WIDTH), (ENC // 2) ** -0.5, 1.5, ((0, 8),)),
        "w_mid": noise(splits[4], (NB, 2, WIDTH, WIDTH), (WIDTH // 2) ** -0.5, 0.5, ((0, 8),)),
        "w_feat": noise(splits[5], (NB, WIDTH, FEAT), WIDTH ** -0.5, 0.375, ((0, 8),)),
        "w_density": noise(splits[6], (NB, WIDTH), WIDTH ** -0.5, 0.375, ((0, 8),)),
        "w_conv": noise(splits[7], (4, 3, 3, FEAT, FEAT), (9 * FEAT // 2) ** -0.5, 0.375),
        "w_color": noise(splits[8], (3, FEAT), FEAT ** -0.5, 0.75),
    }


step_length = 0.03
highest = lax.Precision.HIGHEST


def block_field(samples, w_first, w_hidden, w_head, w_dens):
    count = samples.shape[0]
    flat = samples.reshape(count * SAMP, ENC)
    hidden = jax.nn.relu(jnp.dot(flat, w_first, preferred_element_type=jnp.float32)).astype(jnp.bfloat16)
    hidden = jax.nn.relu(jnp.dot(hidden, w_hidden[0], preferred_element_type=jnp.float32)).astype(jnp.bfloat16)
    hidden = jax.nn.relu(jnp.dot(hidden, w_hidden[1], preferred_element_type=jnp.float32)).astype(jnp.bfloat16)
    feature = lax.dot_general(w_head, hidden, (((0,), (1,)), ((), ())), preferred_element_type=jnp.float32)
    density = jax.nn.softplus(jnp.dot(hidden, w_dens, preferred_element_type=jnp.float32))
    optical = step_length * density.reshape(count, SAMP)
    earlier = jnp.cumsum(optical, axis=1) - optical
    weights = jnp.exp(-earlier) * (-jnp.expm1(-optical))
    colour = jnp.sum(feature.reshape(feature.shape[0], count, SAMP) * weights[None], axis=2)
    return jnp.sum(optical, axis=1), colour


def ranks_of(order_row):
    blocks = order_row.shape[0]
    places = jnp.arange(blocks, dtype=jnp.int32)
    hits = (order_row[None, :] == places[:, None]).astype(jnp.int32)
    return jnp.sum(places[None, :] * hits, axis=1)


def column_masks(seam_link, width):
    total = width * N_PATCH
    column = jnp.arange(total, dtype=jnp.int32)
    owner = column // width
    prior = jnp.concatenate([jnp.zeros((1,), jnp.int32), seam_link[:-1]])
    left_open = jnp.where(column % width == 0, prior[owner], 1)
    right_open = jnp.where(column % width == width - 1, seam_link[owner], 1)
    return left_open.astype(jnp.bfloat16), right_open.astype(jnp.bfloat16)


def convolve(image, kernel, seam_link):
    rows = image.shape[1]
    total = image.shape[2]
    left_open, right_open = column_masks(seam_link, total // N_PATCH)
    padded = jnp.pad(image, ((0, 0), (1, 1), (1, 1)))
    result = jnp.zeros((kernel.shape[2], rows, total), jnp.float32)
    for down in range(3):
        for across in range(3):
            window = padded[:, down:down + rows, across:across + total]
            if across == 0:
                window = window * left_open[None, None, :]
            if across == 2:
                window = window * right_open[None, None, :]
            result = result + lax.dot_general(kernel[down, across], window, (((1,), (0,)), ((), ())), preferred_element_type=jnp.float32)
    return result


def enlarge(image):
    return jnp.repeat(jnp.repeat(image, 2, axis=1), 2, axis=2)


def reference(samples_in, block_order, seam_link, w_in, w_mid, w_feat, w_density, w_conv, w_color):
    def render_patch(patch):
        columns = lax.dynamic_slice_in_dim(samples_in, patch * COLS_LO, COLS_LO, 2)
        rays = columns.reshape(NB, IMG_ROWS * COLS_LO, SAMP * ENC)
        depth_all, colour_all = lax.map(lambda parts: block_field(parts[0], parts[1], parts[2], parts[3], parts[4]), (rays, w_in, w_mid, w_feat, w_density))
        rank = ranks_of(block_order[patch])
        earlier = (rank[:, None] < rank[None, :]).astype(jnp.float32)
        prefix = jnp.dot(earlier.T, depth_all, precision=highest)
        mixed = jnp.einsum("br,bfr->fr", jnp.exp(-prefix), colour_all, precision=highest)
        return mixed.astype(jnp.bfloat16)

    images = lax.map(render_patch, jnp.arange(N_PATCH, dtype=jnp.int32))
    composite = images.reshape(N_PATCH, FEAT, IMG_ROWS, COLS_LO).transpose(1, 2, 0, 3).reshape(FEAT, IMG_ROWS, N_PATCH * COLS_LO)
    decoded = jax.nn.relu(convolve(enlarge(composite), w_conv[0], seam_link)).astype(jnp.bfloat16)
    decoded = jax.nn.relu(convolve(decoded, w_conv[1], seam_link)).astype(jnp.bfloat16)
    decoded = jax.nn.relu(convolve(enlarge(decoded), w_conv[2], seam_link)).astype(jnp.bfloat16)
    final = convolve(decoded, w_conv[3], seam_link)
    return lax.dot_general(w_color.astype(jnp.float32), final, (((1,), (0,)), ((), ())), precision=highest)
```

```python
import functools

import jax
import jax.numpy as jnp
from jax import lax
from jax.experimental import pallas as pl
from jax.experimental.pallas import tpu as pltpu
from jax.sharding import PartitionSpec as P

f32, bf16 = jnp.float32, jnp.bfloat16
MESH = pl.DeviceIdType.MESH

ENC = 32
SAMP = 4
STEP = 0.03
FEAT = 64
WIDTH = 256
COLS = 64
RAYS = 2048
CHUNK = 1024
PITCH = 128
WINDOW = 512


def iota(shape, dim):
    return lax.broadcasted_iota(jnp.int32, shape, dim)


def relu(x):
    return jnp.maximum(x, 0.0)


def dot(a, b):
    return jnp.dot(a, b, preferred_element_type=f32)


def dot_nt(a, b):
    return lax.dot_general(a, b, (((1,), (1,)), ((), ())), preferred_element_type=f32)


def field_chunk(x, w1, w2, w3, head):
    rays = x.shape[0]
    h = relu(dot_nt(w1, x)).astype(bf16)
    h = jnp.concatenate([h[WIDTH * s : WIDTH * (s + 1)] for s in range(SAMP)], axis=1)
    h = relu(dot(w2, h)).astype(bf16)
    h = relu(dot(w3, h)).astype(bf16)
    out = dot(head, h)
    raw = out[FEAT : FEAT + 1]
    optical = STEP * (jnp.maximum(raw, 0.0) + jnp.log(1.0 + jnp.exp(-jnp.abs(raw))))
    total = jnp.zeros((1, rays), f32)
    colour = jnp.zeros((FEAT, rays), f32)
    for s in range(SAMP):
        here = optical[:, s * rays : (s + 1) * rays]
        weight = jnp.exp(-total) * (1.0 - jnp.exp(-here))
        total = total + here
        colour = colour + weight * out[:FEAT, s * rays : (s + 1) * rays]
    return total, colour


def field_kernel(
    n_block, n_patch, order, seam, x, w_in, w_mid, w_feat, w_dens, window_out, left_out, right_out,
    spread, w1, w2, w3, head, colour, depth, depth_in, part, part_in, own, edges, edge_in,
    depth_send, depth_recv, part_send, part_recv, edge_send, edge_recv,
):
    me = lax.axis_index("block")
    place = lax.axis_index("patch")
    left = lax.rem(place + n_patch - 1, n_patch)
    right = lax.rem(place + 1, n_patch)
    barrier = pltpu.get_barrier_semaphore()
    for k in range(1, n_block):
        pl.semaphore_signal(barrier, inc=1, device_id=(lax.rem(me + k, n_block), place), device_id_type=MESH)
    for side in (left, right):
        pl.semaphore_signal(barrier, inc=1, device_id=(me, side), device_id_type=MESH)

    spread[...] = jnp.zeros_like(spread)
    for m in range(2):
        for s in range(SAMP):
            spread[ENC * s : ENC * (s + 1), WIDTH * s : WIDTH * (s + 1)] = w_in[m]
        w1[m] = spread[...].T
        w2[m] = w_mid[m, 0].T
        w3[m] = w_mid[m, 1].T
        head[m, :FEAT] = w_feat[m].T
        head[m, FEAT:] = jnp.broadcast_to(w_dens[pl.ds(m, 1), :], (16, WIDTH))
    part[:, :128] = jnp.zeros((FEAT, 128), bf16)
    part[:, 128 + RAYS :] = jnp.zeros((FEAT, 128), bf16)

    def chunk(c, carry):
        for m in range(2):
            rows = pl.ds(pl.multiple_of(c * CHUNK, CHUNK), CHUNK)
            total, tint = field_chunk(x[m, rows, :], w1[m], w2[m], w3[m], head[m])
            depth[pl.ds(m, 1), rows] = total
            colour[m, c] = tint
        return carry

    lax.fori_loop(0, RAYS // CHUNK, chunk, 0)

    pl.semaphore_wait(barrier, n_block - 1 + 2)
    depth_copies = []
    for k in range(1, n_block):
        copy = pltpu.make_async_remote_copy(
            src_ref=depth, dst_ref=depth_in.at[k - 1], send_sem=depth_send.at[k - 1],
            recv_sem=depth_recv.at[k - 1], device_id=(lax.rem(me + k, n_block), place), device_id_type=MESH,
        )
        copy.start()
        depth_copies.append(copy)

    def rank_of(first):
        member = first + iota((2, 128), 0)
        rank = jnp.zeros((2, 128), jnp.int32)
        for k in range(16):
            rank = jnp.where(member == order[0, k], k, rank)
        return rank

    mine = rank_of(2 * me)
    thresholds = [mine[m : m + 1] for m in range(2)]
    ranks = [mine] + [rank_of(2 * lax.rem(me + n_block - k, n_block)) for k in range(1, n_block)]
    gates = [[(r < t).astype(f32) for t in thresholds] for r in ranks]
    for copy in depth_copies:
        copy.wait_recv()
    for t in range(RAYS // 128):
        lanes = slice(128 * t, 128 * (t + 1))
        slots = [depth[:, lanes]] + [depth_in[k - 1, :, lanes] for k in range(1, n_block)]
        c, off = t * 128 // CHUNK, t * 128 % CHUNK
        mixed = None
        for m in range(2):
            prefix = sum(slot * gate[m] for slot, gate in zip(slots, gates))
            prefix = prefix[0:1] + prefix[1:2]
            term = jnp.exp(-prefix) * colour[m, c, :, off : off + 128]
            mixed = term if mixed is None else mixed + term
        part[:, 128 + 128 * t : 256 + 128 * t] = mixed.astype(bf16)

    part_copies = []
    for k in range(1, n_block):
        peer = lax.rem(me + k, n_block)
        copy = pltpu.make_async_remote_copy(
            src_ref=part.at[:, pl.ds(pl.multiple_of(256 * peer, 128), WINDOW)], dst_ref=part_in.at[k - 1],
            send_sem=part_send.at[k - 1], recv_sem=part_recv.at[k - 1],
            device_id=(peer, place), device_id_type=MESH,
        )
        copy.start()
        part_copies.append(copy)
    total = part[:, pl.ds(pl.multiple_of(256 * me, 128), WINDOW)].astype(f32)
    link = jnp.where(place < n_patch - 1, seam[0], 0).astype(f32)
    own[FEAT:] = jnp.full((FEAT, WINDOW), link, f32).astype(bf16)
    line = iota((32, WINDOW), 0)
    wanted = (line % 16) // 2 * COLS + line % 2 + jnp.where(line >= 16, COLS - 2, 0)
    pick = (iota((32, WINDOW), 1) == wanted).astype(f32).astype(bf16)
    for k in range(1, n_block):
        part_copies[k - 1].wait_recv()
        total = total + part_in[k - 1].astype(f32)
    window = total.astype(bf16)
    own[:FEAT] = window
    window_out[...] = window
    edges[...] = dot_nt(pick, own[...]).astype(bf16).reshape(2, 16, 128)
    edge_copies = []
    for side, target in ((0, left), (1, right)):
        copy = pltpu.make_async_remote_copy(
            src_ref=edges.at[side], dst_ref=edge_in.at[side], send_sem=edge_send.at[side],
            recv_sem=edge_recv.at[side], device_id=(me, target), device_id_type=MESH,
        )
        copy.start()
        edge_copies.append(copy)
    for copy in edge_copies:
        copy.wait_recv()
    right_out[...] = edge_in[0]
    left_out[...] = edge_in[1]
    for copy in depth_copies + part_copies + edge_copies:
        copy.wait_send()


def field(order, seam, x, w_in, w_mid, w_feat, w_dens, n_block, n_patch):
    vmem = pl.BlockSpec(memory_space=pltpu.VMEM)
    smem = pl.BlockSpec(memory_space=pltpu.SMEM)
    dma = pltpu.SemaphoreType.DMA
    return pl.pallas_call(
        functools.partial(field_kernel, n_block, n_patch),
        out_shape=[
            jax.ShapeDtypeStruct((FEAT, WINDOW), bf16),
            jax.ShapeDtypeStruct((16, 128), bf16),
            jax.ShapeDtypeStruct((16, 128), bf16),
        ],
        in_specs=[smem, smem] + [vmem] * 5,
        out_specs=[vmem] * 3,
        scratch_shapes=[
            pltpu.VMEM((128, 1024), bf16),
            pltpu.VMEM((2, 1024, 128), bf16),
            pltpu.VMEM((2, WIDTH, WIDTH), bf16),
            pltpu.VMEM((2, WIDTH, WIDTH), bf16),
            pltpu.VMEM((2, FEAT + 16, WIDTH), bf16),
            pltpu.VMEM((2, RAYS // CHUNK, FEAT, CHUNK), f32),
            pltpu.VMEM((2, RAYS), f32),
            pltpu.VMEM((n_block - 1, 2, RAYS), f32),
            pltpu.VMEM((FEAT, RAYS + 256), bf16),
            pltpu.VMEM((n_block - 1, FEAT, WINDOW), bf16),
            pltpu.VMEM((2 * FEAT, WINDOW), bf16),
            pltpu.VMEM((2, 16, 128), bf16),
            pltpu.VMEM((2, 16, 128), bf16),
            dma((n_block - 1,)), dma((n_block - 1,)), dma((n_block - 1,)), dma((n_block - 1,)), dma((2,)), dma((2,)),
        ],
        compiler_params=pltpu.CompilerParams(collective_id=0, has_side_effects=True),
        name="field",
    )(order, seam, x, w_in, w_mid, w_feat, w_dens)


def phase_source(phase, tap):
    return (phase + tap - 1) // 2


def put(ref, row, col, value):
    ref[row : row + value.shape[0], col : col + value.shape[1]] = value


def enlarge_weights(ref, w_conv, layer):
    taps = [[w_conv[layer, a, e].astype(f32) for e in range(3)] for a in range(3)]
    for pa in range(2):
        for pb in range(2):
            for dr in range(-1, 2):
                for dc in range(-1, 2):
                    hits = [taps[a][e] for a in range(3) for e in range(3)
                            if phase_source(pa, a) == dr and phase_source(pb, e) == dc]
                    value = sum(hits[1:], hits[0]) if hits else jnp.zeros((FEAT, FEAT), f32)
                    put(ref, (2 * pa + pb) * FEAT, ((dr + 1) * 3 + dc + 1) * FEAT, value.astype(bf16))


def dense_weights(ref, w_conv, layer):
    for qa in range(2):
        for qb in range(2):
            for s in range(-1, 3):
                for t in range(-1, 3):
                    a, e = s - qa + 1, t - qb + 1
                    inside = 0 <= a <= 2 and 0 <= e <= 2
                    value = w_conv[layer, a, e] if inside else jnp.zeros((FEAT, FEAT), bf16)
                    put(ref, (2 * qa + qb) * FEAT, ((s + 1) * 4 + t + 1) * FEAT, value)


def colour_weights(ref, w_conv, w_color, layer):
    ref[...] = jnp.zeros_like(ref)
    for a in range(3):
        for e in range(3):
            tint = dot(w_color[...], w_conv[layer, a, e])
            for i in range(4):
                for j in range(4):
                    group = (i - a + 2) * 6 + (j - e + 2)
                    cell = ((i // 2 * 2 + j // 2) * 2 + i % 2) * 2 + j % 2
                    put(ref, 8 * group, cell * FEAT, tint)


def moved(x, by):
    return pltpu.roll(x, (-by) % x.shape[1], 1)


def lines(x, first, count):
    return x[:, first * PITCH : (first + count) * PITCH]


def decoder_kernel(n_block, n_patch, seam, window, left_edge, right_edge, w_conv, w_color, out, k0, k1, k2, k3, res):
    me = lax.axis_index("block")
    place = lax.axis_index("patch")
    enlarge_weights(k0, w_conv, 0)
    dense_weights(k1, w_conv, 1)
    enlarge_weights(k2, w_conv, 2)
    colour_weights(k3, w_conv, w_color, 3)

    lane = iota((1, PITCH), 1)
    right_open = jnp.where(place < n_patch - 1, seam[0], 0).astype(f32)
    left_open = left_edge[0:1, FEAT : FEAT + 1].astype(f32)
    inner = jnp.where(lane < 2, left_open, jnp.where(lane < COLS + 2, 1.0, jnp.where(lane < COLS + 4, right_open, 0.0)))
    top = inner * jnp.where(me > 0, 1.0, 0.0)
    bottom = inner * jnp.where(me < n_block - 1, 1.0, 0.0)
    mask = jnp.concatenate([top] + [inner] * 4 + [bottom], axis=1)

    source = iota((128, 256), 0)
    move = (iota((128, 256), 1) == source // COLS * PITCH + source % COLS + 2).astype(f32).astype(bf16)
    body = jnp.concatenate([window[:, 128 * t : 128 * (t + 1)] for t in range(4)], axis=0)
    body = dot(body, move)
    image = jnp.concatenate([body[FEAT * t : FEAT * (t + 1)] for t in range(4)], axis=1)
    source = iota((32, 8 * PITCH), 0)
    target = (source % 16) // 2 * PITCH + source % 2 + jnp.where(source >= 16, COLS + 2, 0)
    halo_move = (iota((32, 8 * PITCH), 1) == target).astype(f32).astype(bf16)
    halo = jnp.concatenate([left_edge[...], right_edge[...]], axis=0).astype(f32).T
    image = image + dot(halo[:FEAT].astype(bf16), halo_move)
    image = image * jnp.concatenate([inner] * 8, axis=1)

    views = {-1: moved(image, -1).astype(bf16), 0: image.astype(bf16), 1: moved(image, 1).astype(bf16)}
    patches = jnp.concatenate([lines(views[dc], 1 + dr, 6) for dr in range(-1, 2) for dc in range(-1, 2)], axis=0)
    first = relu(dot(k0[...], patches)) * mask

    def column_views(maps):
        cell = lambda a, b: maps[(2 * a + b) * FEAT : (2 * a + b + 1) * FEAT]
        return [{-1: moved(cell(a, 1), -1).astype(bf16), 0: cell(a, 0).astype(bf16), 1: cell(a, 1).astype(bf16),
                 2: moved(cell(a, 0), 1).astype(bf16)} for a in range(2)]

    views = column_views(first)
    empty = jnp.zeros((FEAT, PITCH), bf16)
    parts = []
    for s in range(-1, 3):
        for t in range(-1, 3):
            view = views[s % 2][t]
            if s == -1:
                view = jnp.concatenate([empty, lines(view, 0, 5)], axis=1)
            if s == 2:
                view = jnp.concatenate([lines(view, 1, 5), empty], axis=1)
            parts.append(view)
    second = relu(dot(k1[...], jnp.concatenate(parts, axis=0))) * mask

    views = column_views(second)
    parts = []
    for qa in range(2):
        for qb in range(2):
            cells = []
            for s in range(qa - 1, qa + 2):
                for t in range(qb - 1, qb + 2):
                    start = s // 2 + 1 - qa
                    cells.append(lines(views[s % 2][t], start, 5))
            third = relu(dot(k2[...], jnp.concatenate(cells, axis=0))) * lines(mask, 1 - qa, 5)
            third = third.astype(bf16)
            blank = jnp.zeros((4 * FEAT, PITCH), bf16)
            parts.append(jnp.concatenate([third, blank] if qa else [blank, third], axis=1))
    spread = dot(k3[...].astype(bf16), jnp.concatenate(parts, axis=0))

    def cell(i, j):
        group = (i + 1) * 6 + j + 1
        return spread[8 * group : 8 * group + 8]

    def row(i, j):
        value = lines(cell(i, j), 1, 4)
        if i == 0:
            value = value + lines(cell(4, j), 0, 4)
        if i == 3:
            value = value + lines(cell(-1, j), 2, 4)
        return value

    stack = []
    for i in range(4):
        cols = [row(i, j) for j in range(-1, 5)]
        middle = cols[1:5]
        middle[0] = middle[0] + moved(cols[5], -1)
        middle[3] = middle[3] + moved(cols[0], 1)
        stack.append(middle)
    wide = jnp.concatenate(
        [jnp.concatenate([lines(stack[i][j], r, 1) for j in range(4)], axis=1) for r in range(4) for i in range(4)], axis=0
    )
    source = iota((4 * PITCH, 256), 0)
    at = source % PITCH - 2
    target = jnp.where((at >= 0) & (at < COLS), 4 * at + source // PITCH, -1)
    weave = (iota((4 * PITCH, 256), 1) == target).astype(f32).astype(bf16)
    high = wide.astype(bf16)
    low = (wide - high.astype(f32)).astype(bf16)
    woven = dot(high, weave) + dot(low, weave)
    for half in range(2):
        lanes = slice(128 * half, 128 * (half + 1))
        res[half] = woven[:, lanes]
        for k in range(3):
            out[k, :, lanes] = res[half, pl.ds(k, 16, stride=8), :]


def decoder(seam, window, left_edge, right_edge, w_conv, w_color, n_block, n_patch):
    vmem = pl.BlockSpec(memory_space=pltpu.VMEM)
    return pl.pallas_call(
        functools.partial(decoder_kernel, n_block, n_patch),
        out_shape=jax.ShapeDtypeStruct((3, 16, 256), f32),
        in_specs=[pl.BlockSpec(memory_space=pltpu.SMEM)] + [vmem] * 5,
        out_specs=vmem,
        scratch_shapes=[
            pltpu.VMEM((256, 576), bf16),
            pltpu.VMEM((256, 1024), bf16),
            pltpu.VMEM((256, 576), bf16),
            pltpu.VMEM((288, 1024), f32),
            pltpu.VMEM((2, 128, 128), f32),
        ],
        name="decoder",
    )(seam, window, left_edge, right_edge, w_conv, w_color)


def body(samples_in, block_order, seam_link, w_in, w_mid, w_feat, w_density, w_conv, w_color):
    n_block, n_patch = lax.axis_size("block"), lax.axis_size("patch")
    x = samples_in.reshape(2, RAYS, SAMP * ENC)
    window, left_edge, right_edge = field(block_order, seam_link, x, w_in, w_mid, w_feat, w_density, n_block, n_patch)
    return decoder(seam_link, window, left_edge, right_edge, w_conv, w_color, n_block, n_patch)


def solution(mesh):
    return jax.shard_map(
        body,
        mesh=mesh,
        in_specs=(
            P("block", None, "patch", None),
            P("patch", None),
            P("patch"),
            P("block", None, None),
            P("block", None, None, None),
            P("block", None, None),
            P("block", None),
            P(),
            P(),
        ),
        out_specs=P(None, "block", "patch"),
        check_vma=False,
    )
```

```python
import functools

import jax
import jax.numpy as jnp
from jax import lax
from jax.experimental import pallas as pl
from jax.experimental.pallas import tpu as pltpu
from jax.sharding import PartitionSpec as P

f32, bf16 = jnp.float32, jnp.bfloat16
MESH = pl.DeviceIdType.MESH

ENC = 32
SAMP = 4
STEP = 0.03
FEAT = 64
WIDTH = 256
COLS = 64
RAYS = 2048
CHUNK = 1024
PITCH = 128
WINDOW = 512


def iota(shape, dim):
    return lax.broadcasted_iota(jnp.int32, shape, dim)


def relu(x):
    return jnp.maximum(x, 0.0)


def dot(a, b):
    return jnp.dot(a, b, preferred_element_type=f32)


def dot_nt(a, b):
    return lax.dot_general(a, b, (((1,), (1,)), ((), ())), preferred_element_type=f32)


def field_chunk(x, w1, w2, w3, head):
    rays = x.shape[0]
    h = relu(dot_nt(w1, x)).astype(bf16)
    h = jnp.concatenate([h[WIDTH * s : WIDTH * (s + 1)] for s in range(SAMP)], axis=1)
    h = relu(dot(w2, h)).astype(bf16)
    h = relu(dot(w3, h)).astype(bf16)
    out = dot(head, h)
    raw = out[FEAT : FEAT + 1]
    optical = STEP * (jnp.maximum(raw, 0.0) + jnp.log(1.0 + jnp.exp(-jnp.abs(raw))))
    total = jnp.zeros((1, rays), f32)
    colour = jnp.zeros((FEAT, rays), f32)
    for s in range(SAMP):
        here = optical[:, s * rays : (s + 1) * rays]
        weight = jnp.exp(-total) * (1.0 - jnp.exp(-here))
        total = total + here
        colour = colour + weight * out[:FEAT, s * rays : (s + 1) * rays]
    return total, colour


def field_kernel(
    n_block, n_patch, order, seam, x, w_in, w_mid, w_feat, w_dens, window_out, left_out, right_out,
    spread, w1, w2, w3, head, colour, depth, depth_in, part, part_in, own, edges, edge_in,
    depth_send, depth_recv, part_send, part_recv, edge_send, edge_recv,
):
    me = lax.axis_index("block")
    place = lax.axis_index("patch")
    left = lax.rem(place + n_patch - 1, n_patch)
    right = lax.rem(place + 1, n_patch)
    edge_in[...] = jnp.zeros_like(edge_in)
    barrier = pltpu.get_barrier_semaphore()
    for k in range(1, n_block):
        pl.semaphore_signal(barrier, inc=1, device_id=(lax.rem(me + k, n_block), place), device_id_type=MESH)
    sides = ((left, place > 0), (right, place < n_patch - 1))
    for side, there in sides:

        @pl.when(there)
        def _():
            pl.semaphore_signal(barrier, inc=1, device_id=(me, side), device_id_type=MESH)


    spread[...] = jnp.zeros_like(spread)
    for m in range(2):
        for s in range(SAMP):
            spread[ENC * s : ENC * (s + 1), WIDTH * s : WIDTH * (s + 1)] = w_in[m]
        w1[m] = spread[...].T
        w2[m] = w_mid[m, 0].T
        w3[m] = w_mid[m, 1].T
        head[m, :FEAT] = w_feat[m]
        head[m, FEAT:] = jnp.broadcast_to(w_dens[pl.ds(m, 1), :], (16, WIDTH))
    part[:, :128] = jnp.zeros((FEAT, 128), bf16)
    part[:, 128 + RAYS :] = jnp.zeros((FEAT, 128), bf16)

    def chunk(c, carry):
        for m in range(2):
            rows = pl.ds(pl.multiple_of(c * CHUNK, CHUNK), CHUNK)
            total, tint = field_chunk(x[m, rows, :], w1[m], w2[m], w3[m], head[m])
            depth[pl.ds(m, 1), rows] = total
            colour[m, c] = tint
        return carry

    lax.fori_loop(0, RAYS // CHUNK, chunk, 0)

    count = (place > 0).astype(jnp.int32) + (place < n_patch - 1).astype(jnp.int32)
    pl.semaphore_wait(barrier, n_block - 1 + count)
    depth_copies = []
    for k in range(1, n_block):
        copy = pltpu.make_async_remote_copy(
            src_ref=depth, dst_ref=depth_in.at[k - 1], send_sem=depth_send.at[k - 1],
            recv_sem=depth_recv.at[k - 1], device_id=(lax.rem(me + k, n_block), place), device_id_type=MESH,
        )
        copy.start()
        depth_copies.append(copy)

    def rank_of(first):
        member = first + iota((2, 128), 0)
        rank = jnp.zeros((2, 128), jnp.int32)
        for k in range(16):
            rank = jnp.where(member == order[0, k], k, rank)
        return rank

    mine = rank_of(2 * me)
    thresholds = [mine[m : m + 1] for m in range(2)]
    ranks = [mine] + [rank_of(2 * lax.rem(me + n_block - k, n_block)) for k in range(1, n_block)]
    gates = [[(r < t).astype(f32) for t in thresholds] for r in ranks]
    for copy in depth_copies:
        copy.wait_recv()
    for t in range(RAYS // 128):
        lanes = slice(128 * t, 128 * (t + 1))
        slots = [depth[:, lanes]] + [depth_in[k - 1, :, lanes] for k in range(1, n_block)]
        c, off = t * 128 // CHUNK, t * 128 % CHUNK
        mixed = None
        for m in range(2):
            prefix = sum(slot * gate[m] for slot, gate in zip(slots, gates))
            prefix = prefix[0:1] + prefix[1:2]
            term = jnp.exp(-prefix) * colour[m, c, :, off : off + 128]
            mixed = term if mixed is None else mixed + term
        part[:, 128 + 128 * t : 256 + 128 * t] = mixed.astype(bf16)

    part_copies = []
    for k in range(1, n_block):
        peer = lax.rem(me + k, n_block)
        copy = pltpu.make_async_remote_copy(
            src_ref=part.at[:, pl.ds(pl.multiple_of(256 * peer, 128), WINDOW)], dst_ref=part_in.at[k - 1],
            send_sem=part_send.at[k - 1], recv_sem=part_recv.at[k - 1],
            device_id=(peer, place), device_id_type=MESH,
        )
        copy.start()
        part_copies.append(copy)
    total = part[:, pl.ds(pl.multiple_of(256 * me, 128), WINDOW)].astype(f32)
    link = jnp.where(place < n_patch - 1, seam[0], 0).astype(f32)
    own[FEAT:] = jnp.full((FEAT, WINDOW), link, f32).astype(bf16)
    line = iota((32, WINDOW), 0)
    wanted = (line % 16) // 2 * COLS + line % 2 + jnp.where(line >= 16, COLS - 2, 0)
    pick = (iota((32, WINDOW), 1) == wanted).astype(f32).astype(bf16)
    for k in range(1, n_block):
        part_copies[k - 1].wait_recv()
        total = total + part_in[k - 1].astype(f32)
    window = total.astype(bf16)
    own[:FEAT] = window
    window_out[...] = window
    edges[...] = dot_nt(pick, own[...]).astype(bf16).reshape(2, 16, 128)
    edge_copies = [
        pltpu.make_async_remote_copy(
            src_ref=edges.at[side], dst_ref=edge_in.at[side], send_sem=edge_send.at[side],
            recv_sem=edge_recv.at[side], device_id=(me, sides[side][0]), device_id_type=MESH,
        )
        for side in range(2)
    ]
    for side in range(2):
        pl.when(sides[side][1])(edge_copies[side].start)
    for side in range(2):
        pl.when(sides[1 - side][1])(edge_copies[side].wait_recv)
    right_out[...] = edge_in[0]
    left_out[...] = edge_in[1]
    for copy in depth_copies + part_copies:
        copy.wait_send()
    for side in range(2):
        pl.when(sides[side][1])(edge_copies[side].wait_send)


def field(order, seam, x, w_in, w_mid, w_feat, w_dens, n_block, n_patch):
    vmem = pl.BlockSpec(memory_space=pltpu.VMEM)
    smem = pl.BlockSpec(memory_space=pltpu.SMEM)
    dma = pltpu.SemaphoreType.DMA
    return pl.pallas_call(
        functools.partial(field_kernel, n_block, n_patch),
        out_shape=[
            jax.ShapeDtypeStruct((FEAT, WINDOW), bf16),
            jax.ShapeDtypeStruct((16, 128), bf16),
            jax.ShapeDtypeStruct((16, 128), bf16),
        ],
        in_specs=[smem, smem] + [vmem] * 5,
        out_specs=[vmem] * 3,
        scratch_shapes=[
            pltpu.VMEM((128, 1024), bf16),
            pltpu.VMEM((2, 1024, 128), bf16),
            pltpu.VMEM((2, WIDTH, WIDTH), bf16),
            pltpu.VMEM((2, WIDTH, WIDTH), bf16),
            pltpu.VMEM((2, FEAT + 16, WIDTH), bf16),
            pltpu.VMEM((2, RAYS // CHUNK, FEAT, CHUNK), f32),
            pltpu.VMEM((2, RAYS), f32),
            pltpu.VMEM((n_block - 1, 2, RAYS), f32),
            pltpu.VMEM((FEAT, RAYS + 256), bf16),
            pltpu.VMEM((n_block - 1, FEAT, WINDOW), bf16),
            pltpu.VMEM((2 * FEAT, WINDOW), bf16),
            pltpu.VMEM((2, 16, 128), bf16),
            pltpu.VMEM((2, 16, 128), bf16),
            dma((n_block - 1,)), dma((n_block - 1,)), dma((n_block - 1,)), dma((n_block - 1,)), dma((2,)), dma((2,)),
        ],
        compiler_params=pltpu.CompilerParams(collective_id=0, has_side_effects=True),
        name="field",
    )(order, seam, x, w_in, w_mid, w_feat, w_dens)


def phase_source(phase, tap):
    return (phase + tap - 1) // 2


def put(ref, row, col, value):
    ref[row : row + value.shape[0], col : col + value.shape[1]] = value


def enlarge_weights(ref, w_conv, layer):
    taps = [[w_conv[layer, a, e].astype(f32) for e in range(3)] for a in range(3)]
    for pa in range(2):
        for pb in range(2):
            for dr in range(-1, 2):
                for dc in range(-1, 2):
                    hits = [taps[a][e] for a in range(3) for e in range(3)
                            if phase_source(pa, a) == dr and phase_source(pb, e) == dc]
                    value = sum(hits[1:], hits[0]) if hits else jnp.zeros((FEAT, FEAT), f32)
                    put(ref, (2 * pa + pb) * FEAT, ((dr + 1) * 3 + dc + 1) * FEAT, value.astype(bf16))


def dense_weights(ref, w_conv, layer):
    for qa in range(2):
        for qb in range(2):
            for s in range(-1, 3):
                for t in range(-1, 3):
                    a, e = s - qa + 1, t - qb + 1
                    inside = 0 <= a <= 2 and 0 <= e <= 2
                    value = w_conv[layer, a, e] if inside else jnp.zeros((FEAT, FEAT), bf16)
                    put(ref, (2 * qa + qb) * FEAT, ((s + 1) * 4 + t + 1) * FEAT, value)


def colour_weights(ref, w_conv, w_color, layer):
    ref[...] = jnp.zeros_like(ref)
    for a in range(3):
        for e in range(3):
            tint = dot(w_color[...], w_conv[layer, a, e])
            for i in range(4):
                for j in range(4):
                    group = (i - a + 2) * 6 + (j - e + 2)
                    cell = ((i // 2 * 2 + j // 2) * 2 + i % 2) * 2 + j % 2
                    put(ref, 8 * group, cell * FEAT, tint)


def moved(x, by):
    return pltpu.roll(x, (-by) % x.shape[1], 1)


def lines(x, first, count):
    return x[:, first * PITCH : (first + count) * PITCH]


def decoder_kernel(n_block, n_patch, seam, window, left_edge, right_edge, w_conv, w_color, out, k0, k1, k2, k3, res):
    me = lax.axis_index("block")
    place = lax.axis_index("patch")
    enlarge_weights(k0, w_conv, 0)
    dense_weights(k1, w_conv, 1)
    enlarge_weights(k2, w_conv, 2)
    colour_weights(k3, w_conv, w_color, 3)

    lane = iota((1, PITCH), 1)
    right_open = jnp.where(place < n_patch - 1, seam[0], 0).astype(f32)
    left_open = left_edge[0:1, FEAT : FEAT + 1].astype(f32)
    inner = jnp.where(lane < 2, left_open, jnp.where(lane < COLS + 2, 1.0, jnp.where(lane < COLS + 4, right_open, 0.0)))
    top = inner * jnp.where(me > 0, 1.0, 0.0)
    bottom = inner * jnp.where(me < n_block - 1, 1.0, 0.0)
    mask = jnp.concatenate([top] + [inner] * 4 + [bottom], axis=1)

    source = iota((128, 256), 0)
    move = (iota((128, 256), 1) == source // COLS * PITCH + source % COLS + 2).astype(f32).astype(bf16)
    body = jnp.concatenate([window[:, 128 * t : 128 * (t + 1)] for t in range(4)], axis=0)
    body = dot(body, move)
    image = jnp.concatenate([body[FEAT * t : FEAT * (t + 1)] for t in range(4)], axis=1)
    source = iota((32, 8 * PITCH), 0)
    target = (source % 16) // 2 * PITCH + source % 2 + jnp.where(source >= 16, COLS + 2, 0)
    halo_move = (iota((32, 8 * PITCH), 1) == target).astype(f32).astype(bf16)
    halo = jnp.concatenate([left_edge[...], right_edge[...]], axis=0).astype(f32).T
    image = image + dot(halo[:FEAT].astype(bf16), halo_move)
    image = image * jnp.concatenate([inner] * 8, axis=1)

    views = {-1: moved(image, -1).astype(bf16), 0: image.astype(bf16), 1: moved(image, 1).astype(bf16)}
    patches = jnp.concatenate([lines(views[dc], 1 + dr, 6) for dr in range(-1, 2) for dc in range(-1, 2)], axis=0)
    first = relu(dot(k0[...], patches)) * mask

    def column_views(maps):
        cell = lambda a, b: maps[(2 * a + b) * FEAT : (2 * a + b + 1) * FEAT]
        return [{-1: moved(cell(a, 1), -1).astype(bf16), 0: cell(a, 0).astype(bf16), 1: cell(a, 1).astype(bf16),
                 2: moved(cell(a, 0), 1).astype(bf16)} for a in range(2)]

    views = column_views(first)
    empty = jnp.zeros((FEAT, PITCH), bf16)
    parts = []
    for s in range(-1, 3):
        for t in range(-1, 3):
            view = views[s % 2][t]
            if s == -1:
                view = jnp.concatenate([empty, lines(view, 0, 5)], axis=1)
            if s == 2:
                view = jnp.concatenate([lines(view, 1, 5), empty], axis=1)
            parts.append(view)
    second = relu(dot(k1[...], jnp.concatenate(parts, axis=0))) * mask

    views = column_views(second)
    parts = []
    for qa in range(2):
        for qb in range(2):
            cells = []
            for s in range(qa - 1, qa + 2):
                for t in range(qb - 1, qb + 2):
                    start = s // 2 + 1 - qa
                    cells.append(lines(views[s % 2][t], start, 5))
            third = relu(dot(k2[...], jnp.concatenate(cells, axis=0))) * lines(mask, 1 - qa, 5)
            third = third.astype(bf16)
            blank = jnp.zeros((4 * FEAT, PITCH), bf16)
            parts.append(jnp.concatenate([third, blank] if qa else [blank, third], axis=1))
    spread = dot(k3[...].astype(bf16), jnp.concatenate(parts, axis=0))

    def cell(i, j):
        group = (i + 1) * 6 + j + 1
        return spread[8 * group : 8 * group + 8]

    def row(i, j):
        value = lines(cell(i, j), 1, 4)
        if i == 0:
            value = value + lines(cell(4, j), 0, 4)
        if i == 3:
            value = value + lines(cell(-1, j), 2, 4)
        return value

    stack = []
    for i in range(4):
        cols = [row(i, j) for j in range(-1, 5)]
        middle = cols[1:5]
        middle[0] = middle[0] + moved(cols[5], -1)
        middle[3] = middle[3] + moved(cols[0], 1)
        stack.append(middle)
    wide = jnp.concatenate(
        [jnp.concatenate([lines(stack[i][j], r, 1) for j in range(4)], axis=1) for r in range(4) for i in range(4)], axis=0
    )
    source = iota((4 * PITCH, 256), 0)
    at = source % PITCH - 2
    target = jnp.where((at >= 0) & (at < COLS), 4 * at + source // PITCH, -1)
    weave = (iota((4 * PITCH, 256), 1) == target).astype(f32).astype(bf16)
    high = wide.astype(bf16)
    low = (wide - high.astype(f32)).astype(bf16)
    woven = dot(high, weave) + dot(low, weave)
    for half in range(2):
        lanes = slice(128 * half, 128 * (half + 1))
        res[half] = woven[:, lanes]
        for k in range(3):
            out[k, :, lanes] = res[half, pl.ds(k, 16, stride=8), :]


def decoder(seam, window, left_edge, right_edge, w_conv, w_color, n_block, n_patch):
    vmem = pl.BlockSpec(memory_space=pltpu.VMEM)
    return pl.pallas_call(
        functools.partial(decoder_kernel, n_block, n_patch),
        out_shape=jax.ShapeDtypeStruct((3, 16, 256), f32),
        in_specs=[pl.BlockSpec(memory_space=pltpu.SMEM)] + [vmem] * 5,
        out_specs=vmem,
        scratch_shapes=[
            pltpu.VMEM((256, 576), bf16),
            pltpu.VMEM((256, 1024), bf16),
            pltpu.VMEM((256, 576), bf16),
            pltpu.VMEM((288, 1024), f32),
            pltpu.VMEM((2, 128, 128), f32),
        ],
        name="decoder",
    )(seam, window, left_edge, right_edge, w_conv, w_color)


def body(samples_in, block_order, seam_link, w_in, w_mid, w_feat, w_density, w_conv, w_color):
    n_block, n_patch = lax.axis_size("block"), lax.axis_size("patch")
    x = samples_in.reshape(2, RAYS, SAMP * ENC)
    window, left_edge, right_edge = field(
        block_order, seam_link, x, w_in, w_mid, jnp.swapaxes(w_feat, 1, 2), w_density, n_block, n_patch
    )
    return decoder(seam_link, window, left_edge, right_edge, w_conv, w_color, n_block, n_patch)


def solution(mesh):
    return jax.shard_map(
        body,
        mesh=mesh,
        in_specs=(
            P("block", None, "patch", None),
            P("patch", None),
            P("patch"),
            P("block", None, None),
            P("block", None, None, None),
            P("block", None, None),
            P("block", None),
            P(),
            P(),
        ),
        out_specs=P(None, "block", "patch"),
        check_vma=False,
    )
```

```python
import functools

import jax
import jax.numpy as jnp
from jax import lax
from jax.experimental import pallas as pl
from jax.experimental.pallas import tpu as pltpu
from jax.sharding import PartitionSpec as P

f32, bf16 = jnp.float32, jnp.bfloat16
MESH = pl.DeviceIdType.MESH

ENC = 32
SAMP = 4
STEP = 0.03
FEAT = 64
WIDTH = 256
COLS = 64
RAYS = 2048
PITCH = 128


def iota(shape, dim):
    return lax.broadcasted_iota(jnp.int32, shape, dim)


def relu(x):
    return jnp.maximum(x, 0.0)


def dot(a, b):
    return jnp.dot(a, b, preferred_element_type=f32)


def dot_nt(a, b):
    return lax.dot_general(a, b, (((1,), (1,)), ((), ())), preferred_element_type=f32)


def field_chunk(x, w1, w2, w3, head):
    rays = x.shape[0]
    h = relu(dot_nt(w1, x)).astype(bf16)
    h = jnp.concatenate([h[WIDTH * s : WIDTH * (s + 1)] for s in range(SAMP)], axis=1)
    h = relu(dot(w2, h)).astype(bf16)
    h = relu(dot(w3, h)).astype(bf16)
    out = dot(head, h)
    raw = out[FEAT : FEAT + 1]
    optical = STEP * (jnp.maximum(raw, 0.0) + jnp.log(1.0 + jnp.exp(-jnp.abs(raw))))
    total = jnp.zeros((1, rays), f32)
    colour = jnp.zeros((FEAT, rays), f32)
    for s in range(SAMP):
        here = optical[:, s * rays : (s + 1) * rays]
        weight = jnp.exp(-total) * (1.0 - jnp.exp(-here))
        total = total + here
        colour = colour + weight * out[:FEAT, s * rays : (s + 1) * rays]
    return total, colour


def tile_of(device, unit):
    parity, late = unit // 2, unit % 2
    apart = (device + parity) % 2
    tile = device + (1 - 2 * late) * apart
    return (tile - parity + 8) // 2 % 4


def field_kernel(
    n_block, n_patch, order, seam, x, w_in, w_mid, w_feat, w_dens, window_out, halo_out, link_out,
    spread, w1, w2, w3, head, rays_out, rays_in, meta, meta_in, colour, depth, colour_in, depth_in, lines16,
    rays_send, rays_recv, meta_send, meta_recv, colour_send, colour_recv, depth_send, depth_recv,
):
    me = lax.axis_index("block")
    place = lax.axis_index("patch")
    sides = ((place - 1, place > 0), (place + 1, place < n_patch - 1))
    rays_in[...] = jnp.zeros_like(rays_in)
    meta_in[...] = jnp.zeros_like(meta_in)
    barrier = pltpu.get_barrier_semaphore()
    for k in range(1, n_block):
        pl.semaphore_signal(barrier, inc=1, device_id=((me + k) % n_block, place), device_id_type=MESH)
    for side, there in sides:

        @pl.when(there)
        def _():
            pl.semaphore_signal(barrier, inc=1, device_id=(me, side), device_id_type=MESH)

    line = iota((16, 256), 0)
    wanted = line % 8 // 2 * COLS + line % 2 + jnp.where(line >= 8, COLS - 2, 0)
    pick = (iota((16, 256), 1) == wanted).astype(f32).astype(bf16)
    for m in range(2):
        found = [dot(pick, x[m, 2 * g : 2 * g + 2].reshape(256, 128)) for g in range(8)]
        for side in range(2):
            rows = jnp.concatenate([f[8 * side : 8 * side + 8] for f in found], axis=0)
            rays_out[side, m] = rows.astype(bf16)
    slot = iota((16, 128), 0)
    member = 2 * ((me + n_block - slot // 2) % n_block) + slot % 2
    rank = jnp.zeros((16, 128), jnp.int32)
    for k in range(16):
        rank = jnp.where(member == order[0, k], k, rank)
    meta[:16] = rank
    meta[16:] = jnp.full((8, 128), jnp.where(place < n_patch - 1, seam[0], 0), jnp.int32)

    spread[...] = jnp.zeros_like(spread)
    for m in range(2):
        for s in range(SAMP):
            spread[ENC * s : ENC * (s + 1), WIDTH * s : WIDTH * (s + 1)] = w_in[m]
        w1[m] = spread[...].T
        w2[m] = w_mid[m, 0].T
        w3[m] = w_mid[m, 1].T
        head[m, :FEAT] = w_feat[m]
        head[m, FEAT:] = jnp.broadcast_to(w_dens[pl.ds(m, 1), :], (16, WIDTH))

    def side_copies(side):
        target = (me, sides[side][0])
        return [
            pltpu.make_async_remote_copy(
                src_ref=rays_out.at[side], dst_ref=rays_in.at[1 - side], send_sem=rays_send.at[side],
                recv_sem=rays_recv.at[1 - side], device_id=target, device_id_type=MESH,
            ),
            pltpu.make_async_remote_copy(
                src_ref=meta, dst_ref=meta_in.at[1 - side], send_sem=meta_send.at[side],
                recv_sem=meta_recv.at[1 - side], device_id=target, device_id_type=MESH,
            ),
        ]

    def send(unit, m, tiles):
        for k in range(1, n_block):
            peer = (me + k) % n_block
            tile = tile_of(peer, unit) if tiles > 1 else 0
            for src, dst, ssem, rsem in (
                (colour, colour_in, colour_send, colour_recv), (depth, depth_in, depth_send, depth_recv),
            ):
                pltpu.make_async_remote_copy(
                    src_ref=src.at[unit, m, tile], dst_ref=dst.at[unit, m, k - 1], send_sem=ssem.at[unit, m],
                    recv_sem=rsem.at[unit, m], device_id=(peer, place), device_id_type=MESH,
                ).start()

    def compute(unit, m, rays, tiles):
        total, tint = field_chunk(rays, w1[m], w2[m], w3[m], head[m])
        tint = tint.astype(bf16)
        for j in range(tiles):
            depth[unit, m, j] = total[:, 128 * j : 128 * (j + 1)]
            colour[unit, m, j] = tint[:, 128 * j : 128 * (j + 1)]

    def full(unit, first):
        for m in range(2):
            compute(unit, m, jnp.concatenate([x[m, 4 * j + unit] for j in range(4)], axis=0), 4)
            if first is not None and m == 0:

                @pl.when(first)
                def _():
                    count = (place > 0).astype(jnp.int32) + (place < n_patch - 1).astype(jnp.int32)
                    pl.semaphore_wait(barrier, n_block - 1 + count)
                    for side in range(2):
                        for copy in side_copies(side):
                            pl.when(sides[side][1])(copy.start)

            send(unit, m, 4)

    def loop(unit, carry):
        full(unit, unit == 0)
        return carry

    lax.fori_loop(0, 3, loop, 0)
    for side in range(2):
        for copy in side_copies(side):
            pl.when(sides[1 - side][1])(copy.wait_recv)
    for m in range(2):
        compute(4, m, jnp.concatenate([rays_in[0, m], rays_in[1, m]], axis=0), 1)
        send(4, m, 1)
    full(3, None)

    def combine(unit, tile, ranks):
        for m in range(2):
            for got, sem in ((colour_in, colour_recv), (depth_in, depth_recv)):
                pltpu.make_async_copy(got.at[unit, m], got.at[unit, m], sem.at[unit, m]).wait()
            lines16[m : m + 1] = depth[unit, m, tile]
            for k in range(1, n_block):
                lines16[2 * k + m : 2 * k + m + 1] = depth_in[unit, m, k - 1]
        depths = lines16[...]
        mixed = jnp.zeros((FEAT, 128), f32)
        for i in range(16):
            k, m = i // 2, i % 2
            prefix = jnp.sum(jnp.where(ranks < ranks[i : i + 1], depths, 0.0), axis=0, keepdims=True)
            tint = colour[unit, m, tile] if k == 0 else colour_in[unit, m, k - 1]
            mixed = mixed + jnp.exp(-prefix) * tint.astype(f32)
        return mixed

    def own_tile(unit):
        mixed = combine(unit, tile_of(me, unit), meta[:16])
        late = unit % 2
        apart = (me + unit // 2) % 2
        at = 1 + late + (2 - 4 * late) * apart
        outside = ((at == 0) & (me == 0)) | ((at == 3) & (me == n_block - 1))
        window_out[at] = (mixed * jnp.where(outside, 0.0, 1.0)).astype(bf16)

    for unit in range(3):
        own_tile(unit)
    ranks = jnp.where(iota((16, 128), 1) < 64, meta_in[0, :16], meta_in[1, :16])
    halo_out[...] = combine(4, 0, ranks).astype(bf16)
    link_out[...] = meta_in[0, 16:]
    own_tile(3)

    for side in range(2):
        for copy in side_copies(side):
            pl.when(sides[side][1])(copy.wait_send)
    for unit in range(5):
        for m in range(2):
            for got, sem in ((colour_in, colour_send), (depth_in, depth_send)):
                pltpu.make_async_copy(got.at[unit, m], got.at[unit, m], sem.at[unit, m]).wait()


def field(order, seam, x, w_in, w_mid, w_feat, w_dens, n_block, n_patch):
    vmem = pl.BlockSpec(memory_space=pltpu.VMEM)
    smem = pl.BlockSpec(memory_space=pltpu.SMEM)
    dma = pltpu.SemaphoreType.DMA
    return pl.pallas_call(
        functools.partial(field_kernel, n_block, n_patch),
        out_shape=[
            jax.ShapeDtypeStruct((4, FEAT, 128), bf16),
            jax.ShapeDtypeStruct((FEAT, 128), bf16),
            jax.ShapeDtypeStruct((8, 128), jnp.int32),
        ],
        in_specs=[smem, smem] + [vmem] * 5,
        out_specs=[vmem] * 3,
        scratch_shapes=[
            pltpu.VMEM((128, 1024), bf16),
            pltpu.VMEM((2, 1024, 128), bf16),
            pltpu.VMEM((2, WIDTH, WIDTH), bf16),
            pltpu.VMEM((2, WIDTH, WIDTH), bf16),
            pltpu.VMEM((2, FEAT + 16, WIDTH), bf16),
            pltpu.VMEM((2, 2, 64, 128), bf16),
            pltpu.VMEM((2, 2, 64, 128), bf16),
            pltpu.VMEM((24, 128), jnp.int32),
            pltpu.VMEM((2, 24, 128), jnp.int32),
            pltpu.VMEM((5, 2, 4, FEAT, 128), bf16),
            pltpu.VMEM((5, 2, 4, 1, 128), f32),
            pltpu.VMEM((5, 2, n_block - 1, FEAT, 128), bf16),
            pltpu.VMEM((5, 2, n_block - 1, 1, 128), f32),
            pltpu.VMEM((16, 128), f32),
            dma((2,)), dma((2,)), dma((2,)), dma((2,)), dma((5, 2)), dma((5, 2)), dma((5, 2)), dma((5, 2)),
        ],
        compiler_params=pltpu.CompilerParams(collective_id=0, has_side_effects=True),
        name="field",
    )(order, seam, x, w_in, w_mid, w_feat, w_dens)


def phase_source(phase, tap):
    return (phase + tap - 1) // 2


def put(ref, row, col, value):
    ref[row : row + value.shape[0], col : col + value.shape[1]] = value


def enlarge_weights(ref, w_conv, layer):
    taps = [[w_conv[layer, a, e].astype(f32) for e in range(3)] for a in range(3)]
    for pa in range(2):
        for pb in range(2):
            for dr in range(-1, 2):
                for dc in range(-1, 2):
                    hits = [taps[a][e] for a in range(3) for e in range(3)
                            if phase_source(pa, a) == dr and phase_source(pb, e) == dc]
                    value = sum(hits[1:], hits[0]) if hits else jnp.zeros((FEAT, FEAT), f32)
                    put(ref, (2 * pa + pb) * FEAT, ((dr + 1) * 3 + dc + 1) * FEAT, value.astype(bf16))


def dense_weights(ref, w_conv, layer):
    for qa in range(2):
        for qb in range(2):
            for s in range(-1, 3):
                for t in range(-1, 3):
                    a, e = s - qa + 1, t - qb + 1
                    inside = 0 <= a <= 2 and 0 <= e <= 2
                    value = w_conv[layer, a, e] if inside else jnp.zeros((FEAT, FEAT), bf16)
                    put(ref, (2 * qa + qb) * FEAT, ((s + 1) * 4 + t + 1) * FEAT, value)


def colour_weights(ref, w_conv, w_color, layer):
    ref[...] = jnp.zeros_like(ref)
    for a in range(3):
        for e in range(3):
            tint = dot(w_color[...], w_conv[layer, a, e])
            for i in range(4):
                for j in range(4):
                    group = (i - a + 2) * 6 + (j - e + 2)
                    cell = ((i // 2 * 2 + j // 2) * 2 + i % 2) * 2 + j % 2
                    put(ref, 8 * group, cell * FEAT, tint)


def moved(x, by):
    return pltpu.roll(x, (-by) % x.shape[1], 1)


def lines(x, first, count):
    return x[:, first * PITCH : (first + count) * PITCH]


def decoder_kernel(n_block, n_patch, seam, window, halo, link, w_conv, w_color, out, k0, k1, k2, k3, res):
    me = lax.axis_index("block")
    place = lax.axis_index("patch")
    enlarge_weights(k0, w_conv, 0)
    dense_weights(k1, w_conv, 1)
    enlarge_weights(k2, w_conv, 2)
    colour_weights(k3, w_conv, w_color, 3)

    lane = iota((1, PITCH), 1)
    right_open = jnp.where(place < n_patch - 1, seam[0], 0).astype(f32)
    left_open = link[0:1].astype(f32)
    inner = jnp.where(lane < 2, left_open, jnp.where(lane < COLS + 2, 1.0, jnp.where(lane < COLS + 4, right_open, 0.0)))
    top = inner * jnp.where(me > 0, 1.0, 0.0)
    bottom = inner * jnp.where(me < n_block - 1, 1.0, 0.0)
    mask = jnp.concatenate([top] + [inner] * 4 + [bottom], axis=1)

    source = iota((128, 256), 0)
    move = (iota((128, 256), 1) == source // COLS * PITCH + source % COLS + 2).astype(f32).astype(bf16)
    body = dot(window[...].reshape(4 * FEAT, 128), move)
    image = jnp.concatenate([body[FEAT * t : FEAT * (t + 1)] for t in range(4)], axis=1)
    source = iota((128, 8 * PITCH), 0)
    row = source % 64 // 2 - 4 * me + 2
    target = row * PITCH + source % 2 + jnp.where(source >= 64, COLS + 2, 0)
    target = jnp.where((row >= 0) & (row < 8), target, -1)
    halo_move = (iota((128, 8 * PITCH), 1) == target).astype(f32).astype(bf16)
    image = image + dot(halo[...], halo_move)
    image = image * jnp.concatenate([inner] * 8, axis=1)

    views = {-1: moved(image, -1).astype(bf16), 0: image.astype(bf16), 1: moved(image, 1).astype(bf16)}
    patches = jnp.concatenate([lines(views[dc], 1 + dr, 6) for dr in range(-1, 2) for dc in range(-1, 2)], axis=0)
    first = relu(dot(k0[...], patches)) * mask

    def column_views(maps):
        cell = lambda a, b: maps[(2 * a + b) * FEAT : (2 * a + b + 1) * FEAT]
        return [{-1: moved(cell(a, 1), -1).astype(bf16), 0: cell(a, 0).astype(bf16), 1: cell(a, 1).astype(bf16),
                 2: moved(cell(a, 0), 1).astype(bf16)} for a in range(2)]

    views = column_views(first)
    empty = jnp.zeros((FEAT, PITCH), bf16)
    parts = []
    for s in range(-1, 3):
        for t in range(-1, 3):
            view = views[s % 2][t]
            if s == -1:
                view = jnp.concatenate([empty, lines(view, 0, 5)], axis=1)
            if s == 2:
                view = jnp.concatenate([lines(view, 1, 5), empty], axis=1)
            parts.append(view)
    second = relu(dot(k1[...], jnp.concatenate(parts, axis=0))) * mask

    views = column_views(second)
    parts = []
    for qa in range(2):
        for qb in range(2):
            cells = []
            for s in range(qa - 1, qa + 2):
                for t in range(qb - 1, qb + 2):
                    start = s // 2 + 1 - qa
                    cells.append(lines(views[s % 2][t], start, 5))
            third = relu(dot(k2[...], jnp.concatenate(cells, axis=0))) * lines(mask, 1 - qa, 5)
            third = third.astype(bf16)
            blank = jnp.zeros((4 * FEAT, PITCH), bf16)
            parts.append(jnp.concatenate([third, blank] if qa else [blank, third], axis=1))
    spread = dot(k3[...].astype(bf16), jnp.concatenate(parts, axis=0))

    def cell(i, j):
        group = (i + 1) * 6 + j + 1
        return spread[8 * group : 8 * group + 8]

    def row(i, j):
        value = lines(cell(i, j), 1, 4)
        if i == 0:
            value = value + lines(cell(4, j), 0, 4)
        if i == 3:
            value = value + lines(cell(-1, j), 2, 4)
        return value

    stack = []
    for i in range(4):
        cols = [row(i, j) for j in range(-1, 5)]
        middle = cols[1:5]
        middle[0] = middle[0] + moved(cols[5], -1)
        middle[3] = middle[3] + moved(cols[0], 1)
        stack.append(middle)
    wide = jnp.concatenate(
        [jnp.concatenate([lines(stack[i][j], r, 1) for j in range(4)], axis=1) for r in range(4) for i in range(4)], axis=0
    )
    source = iota((4 * PITCH, 256), 0)
    at = source % PITCH - 2
    target = jnp.where((at >= 0) & (at < COLS), 4 * at + source // PITCH, -1)
    weave = (iota((4 * PITCH, 256), 1) == target).astype(f32).astype(bf16)
    high = wide.astype(bf16)
    low = (wide - high.astype(f32)).astype(bf16)
    woven = dot(high, weave) + dot(low, weave)
    for half in range(2):
        lanes = slice(128 * half, 128 * (half + 1))
        res[half] = woven[:, lanes]
        for k in range(3):
            out[k, :, lanes] = res[half, pl.ds(k, 16, stride=8), :]


def decoder(seam, window, halo, link, w_conv, w_color, n_block, n_patch):
    vmem = pl.BlockSpec(memory_space=pltpu.VMEM)
    return pl.pallas_call(
        functools.partial(decoder_kernel, n_block, n_patch),
        out_shape=jax.ShapeDtypeStruct((3, 16, 256), f32),
        in_specs=[pl.BlockSpec(memory_space=pltpu.SMEM)] + [vmem] * 5,
        out_specs=vmem,
        scratch_shapes=[
            pltpu.VMEM((256, 576), bf16),
            pltpu.VMEM((256, 1024), bf16),
            pltpu.VMEM((256, 576), bf16),
            pltpu.VMEM((288, 1024), f32),
            pltpu.VMEM((2, 128, 128), f32),
        ],
        name="decoder",
    )(seam, window, halo, link, w_conv, w_color)


def body(samples_in, block_order, seam_link, w_in, w_mid, w_feat, w_density, w_conv, w_color):
    n_block, n_patch = lax.axis_size("block"), lax.axis_size("patch")
    x = samples_in.reshape(2, RAYS // 128, 128, SAMP * ENC)
    window, halo, link = field(
        block_order, seam_link, x, w_in, w_mid, jnp.swapaxes(w_feat, 1, 2), w_density, n_block, n_patch
    )
    return decoder(seam_link, window, halo, link, w_conv, w_color, n_block, n_patch)


def solution(mesh):
    return jax.shard_map(
        body,
        mesh=mesh,
        in_specs=(
            P("block", None, "patch", None),
            P("patch", None),
            P("patch"),
            P("block", None, None),
            P("block", None, None, None),
            P("block", None, None),
            P("block", None),
            P(),
            P(),
        ),
        out_specs=P(None, "block", "patch"),
        check_vma=False,
    )
```

```python
import functools

import jax
import jax.numpy as jnp
from jax import lax
from jax.experimental import pallas as pl
from jax.experimental.pallas import tpu as pltpu
from jax.sharding import PartitionSpec as P

f32, bf16 = jnp.float32, jnp.bfloat16
MESH = pl.DeviceIdType.MESH

ENC = 32
SAMP = 4
STEP = 0.03
FEAT = 64
WIDTH = 256
COLS = 64
RAYS = 2048
PITCH = 128


def iota(shape, dim):
    return lax.broadcasted_iota(jnp.int32, shape, dim)


def relu(x):
    return jnp.maximum(x, 0.0)


def dot(a, b):
    return jnp.dot(a, b, preferred_element_type=f32)


def dot_nt(a, b):
    return lax.dot_general(a, b, (((1,), (1,)), ((), ())), preferred_element_type=f32)


def field_chunks(streams):
    count = len(streams)
    hs = [relu(dot_nt(w1, x)).astype(bf16) for x, w1, w2, w3, head in streams]
    hs = [jnp.concatenate([h[WIDTH * s : WIDTH * (s + 1)] for s in range(SAMP)], axis=1) for h in hs]
    hs = [relu(dot(streams[i][2], hs[i])).astype(bf16) for i in range(count)]
    hs = [relu(dot(streams[i][3], hs[i])).astype(bf16) for i in range(count)]
    outs = [dot(streams[i][4], hs[i]) for i in range(count)]
    results = []
    for out in outs:
        rays = out.shape[1] // SAMP
        raw = out[FEAT : FEAT + 1]
        optical = STEP * (jnp.maximum(raw, 0.0) + jnp.log(1.0 + jnp.exp(-jnp.abs(raw))))
        total = jnp.zeros((1, rays), f32)
        colour = jnp.zeros((FEAT, rays), f32)
        for s in range(SAMP):
            here = optical[:, s * rays : (s + 1) * rays]
            weight = jnp.exp(-total) * (1.0 - jnp.exp(-here))
            total = total + here
            colour = colour + weight * out[:FEAT, s * rays : (s + 1) * rays]
        results.append((total, colour))
    return results


def last_tile(device):
    return ((device + 1) // 2 + 3) % 4


def field_kernel(
    n_block, n_patch, order, seam, x, w_in, w_mid, w_feat, w_dens, window_out, halo_out, link_out,
    spread, w1, w2, w3, head, rays_out, rays_in, meta, meta_in, depth_rows, tiles, tiles_in, last_in, passed, passed_in,
    halo, halo_in, halo_depth, halo_depth_in, lines16, shares,
    rays_send, rays_recv, meta_send, meta_recv, tile_send, tile_recv, last_send, last_recv, pass_send, pass_recv,
    halo_send, halo_recv,
):
    me = lax.axis_index("block")
    place = lax.axis_index("patch")
    sides = ((place - 1, place > 0), (place + 1, place < n_patch - 1))
    rays_in[...] = jnp.zeros_like(rays_in)
    meta_in[...] = jnp.zeros_like(meta_in)
    barrier = pltpu.get_barrier_semaphore()
    for k in range(1, n_block):
        pl.semaphore_signal(barrier, inc=1, device_id=((me + k) % n_block, place), device_id_type=MESH)
    for side, there in sides:

        @pl.when(there)
        def _():
            pl.semaphore_signal(barrier, inc=1, device_id=(me, side), device_id_type=MESH)

    line = iota((16, 256), 0)
    wanted = line % 8 // 2 * COLS + line % 2 + jnp.where(line >= 8, COLS - 2, 0)
    pick = (iota((16, 256), 1) == wanted).astype(f32).astype(bf16)
    for m in range(2):
        found = [dot(pick, x[m, 2 * g : 2 * g + 2].reshape(256, 128)) for g in range(8)]
        for side in range(2):
            rows = jnp.concatenate([f[8 * side : 8 * side + 8] for f in found], axis=0)
            rays_out[side, m] = rows.astype(bf16)
    slot = iota((16, 128), 0)
    member = 2 * ((me + n_block - slot // 2) % n_block) + slot % 2
    rank = jnp.zeros((16, 128), jnp.int32)
    for k in range(16):
        rank = jnp.where(member == order[0, k], k, rank)
    meta[:16] = rank
    meta[16:] = jnp.full((8, 128), jnp.where(place < n_patch - 1, seam[0], 0), jnp.int32)

    spread[...] = jnp.zeros_like(spread)
    for m in range(2):
        for s in range(SAMP):
            spread[ENC * s : ENC * (s + 1), WIDTH * s : WIDTH * (s + 1)] = w_in[m]
        w1[m] = spread[...].T
        w2[m] = w_mid[m, 0].T
        w3[m] = w_mid[m, 1].T
        head[m, :FEAT] = w_feat[m]
        head[m, FEAT:] = jnp.broadcast_to(w_dens[pl.ds(m, 1), :], (16, WIDTH))
    depth_rows[...] = jnp.zeros_like(depth_rows)

    def side_copies(side):
        target = (me, sides[side][0])
        return [
            pltpu.make_async_remote_copy(
                src_ref=rays_out.at[side], dst_ref=rays_in.at[1 - side], send_sem=rays_send.at[side],
                recv_sem=rays_recv.at[1 - side], device_id=target, device_id_type=MESH,
            ),
            pltpu.make_async_remote_copy(
                src_ref=meta, dst_ref=meta_in.at[1 - side], send_sem=meta_send.at[side],
                recv_sem=meta_recv.at[1 - side], device_id=target, device_id_type=MESH,
            ),
        ]

    def weights(m):
        return w1[m], w2[m], w3[m], head[m]

    def depth_block(m, total):
        lanes = slice(0, total.shape[1])
        high = total.astype(bf16).astype(f32)
        depth_rows[m : m + 1, lanes] = high
        depth_rows[2 + m : 3 + m, lanes] = total - high

    def rays_of(unit, m):
        return jnp.concatenate([x[m, 4 * j + unit] for j in range(4)], axis=0)

    def keep(unit, m, tint):
        tint = tint.astype(bf16)
        for j in range(4):
            tiles[unit, j, FEAT * m : FEAT * (m + 1)] = tint[:, 128 * j : 128 * (j + 1)]

    def keep_depth(unit):
        rows = depth_rows[...].astype(bf16)
        for j in range(4):
            tiles[unit, j, 2 * FEAT :] = rows[:, 128 * j : 128 * (j + 1)]

    def loop(unit, carry):
        results = field_chunks([(rays_of(unit, m), *weights(m)) for m in range(2)])
        for m, (total, tint) in enumerate(results):
            keep(unit, m, tint)
            depth_block(m, total)
        keep_depth(unit)

        @pl.when(unit == 0)
        def _():
            count = (place > 0).astype(jnp.int32) + (place < n_patch - 1).astype(jnp.int32)
            pl.semaphore_wait(barrier, n_block - 1 + count)
            for side in range(2):
                for copy in side_copies(side):
                    pl.when(sides[side][1])(copy.start)

        for j in range(4):
            owner = 2 * j + unit // 2

            @pl.when(owner != me)
            def _():
                pltpu.make_async_remote_copy(
                    src_ref=tiles.at[unit, j], dst_ref=tiles_in.at[unit, (owner + n_block - me) % n_block - 1],
                    send_sem=tile_send.at[unit], recv_sem=tile_recv.at[unit],
                    device_id=(owner, place), device_id_type=MESH,
                ).start()

        return carry

    lax.fori_loop(0, 3, loop, 0)

    for side in range(2):
        for copy in side_copies(side):
            pl.when(sides[1 - side][1])(copy.wait_recv)
    results = field_chunks([(jnp.concatenate([rays_in[0, m], rays_in[1, m]], axis=0), *weights(m)) for m in range(2)])
    for m, (total, tint) in enumerate(results):
        depth_block(m, total)
    halo_depth[...] = depth_rows[:, :128].astype(bf16)
    ray = iota((144, 128), 0) - 8
    source = jnp.where((ray >= 0) & (ray < 128), ray // 2 % 2 * 64 + ray // 4 * 2 + ray % 2, -1)
    turn = (iota((144, 128), 1) == source).astype(f32).astype(bf16)
    both = jnp.concatenate([tint for total, tint in results], axis=0).astype(bf16)
    halo[...] = dot_nt(turn, both).astype(bf16)

    def halo_copies(k):
        peer = (me + k) % n_block
        return [
            pltpu.make_async_remote_copy(
                src_ref=halo.at[pl.ds(pl.multiple_of(16 * peer, 16), 32)], dst_ref=halo_in.at[k - 1],
                send_sem=halo_send.at[0, k - 1], recv_sem=halo_recv.at[0, k - 1],
                device_id=(peer, place), device_id_type=MESH,
            ),
            pltpu.make_async_remote_copy(
                src_ref=halo_depth, dst_ref=halo_depth_in.at[k - 1],
                send_sem=halo_send.at[1, k - 1], recv_sem=halo_recv.at[1, k - 1],
                device_id=(peer, place), device_id_type=MESH,
            ),
        ]

    for k in range(1, n_block):
        for copy in halo_copies(k):
            copy.start()

    def last_copy(k, m):
        peer = (me + k) % n_block
        rows = pl.ds(0, FEAT) if m == 0 else pl.ds(FEAT, FEAT + 8)
        return pltpu.make_async_remote_copy(
            src_ref=tiles.at[3, last_tile(peer), rows], dst_ref=last_in.at[k - 1, rows],
            send_sem=last_send.at[m, k - 1], recv_sem=last_recv.at[m, k - 1],
            device_id=(peer, place), device_id_type=MESH,
        )

    for m in range(2):
        ((total, tint),) = field_chunks([(rays_of(3, m), *weights(m))])
        keep(3, m, tint)
        depth_block(m, total)
        if m == 1:
            keep_depth(3)
        for k in range(1, n_block):
            last_copy(k, m).start()

    def order_weights(blocks, ranks):
        for k, block in enumerate(blocks):
            block = block.astype(f32)
            lines16[2 * k : 2 * k + 2] = block[0:2] + block[2:4]
        depths = lines16[...]
        prefixes = [
            jnp.sum(jnp.where(ranks < ranks[i : i + 1], depths, 0.0), axis=0, keepdims=True) for i in range(16)
        ]
        return [jnp.exp(-prefix) for prefix in prefixes]

    def combine(own, got):
        slots = [own] + [got.at[k - 1] for k in range(1, n_block)]
        factors = order_weights([slot[2 * FEAT :] for slot in slots], meta[:16])
        mixed = jnp.zeros((FEAT, 128), f32)
        for i in range(16):
            tint = slots[i // 2][i % 2 * FEAT : (i % 2 + 1) * FEAT]
            mixed = mixed + factors[i] * tint.astype(f32)
        return mixed

    def pass_copy(unit):
        target = me - 1 if unit % 2 == 0 else me + 1
        return pltpu.make_async_remote_copy(
            src_ref=passed.at[unit], dst_ref=passed_in.at[unit], send_sem=pass_send.at[unit],
            recv_sem=pass_recv.at[unit], device_id=(target, place), device_id_type=MESH,
        )

    def mine(unit):
        return me % 2 == unit // 2

    def has_target(unit):
        return mine(unit) & ((me > 0) if unit % 2 == 0 else (me < n_block - 1))

    def has_source(unit):
        return (me % 2 != unit // 2) & ((me < n_block - 1) if unit % 2 == 0 else (me > 0))

    for unit in range(3):

        @pl.when(mine(unit))
        def _():
            pltpu.make_async_copy(tiles_in.at[unit], tiles_in.at[unit], tile_recv.at[unit]).wait()
            passed[unit] = combine(tiles.at[unit, me // 2], tiles_in.at[unit]).astype(bf16)

        pl.when(has_target(unit))(pass_copy(unit).start)

        @pl.when(mine(unit))
        def _():
            window_out[1 + unit % 2] = passed[unit]

    for k in range(1, n_block):
        for copy in halo_copies(k):
            copy.wait_recv()
    ranks = jnp.where(iota((16, 128), 1) < 64, meta_in[0, :16], meta_in[1, :16])
    factors = order_weights([halo_depth[...]] + [halo_depth_in[k - 1] for k in range(1, n_block)], ranks)
    for i in range(16):
        shares[i : i + 1] = factors[i]
    line = iota((32, 128), 0)
    row = line // 4 + 4 * me - 2
    source = jnp.where((row >= 0) & (row < 32), line // 2 % 2 * 64 + row * 2 + line % 2, -1)
    turn = (iota((32, 128), 1) == source).astype(f32).astype(bf16)
    high = shares[...].astype(bf16)
    low = (shares[...] - high.astype(f32)).astype(bf16)
    share = dot_nt(turn, high) + dot_nt(turn, low)
    mixed = jnp.zeros((32, 128), f32)
    for k in range(n_block):
        tint = halo[pl.ds(pl.multiple_of(16 * me, 16), 32), :] if k == 0 else halo_in[k - 1]
        factor = jnp.where(iota((32, 128), 1) < 64, share[:, 2 * k : 2 * k + 1], share[:, 2 * k + 1 : 2 * k + 2])
        mixed = mixed + factor * tint.astype(f32)
    halo_out[...] = (mixed + pltpu.roll(mixed, 64, 1)).astype(bf16)
    link_out[...] = meta_in[0, 16:]

    for unit in range(3):

        @pl.when(has_source(unit))
        def _():
            pass_copy(unit).wait_recv()
            window_out[3 - unit % 2 * 3] = passed_in[unit]

    @pl.when(me == n_block - 1)
    def _():
        window_out[3] = jnp.zeros((FEAT, 128), bf16)

    for m in range(2):
        for k in range(1, n_block):
            last_copy(k, m).wait_recv()
    mixed = combine(tiles.at[3, last_tile(me)], last_in)
    window_out[me % 2 * 2] = (mixed * jnp.where(me > 0, 1.0, 0.0)).astype(bf16)

    for side in range(2):
        for copy in side_copies(side):
            pl.when(sides[side][1])(copy.wait_send)
    for k in range(1, n_block):
        for copy in halo_copies(k) + [last_copy(k, 0), last_copy(k, 1)]:
            copy.wait_send()
    for unit in range(3):
        pl.when(has_target(unit))(pass_copy(unit).wait_send)
        sent = pltpu.make_async_copy(tiles_in.at[unit, pl.ds(0, 3)], tiles_in.at[unit, pl.ds(0, 3)], tile_send.at[unit])
        more = pltpu.make_async_copy(tiles_in.at[unit, 3], tiles_in.at[unit, 3], tile_send.at[unit])
        sent.wait()
        pl.when(me % 2 != unit // 2)(more.wait)


def field(order, seam, x, w_in, w_mid, w_feat, w_dens, n_block, n_patch):
    vmem = pl.BlockSpec(memory_space=pltpu.VMEM)
    smem = pl.BlockSpec(memory_space=pltpu.SMEM)
    dma = pltpu.SemaphoreType.DMA
    peers = n_block - 1
    rows = 2 * FEAT + 8
    return pl.pallas_call(
        functools.partial(field_kernel, n_block, n_patch),
        out_shape=[
            jax.ShapeDtypeStruct((4, FEAT, 128), bf16),
            jax.ShapeDtypeStruct((32, 128), bf16),
            jax.ShapeDtypeStruct((8, 128), jnp.int32),
        ],
        in_specs=[smem, smem] + [vmem] * 5,
        out_specs=[vmem] * 3,
        scratch_shapes=[
            pltpu.VMEM((128, 1024), bf16),
            pltpu.VMEM((2, 1024, 128), bf16),
            pltpu.VMEM((2, WIDTH, WIDTH), bf16),
            pltpu.VMEM((2, WIDTH, WIDTH), bf16),
            pltpu.VMEM((2, FEAT + 16, WIDTH), bf16),
            pltpu.VMEM((2, 2, 64, 128), bf16),
            pltpu.VMEM((2, 2, 64, 128), bf16),
            pltpu.VMEM((24, 128), jnp.int32),
            pltpu.VMEM((2, 24, 128), jnp.int32),
            pltpu.VMEM((8, 512), f32),
            pltpu.VMEM((4, 4, rows, 128), bf16),
            pltpu.VMEM((3, peers, rows, 128), bf16),
            pltpu.VMEM((peers, rows, 128), bf16),
            pltpu.VMEM((3, FEAT, 128), bf16),
            pltpu.VMEM((3, FEAT, 128), bf16),
            pltpu.VMEM((144, 128), bf16),
            pltpu.VMEM((peers, 32, 128), bf16),
            pltpu.VMEM((8, 128), bf16),
            pltpu.VMEM((peers, 8, 128), bf16),
            pltpu.VMEM((16, 128), f32),
            pltpu.VMEM((16, 128), f32),
            dma((2,)), dma((2,)), dma((2,)), dma((2,)), dma((3,)), dma((3,)), dma((2, peers)), dma((2, peers)),
            dma((3,)), dma((3,)), dma((2, peers)), dma((2, peers)),
        ],
        compiler_params=pltpu.CompilerParams(collective_id=0, has_side_effects=True),
        name="field",
    )(order, seam, x, w_in, w_mid, w_feat, w_dens)


def phase_source(phase, tap):
    return (phase + tap - 1) // 2


def put(ref, row, col, value):
    ref[row : row + value.shape[0], col : col + value.shape[1]] = value


def enlarge_weights(ref, w_conv, layer):
    taps = [[w_conv[layer, a, e].astype(f32) for e in range(3)] for a in range(3)]
    for pa in range(2):
        for pb in range(2):
            for dr in range(-1, 2):
                for dc in range(-1, 2):
                    hits = [taps[a][e] for a in range(3) for e in range(3)
                            if phase_source(pa, a) == dr and phase_source(pb, e) == dc]
                    value = sum(hits[1:], hits[0]) if hits else jnp.zeros((FEAT, FEAT), f32)
                    put(ref, (2 * pa + pb) * FEAT, ((dr + 1) * 3 + dc + 1) * FEAT, value.astype(bf16))


def dense_weights(ref, w_conv, layer):
    for qa in range(2):
        for qb in range(2):
            for s in range(-1, 3):
                for t in range(-1, 3):
                    a, e = s - qa + 1, t - qb + 1
                    inside = 0 <= a <= 2 and 0 <= e <= 2
                    value = w_conv[layer, a, e] if inside else jnp.zeros((FEAT, FEAT), bf16)
                    put(ref, (2 * qa + qb) * FEAT, ((s + 1) * 4 + t + 1) * FEAT, value)


def colour_weights(ref, w_conv, w_color, layer):
    ref[...] = jnp.zeros_like(ref)
    for a in range(3):
        for e in range(3):
            tint = dot(w_color[...], w_conv[layer, a, e])
            for i in range(4):
                for j in range(4):
                    group = (i - a + 2) * 6 + (j - e + 2)
                    cell = ((i // 2 * 2 + j // 2) * 2 + i % 2) * 2 + j % 2
                    put(ref, 8 * group, cell * FEAT, tint)


def moved(x, by):
    return pltpu.roll(x, (-by) % x.shape[1], 1)


def lines(x, first, count):
    return x[:, first * PITCH : (first + count) * PITCH]


def decoder_kernel(n_block, n_patch, seam, window, halo, link, w_conv, w_color, out, k0, k1, k2, k3, res):
    me = lax.axis_index("block")
    place = lax.axis_index("patch")
    enlarge_weights(k0, w_conv, 0)
    dense_weights(k1, w_conv, 1)
    enlarge_weights(k2, w_conv, 2)
    colour_weights(k3, w_conv, w_color, 3)

    lane = iota((1, PITCH), 1)
    right_open = jnp.where(place < n_patch - 1, seam[0], 0).astype(f32)
    left_open = link[0:1].astype(f32)
    inner = jnp.where(lane < 2, left_open, jnp.where(lane < COLS + 2, 1.0, jnp.where(lane < COLS + 4, right_open, 0.0)))
    top = inner * jnp.where(me > 0, 1.0, 0.0)
    bottom = inner * jnp.where(me < n_block - 1, 1.0, 0.0)
    mask = jnp.concatenate([top] + [inner] * 4 + [bottom], axis=1)

    source = iota((128, 256), 0)
    move = (iota((128, 256), 1) == source // COLS * PITCH + source % COLS + 2).astype(f32).astype(bf16)
    body = dot(window[...].reshape(4 * FEAT, 128), move)
    image = jnp.concatenate([body[FEAT * t : FEAT * (t + 1)] for t in range(4)], axis=1)
    source = iota((32, 8 * PITCH), 0)
    target = source // 4 * PITCH + source % 2 + source // 2 % 2 * (COLS + 2)
    halo_move = (iota((32, 8 * PITCH), 1) == target).astype(f32).astype(bf16)
    image = image + dot(halo[...].astype(f32).T[:FEAT].astype(bf16), halo_move)
    image = image * jnp.concatenate([inner] * 8, axis=1)

    views = {-1: moved(image, -1).astype(bf16), 0: image.astype(bf16), 1: moved(image, 1).astype(bf16)}
    patches = jnp.concatenate([lines(views[dc], 1 + dr, 6) for dr in range(-1, 2) for dc in range(-1, 2)], axis=0)
    first = relu(dot(k0[...], patches)) * mask

    def column_views(maps):
        cell = lambda a, b: maps[(2 * a + b) * FEAT : (2 * a + b + 1) * FEAT]
        return [{-1: moved(cell(a, 1), -1).astype(bf16), 0: cell(a, 0).astype(bf16), 1: cell(a, 1).astype(bf16),
                 2: moved(cell(a, 0), 1).astype(bf16)} for a in range(2)]

    views = column_views(first)
    empty = jnp.zeros((FEAT, PITCH), bf16)
    parts = []
    for s in range(-1, 3):
        for t in range(-1, 3):
            view = views[s % 2][t]
            if s == -1:
                view = jnp.concatenate([empty, lines(view, 0, 5)], axis=1)
            if s == 2:
                view = jnp.concatenate([lines(view, 1, 5), empty], axis=1)
            parts.append(view)
    second = relu(dot(k1[...], jnp.concatenate(parts, axis=0))) * mask

    views = column_views(second)
    parts = []
    for qa in range(2):
        for qb in range(2):
            cells = []
            for s in range(qa - 1, qa + 2):
                for t in range(qb - 1, qb + 2):
                    start = s // 2 + 1 - qa
                    cells.append(lines(views[s % 2][t], start, 5))
            third = relu(dot(k2[...], jnp.concatenate(cells, axis=0))) * lines(mask, 1 - qa, 5)
            third = third.astype(bf16)
            blank = jnp.zeros((4 * FEAT, PITCH), bf16)
            parts.append(jnp.concatenate([third, blank] if qa else [blank, third], axis=1))
    spread = dot(k3[...].astype(bf16), jnp.concatenate(parts, axis=0))

    def cell(i, j):
        group = (i + 1) * 6 + j + 1
        return spread[8 * group : 8 * group + 8]

    def row(i, j):
        value = lines(cell(i, j), 1, 4)
        if i == 0:
            value = value + lines(cell(4, j), 0, 4)
        if i == 3:
            value = value + lines(cell(-1, j), 2, 4)
        return value

    stack = []
    for i in range(4):
        cols = [row(i, j) for j in range(-1, 5)]
        middle = cols[1:5]
        middle[0] = middle[0] + moved(cols[5], -1)
        middle[3] = middle[3] + moved(cols[0], 1)
        stack.append(middle)
    wide = jnp.concatenate(
        [jnp.concatenate([lines(stack[i][j], r, 1) for j in range(4)], axis=1) for r in range(4) for i in range(4)], axis=0
    )
    source = iota((4 * PITCH, 256), 0)
    at = source % PITCH - 2
    target = jnp.where((at >= 0) & (at < COLS), 4 * at + source // PITCH, -1)
    weave = (iota((4 * PITCH, 256), 1) == target).astype(f32).astype(bf16)
    high = wide.astype(bf16)
    low = (wide - high.astype(f32)).astype(bf16)
    woven = dot(high, weave) + dot(low, weave)
    for half in range(2):
        lanes = slice(128 * half, 128 * (half + 1))
        res[half] = woven[:, lanes]
        for k in range(3):
            out[k, :, lanes] = res[half, pl.ds(k, 16, stride=8), :]


def decoder(seam, window, halo, link, w_conv, w_color, n_block, n_patch):
    vmem = pl.BlockSpec(memory_space=pltpu.VMEM)
    return pl.pallas_call(
        functools.partial(decoder_kernel, n_block, n_patch),
        out_shape=jax.ShapeDtypeStruct((3, 16, 256), f32),
        in_specs=[pl.BlockSpec(memory_space=pltpu.SMEM)] + [vmem] * 5,
        out_specs=vmem,
        scratch_shapes=[
            pltpu.VMEM((256, 576), bf16),
            pltpu.VMEM((256, 1024), bf16),
            pltpu.VMEM((256, 576), bf16),
            pltpu.VMEM((288, 1024), f32),
            pltpu.VMEM((2, 128, 128), f32),
        ],
        name="decoder",
    )(seam, window, halo, link, w_conv, w_color)


def body(samples_in, block_order, seam_link, w_in, w_mid, w_feat, w_density, w_conv, w_color):
    n_block, n_patch = lax.axis_size("block"), lax.axis_size("patch")
    x = samples_in.reshape(2, RAYS // 128, 128, SAMP * ENC)
    window, halo, link = field(
        block_order, seam_link, x, w_in, w_mid, jnp.swapaxes(w_feat, 1, 2), w_density, n_block, n_patch
    )
    return decoder(seam_link, window, halo, link, w_conv, w_color, n_block, n_patch)


def solution(mesh):
    return jax.shard_map(
        body,
        mesh=mesh,
        in_specs=(
            P("block", None, "patch", None),
            P("patch", None),
            P("patch"),
            P("block", None, None),
            P("block", None, None, None),
            P("block", None, None),
            P("block", None),
            P(),
            P(),
        ),
        out_specs=P(None, "block", "patch"),
        check_vma=False,
    )
```

```python
import functools

import jax
import jax.numpy as jnp
from jax import lax
from jax.experimental import pallas as pl
from jax.experimental.pallas import tpu as pltpu
from jax.sharding import PartitionSpec as P

f32, bf16 = jnp.float32, jnp.bfloat16
MESH = pl.DeviceIdType.MESH

ENC = 32
SAMP = 4
STEP = 0.03
FEAT = 64
WIDTH = 256
COLS = 64
RAYS = 2048
PITCH = 128


def iota(shape, dim):
    return lax.broadcasted_iota(jnp.int32, shape, dim)


def relu(x):
    return jnp.maximum(x, 0.0)


def dot(a, b):
    return jnp.dot(a, b, preferred_element_type=f32)


def dot_nt(a, b):
    return lax.dot_general(a, b, (((1,), (1,)), ((), ())), preferred_element_type=f32)


def field_chunks(streams):
    count = len(streams)
    hs = [relu(dot_nt(w1, x)).astype(bf16) for x, w1, w2, w3, head in streams]
    hs = [jnp.concatenate([h[WIDTH * s : WIDTH * (s + 1)] for s in range(SAMP)], axis=1) for h in hs]
    hs = [relu(dot(streams[i][2], hs[i])).astype(bf16) for i in range(count)]
    hs = [relu(dot(streams[i][3], hs[i])).astype(bf16) for i in range(count)]
    outs = [dot(streams[i][4], hs[i]) for i in range(count)]
    results = []
    for out in outs:
        rays = out.shape[1] // SAMP
        raw = out[FEAT : FEAT + 1]
        optical = STEP * (jnp.maximum(raw, 0.0) + jnp.log(1.0 + jnp.exp(-jnp.abs(raw))))
        total = jnp.zeros((1, rays), f32)
        colour = jnp.zeros((FEAT, rays), f32)
        for s in range(SAMP):
            here = optical[:, s * rays : (s + 1) * rays]
            weight = jnp.exp(-total) * (1.0 - jnp.exp(-here))
            total = total + here
            colour = colour + weight * out[:FEAT, s * rays : (s + 1) * rays]
        results.append((total, colour))
    return results


def phase_source(phase, tap):
    return (phase + tap - 1) // 2


def put(ref, row, col, value):
    ref[row : row + value.shape[0], col : col + value.shape[1]] = value


def enlarge_weights(ref, w_conv, layer):
    taps = [[w_conv[layer, a, e].astype(f32) for e in range(3)] for a in range(3)]
    for pa in range(2):
        for pb in range(2):
            for dr in range(-1, 2):
                for dc in range(-1, 2):
                    hits = [taps[a][e] for a in range(3) for e in range(3)
                            if phase_source(pa, a) == dr and phase_source(pb, e) == dc]
                    value = sum(hits[1:], hits[0]) if hits else jnp.zeros((FEAT, FEAT), f32)
                    put(ref, (2 * pa + pb) * FEAT, ((dr + 1) * 3 + dc + 1) * FEAT, value.astype(bf16))


def dense_weights(ref, w_conv, layer):
    for qa in range(2):
        for qb in range(2):
            for s in range(-1, 3):
                for t in range(-1, 3):
                    a, e = s - qa + 1, t - qb + 1
                    inside = 0 <= a <= 2 and 0 <= e <= 2
                    value = w_conv[layer, a, e] if inside else jnp.zeros((FEAT, FEAT), bf16)
                    put(ref, (2 * qa + qb) * FEAT, ((s + 1) * 4 + t + 1) * FEAT, value)


def colour_weights(ref, w_conv, w_color, layer):
    ref[...] = jnp.zeros_like(ref)
    for a in range(3):
        for e in range(3):
            tint = dot(w_color[...], w_conv[layer, a, e])
            for i in range(4):
                for j in range(4):
                    group = (i - a + 2) * 6 + (j - e + 2)
                    cell = ((i // 2 * 2 + j // 2) * 2 + i % 2) * 2 + j % 2
                    put(ref, 8 * group, cell * FEAT, tint)


def moved(x, by):
    return pltpu.roll(x, (-by) % x.shape[1], 1)


def lines(x, first, count):
    return x[:, first * PITCH : (first + count) * PITCH]


def prepare(w_conv, w_color, k0, k1, k2, k3):
    enlarge_weights(k0, w_conv, 0)
    dense_weights(k1, w_conv, 1)
    enlarge_weights(k2, w_conv, 2)
    colour_weights(k3, w_conv, w_color, 3)


def decode(n_block, n_patch, seam, window, halo, link, out, k0, k1, k2, k3, res):
    me = lax.axis_index("block")
    place = lax.axis_index("patch")

    lane = iota((1, PITCH), 1)
    right_open = jnp.where(place < n_patch - 1, seam[0], 0).astype(f32)
    left_open = link[0:1].astype(f32)
    inner = jnp.where(lane < 2, left_open, jnp.where(lane < COLS + 2, 1.0, jnp.where(lane < COLS + 4, right_open, 0.0)))
    top = inner * jnp.where(me > 0, 1.0, 0.0)
    bottom = inner * jnp.where(me < n_block - 1, 1.0, 0.0)
    mask = jnp.concatenate([top] + [inner] * 4 + [bottom], axis=1)

    source = iota((128, 256), 0)
    move = (iota((128, 256), 1) == source // COLS * PITCH + source % COLS + 2).astype(f32).astype(bf16)
    body = dot(window[...].reshape(4 * FEAT, 128), move)
    image = jnp.concatenate([body[FEAT * t : FEAT * (t + 1)] for t in range(4)], axis=1)
    source = iota((32, 8 * PITCH), 0)
    target = source // 4 * PITCH + source % 2 + source // 2 % 2 * (COLS + 2)
    halo_move = (iota((32, 8 * PITCH), 1) == target).astype(f32).astype(bf16)
    image = image + dot(halo[...].astype(f32).T[:FEAT].astype(bf16), halo_move)
    image = image * jnp.concatenate([inner] * 8, axis=1)

    views = {-1: moved(image, -1).astype(bf16), 0: image.astype(bf16), 1: moved(image, 1).astype(bf16)}
    patches = jnp.concatenate([lines(views[dc], 1 + dr, 6) for dr in range(-1, 2) for dc in range(-1, 2)], axis=0)
    first = relu(dot(k0[...], patches)) * mask

    def column_views(maps):
        cell = lambda a, b: maps[(2 * a + b) * FEAT : (2 * a + b + 1) * FEAT]
        return [{-1: moved(cell(a, 1), -1).astype(bf16), 0: cell(a, 0).astype(bf16), 1: cell(a, 1).astype(bf16),
                 2: moved(cell(a, 0), 1).astype(bf16)} for a in range(2)]

    views = column_views(first)
    empty = jnp.zeros((FEAT, PITCH), bf16)
    parts = []
    for s in range(-1, 3):
        for t in range(-1, 3):
            view = views[s % 2][t]
            if s == -1:
                view = jnp.concatenate([empty, lines(view, 0, 5)], axis=1)
            if s == 2:
                view = jnp.concatenate([lines(view, 1, 5), empty], axis=1)
            parts.append(view)
    second = relu(dot(k1[...], jnp.concatenate(parts, axis=0))) * mask

    views = column_views(second)
    parts = []
    for qa in range(2):
        for qb in range(2):
            cells = []
            for s in range(qa - 1, qa + 2):
                for t in range(qb - 1, qb + 2):
                    start = s // 2 + 1 - qa
                    cells.append(lines(views[s % 2][t], start, 5))
            third = relu(dot(k2[...], jnp.concatenate(cells, axis=0))) * lines(mask, 1 - qa, 5)
            third = third.astype(bf16)
            blank = jnp.zeros((4 * FEAT, PITCH), bf16)
            parts.append(jnp.concatenate([third, blank] if qa else [blank, third], axis=1))
    spread = dot(k3[...].astype(bf16), jnp.concatenate(parts, axis=0))

    def cell(i, j):
        group = (i + 1) * 6 + j + 1
        return spread[8 * group : 8 * group + 8]

    def row(i, j):
        value = lines(cell(i, j), 1, 4)
        if i == 0:
            value = value + lines(cell(4, j), 0, 4)
        if i == 3:
            value = value + lines(cell(-1, j), 2, 4)
        return value

    stack = []
    for i in range(4):
        cols = [row(i, j) for j in range(-1, 5)]
        middle = cols[1:5]
        middle[0] = middle[0] + moved(cols[5], -1)
        middle[3] = middle[3] + moved(cols[0], 1)
        stack.append(middle)
    wide = jnp.concatenate(
        [jnp.concatenate([lines(stack[i][j], r, 1) for j in range(4)], axis=1) for r in range(4) for i in range(4)], axis=0
    )
    source = iota((4 * PITCH, 256), 0)
    at = source % PITCH - 2
    target = jnp.where((at >= 0) & (at < COLS), 4 * at + source // PITCH, -1)
    weave = (iota((4 * PITCH, 256), 1) == target).astype(f32).astype(bf16)
    high = wide.astype(bf16)
    low = (wide - high.astype(f32)).astype(bf16)
    woven = dot(high, weave) + dot(low, weave)
    for half in range(2):
        lanes = slice(128 * half, 128 * (half + 1))
        res[half] = woven[:, lanes]
        for k in range(3):
            out[k, :, lanes] = res[half, pl.ds(k, 16, stride=8), :]


def last_tile(device):
    return ((device + 1) // 2 + 3) % 4


def field_kernel(
    n_block, n_patch, order, seam, x, w_in, w_mid, w_feat, w_dens, w_conv, w_color, out,
    window_out, halo_out, k0, k1, k2, k3, res,
    spread, w1, w2, w3, head, rays_out, rays_in, meta, meta_in, depth_rows, tiles, tiles_in, last_in, passed, passed_in,
    halo, halo_in, halo_depth, halo_depth_in, lines16, shares,
    rays_send, rays_recv, meta_send, meta_recv, tile_send, tile_recv, last_send, last_recv, pass_send, pass_recv,
    halo_send, halo_recv,
):
    me = lax.axis_index("block")
    place = lax.axis_index("patch")
    sides = ((place - 1, place > 0), (place + 1, place < n_patch - 1))
    rays_in[...] = jnp.zeros_like(rays_in)
    meta_in[...] = jnp.zeros_like(meta_in)
    barrier = pltpu.get_barrier_semaphore()
    for k in range(1, n_block):
        pl.semaphore_signal(barrier, inc=1, device_id=((me + k) % n_block, place), device_id_type=MESH)
    for side, there in sides:

        @pl.when(there)
        def _():
            pl.semaphore_signal(barrier, inc=1, device_id=(me, side), device_id_type=MESH)

    line = iota((16, 256), 0)
    wanted = line % 8 // 2 * COLS + line % 2 + jnp.where(line >= 8, COLS - 2, 0)
    pick = (iota((16, 256), 1) == wanted).astype(f32).astype(bf16)
    for m in range(2):
        found = [dot(pick, x[m, 2 * g : 2 * g + 2].reshape(256, 128)) for g in range(8)]
        for side in range(2):
            rows = jnp.concatenate([f[8 * side : 8 * side + 8] for f in found], axis=0)
            rays_out[side, m] = rows.astype(bf16)
    slot = iota((16, 128), 0)
    member = 2 * ((me + n_block - slot // 2) % n_block) + slot % 2
    rank = jnp.zeros((16, 128), jnp.int32)
    for k in range(16):
        rank = jnp.where(member == order[0, k], k, rank)
    meta[:16] = rank
    meta[16:] = jnp.full((8, 128), jnp.where(place < n_patch - 1, seam[0], 0), jnp.int32)

    spread[...] = jnp.zeros_like(spread)
    for m in range(2):
        for s in range(SAMP):
            spread[ENC * s : ENC * (s + 1), WIDTH * s : WIDTH * (s + 1)] = w_in[m]
        w1[m] = spread[...].T
        w2[m] = w_mid[m, 0].T
        w3[m] = w_mid[m, 1].T
        head[m, :FEAT] = w_feat[m]
        head[m, FEAT:] = jnp.broadcast_to(w_dens[pl.ds(m, 1), :], (16, WIDTH))
    depth_rows[...] = jnp.zeros_like(depth_rows)

    def side_copies(side):
        target = (me, sides[side][0])
        return [
            pltpu.make_async_remote_copy(
                src_ref=rays_out.at[side], dst_ref=rays_in.at[1 - side], send_sem=rays_send.at[side],
                recv_sem=rays_recv.at[1 - side], device_id=target, device_id_type=MESH,
            ),
            pltpu.make_async_remote_copy(
                src_ref=meta, dst_ref=meta_in.at[1 - side], send_sem=meta_send.at[side],
                recv_sem=meta_recv.at[1 - side], device_id=target, device_id_type=MESH,
            ),
        ]

    def weights(m):
        return w1[m], w2[m], w3[m], head[m]

    def depth_block(m, total):
        lanes = slice(0, total.shape[1])
        high = total.astype(bf16).astype(f32)
        depth_rows[m : m + 1, lanes] = high
        depth_rows[2 + m : 3 + m, lanes] = total - high

    def rays_of(unit, m):
        return jnp.concatenate([x[m, 4 * j + unit] for j in range(4)], axis=0)

    def keep(unit, m, tint):
        tint = tint.astype(bf16)
        for j in range(4):
            tiles[unit, j, FEAT * m : FEAT * (m + 1)] = tint[:, 128 * j : 128 * (j + 1)]

    def keep_depth(unit):
        rows = depth_rows[...].astype(bf16)
        for j in range(4):
            tiles[unit, j, 2 * FEAT :] = rows[:, 128 * j : 128 * (j + 1)]

    def loop(unit, carry):
        results = field_chunks([(rays_of(unit, m), *weights(m)) for m in range(2)])
        for m, (total, tint) in enumerate(results):
            keep(unit, m, tint)
            depth_block(m, total)
        keep_depth(unit)

        @pl.when(unit == 0)
        def _():
            count = (place > 0).astype(jnp.int32) + (place < n_patch - 1).astype(jnp.int32)
            pl.semaphore_wait(barrier, n_block - 1 + count)
            for side in range(2):
                for copy in side_copies(side):
                    pl.when(sides[side][1])(copy.start)

        for j in range(4):
            owner = 2 * j + unit // 2

            @pl.when(owner != me)
            def _():
                pltpu.make_async_remote_copy(
                    src_ref=tiles.at[unit, j], dst_ref=tiles_in.at[unit, (owner + n_block - me) % n_block - 1],
                    send_sem=tile_send.at[unit], recv_sem=tile_recv.at[unit],
                    device_id=(owner, place), device_id_type=MESH,
                ).start()

        return carry

    lax.fori_loop(0, 3, loop, 0)

    for side in range(2):
        for copy in side_copies(side):
            pl.when(sides[1 - side][1])(copy.wait_recv)
    results = field_chunks([(jnp.concatenate([rays_in[0, m], rays_in[1, m]], axis=0), *weights(m)) for m in range(2)])
    for m, (total, tint) in enumerate(results):
        depth_block(m, total)
    halo_depth[...] = depth_rows[:, :128].astype(bf16)
    ray = iota((144, 128), 0) - 8
    source = jnp.where((ray >= 0) & (ray < 128), ray // 2 % 2 * 64 + ray // 4 * 2 + ray % 2, -1)
    turn = (iota((144, 128), 1) == source).astype(f32).astype(bf16)
    both = jnp.concatenate([tint for total, tint in results], axis=0).astype(bf16)
    halo[...] = dot_nt(turn, both).astype(bf16)

    def halo_copies(k):
        peer = (me + k) % n_block
        return [
            pltpu.make_async_remote_copy(
                src_ref=halo.at[pl.ds(pl.multiple_of(16 * peer, 16), 32)], dst_ref=halo_in.at[k - 1],
                send_sem=halo_send.at[0, k - 1], recv_sem=halo_recv.at[0, k - 1],
                device_id=(peer, place), device_id_type=MESH,
            ),
            pltpu.make_async_remote_copy(
                src_ref=halo_depth, dst_ref=halo_depth_in.at[k - 1],
                send_sem=halo_send.at[1, k - 1], recv_sem=halo_recv.at[1, k - 1],
                device_id=(peer, place), device_id_type=MESH,
            ),
        ]

    for k in range(1, n_block):
        for copy in halo_copies(k):
            copy.start()

    def last_copy(k, m):
        peer = (me + k) % n_block
        rows = pl.ds(0, FEAT) if m == 0 else pl.ds(FEAT, FEAT + 8)
        return pltpu.make_async_remote_copy(
            src_ref=tiles.at[3, last_tile(peer), rows], dst_ref=last_in.at[k - 1, rows],
            send_sem=last_send.at[m, k - 1], recv_sem=last_recv.at[m, k - 1],
            device_id=(peer, place), device_id_type=MESH,
        )

    for m in range(2):
        ((total, tint),) = field_chunks([(rays_of(3, m), *weights(m))])
        keep(3, m, tint)
        depth_block(m, total)
        if m == 1:
            keep_depth(3)
        for k in range(1, n_block):
            last_copy(k, m).start()

    def order_weights(blocks, ranks):
        for k, block in enumerate(blocks):
            block = block.astype(f32)
            lines16[2 * k : 2 * k + 2] = block[0:2] + block[2:4]
        depths = lines16[...]
        prefixes = [
            jnp.sum(jnp.where(ranks < ranks[i : i + 1], depths, 0.0), axis=0, keepdims=True) for i in range(16)
        ]
        return [jnp.exp(-prefix) for prefix in prefixes]

    def combine(own, got):
        slots = [own] + [got.at[k - 1] for k in range(1, n_block)]
        factors = order_weights([slot[2 * FEAT :] for slot in slots], meta[:16])
        mixed = jnp.zeros((FEAT, 128), f32)
        for i in range(16):
            tint = slots[i // 2][i % 2 * FEAT : (i % 2 + 1) * FEAT]
            mixed = mixed + factors[i] * tint.astype(f32)
        return mixed

    def pass_copy(unit):
        target = me - 1 if unit % 2 == 0 else me + 1
        return pltpu.make_async_remote_copy(
            src_ref=passed.at[unit], dst_ref=passed_in.at[unit], send_sem=pass_send.at[unit],
            recv_sem=pass_recv.at[unit], device_id=(target, place), device_id_type=MESH,
        )

    def mine(unit):
        return me % 2 == unit // 2

    def has_target(unit):
        return mine(unit) & ((me > 0) if unit % 2 == 0 else (me < n_block - 1))

    def has_source(unit):
        return (me % 2 != unit // 2) & ((me < n_block - 1) if unit % 2 == 0 else (me > 0))

    for unit in range(3):

        @pl.when(mine(unit))
        def _():
            pltpu.make_async_copy(tiles_in.at[unit], tiles_in.at[unit], tile_recv.at[unit]).wait()
            passed[unit] = combine(tiles.at[unit, me // 2], tiles_in.at[unit]).astype(bf16)

        pl.when(has_target(unit))(pass_copy(unit).start)

        @pl.when(mine(unit))
        def _():
            window_out[1 + unit % 2] = passed[unit]

    prepare(w_conv, w_color, k0, k1, k2, k3)

    for k in range(1, n_block):
        for copy in halo_copies(k):
            copy.wait_recv()
    ranks = jnp.where(iota((16, 128), 1) < 64, meta_in[0, :16], meta_in[1, :16])
    factors = order_weights([halo_depth[...]] + [halo_depth_in[k - 1] for k in range(1, n_block)], ranks)
    for i in range(16):
        shares[i : i + 1] = factors[i]
    line = iota((32, 128), 0)
    row = line // 4 + 4 * me - 2
    source = jnp.where((row >= 0) & (row < 32), line // 2 % 2 * 64 + row * 2 + line % 2, -1)
    turn = (iota((32, 128), 1) == source).astype(f32).astype(bf16)
    high = shares[...].astype(bf16)
    low = (shares[...] - high.astype(f32)).astype(bf16)
    share = dot_nt(turn, high) + dot_nt(turn, low)
    mixed = jnp.zeros((32, 128), f32)
    for k in range(n_block):
        tint = halo[pl.ds(pl.multiple_of(16 * me, 16), 32), :] if k == 0 else halo_in[k - 1]
        factor = jnp.where(iota((32, 128), 1) < 64, share[:, 2 * k : 2 * k + 1], share[:, 2 * k + 1 : 2 * k + 2])
        mixed = mixed + factor * tint.astype(f32)
    halo_out[...] = (mixed + pltpu.roll(mixed, 64, 1)).astype(bf16)

    for unit in range(3):

        @pl.when(has_source(unit))
        def _():
            pass_copy(unit).wait_recv()
            window_out[3 - unit % 2 * 3] = passed_in[unit]

    @pl.when(me == n_block - 1)
    def _():
        window_out[3] = jnp.zeros((FEAT, 128), bf16)

    for m in range(2):
        for k in range(1, n_block):
            last_copy(k, m).wait_recv()
    mixed = combine(tiles.at[3, last_tile(me)], last_in)
    window_out[me % 2 * 2] = (mixed * jnp.where(me > 0, 1.0, 0.0)).astype(bf16)
    decode(n_block, n_patch, seam, window_out, halo_out, meta_in.at[0, pl.ds(16, 8)], out, k0, k1, k2, k3, res)

    for side in range(2):
        for copy in side_copies(side):
            pl.when(sides[side][1])(copy.wait_send)
    for k in range(1, n_block):
        for copy in halo_copies(k) + [last_copy(k, 0), last_copy(k, 1)]:
            copy.wait_send()
    for unit in range(3):
        pl.when(has_target(unit))(pass_copy(unit).wait_send)
        sent = pltpu.make_async_copy(tiles_in.at[unit, pl.ds(0, 3)], tiles_in.at[unit, pl.ds(0, 3)], tile_send.at[unit])
        more = pltpu.make_async_copy(tiles_in.at[unit, 3], tiles_in.at[unit, 3], tile_send.at[unit])
        sent.wait()
        pl.when(me % 2 != unit // 2)(more.wait)


def render(order, seam, x, w_in, w_mid, w_feat, w_dens, w_conv, w_color, n_block, n_patch):
    vmem = pl.BlockSpec(memory_space=pltpu.VMEM)
    smem = pl.BlockSpec(memory_space=pltpu.SMEM)
    dma = pltpu.SemaphoreType.DMA
    peers = n_block - 1
    rows = 2 * FEAT + 8
    return pl.pallas_call(
        functools.partial(field_kernel, n_block, n_patch),
        out_shape=jax.ShapeDtypeStruct((3, 16, 256), f32),
        in_specs=[smem, smem] + [vmem] * 7,
        out_specs=vmem,
        scratch_shapes=[
            pltpu.VMEM((4, FEAT, 128), bf16),
            pltpu.VMEM((32, 128), bf16),
            pltpu.VMEM((256, 576), bf16),
            pltpu.VMEM((256, 1024), bf16),
            pltpu.VMEM((256, 576), bf16),
            pltpu.VMEM((288, 1024), f32),
            pltpu.VMEM((2, 128, 128), f32),
            pltpu.VMEM((128, 1024), bf16),
            pltpu.VMEM((2, 1024, 128), bf16),
            pltpu.VMEM((2, WIDTH, WIDTH), bf16),
            pltpu.VMEM((2, WIDTH, WIDTH), bf16),
            pltpu.VMEM((2, FEAT + 16, WIDTH), bf16),
            pltpu.VMEM((2, 2, 64, 128), bf16),
            pltpu.VMEM((2, 2, 64, 128), bf16),
            pltpu.VMEM((24, 128), jnp.int32),
            pltpu.VMEM((2, 24, 128), jnp.int32),
            pltpu.VMEM((8, 512), f32),
            pltpu.VMEM((4, 4, rows, 128), bf16),
            pltpu.VMEM((3, peers, rows, 128), bf16),
            pltpu.VMEM((peers, rows, 128), bf16),
            pltpu.VMEM((3, FEAT, 128), bf16),
            pltpu.VMEM((3, FEAT, 128), bf16),
            pltpu.VMEM((144, 128), bf16),
            pltpu.VMEM((peers, 32, 128), bf16),
            pltpu.VMEM((8, 128), bf16),
            pltpu.VMEM((peers, 8, 128), bf16),
            pltpu.VMEM((16, 128), f32),
            pltpu.VMEM((16, 128), f32),
            dma((2,)), dma((2,)), dma((2,)), dma((2,)), dma((3,)), dma((3,)), dma((2, peers)), dma((2, peers)),
            dma((3,)), dma((3,)), dma((2, peers)), dma((2, peers)),
        ],
        compiler_params=pltpu.CompilerParams(collective_id=0, has_side_effects=True),
        name="field",
    )(order, seam, x, w_in, w_mid, w_feat, w_dens, w_conv, w_color)


def body(samples_in, block_order, seam_link, w_in, w_mid, w_feat, w_density, w_conv, w_color):
    n_block, n_patch = lax.axis_size("block"), lax.axis_size("patch")
    x = samples_in.reshape(2, RAYS // 128, 128, SAMP * ENC)
    return render(
        block_order, seam_link, x, w_in, w_mid, jnp.swapaxes(w_feat, 1, 2), w_density, w_conv, w_color, n_block, n_patch
    )


def solution(mesh):
    return jax.shard_map(
        body,
        mesh=mesh,
        in_specs=(
            P("block", None, "patch", None),
            P("patch", None),
            P("patch"),
            P("block", None, None),
            P("block", None, None, None),
            P("block", None, None),
            P("block", None),
            P(),
            P(),
        ),
        out_specs=P(None, "block", "patch"),
        check_vma=False,
    )
```

```python
import functools

import jax
import jax.numpy as jnp
from jax import lax
from jax.experimental import pallas as pl
from jax.experimental.pallas import tpu as pltpu
from jax.sharding import PartitionSpec as P

f32, bf16 = jnp.float32, jnp.bfloat16
MESH = pl.DeviceIdType.MESH

ENC = 32
SAMP = 4
STEP = 0.03
FEAT = 64
WIDTH = 256
COLS = 64
RAYS = 2048
PITCH = 128


def iota(shape, dim):
    return lax.broadcasted_iota(jnp.int32, shape, dim)


def relu(x):
    return jnp.maximum(x, 0.0)


def dot(a, b):
    return jnp.dot(a, b, preferred_element_type=f32)


def dot_nt(a, b):
    return lax.dot_general(a, b, (((1,), (1,)), ((), ())), preferred_element_type=f32)


def field_chunks(streams):
    count = len(streams)
    hs = [relu(dot_nt(w1, x)).astype(bf16) for x, w1, w2, w3, head in streams]
    hs = [jnp.concatenate([h[WIDTH * s : WIDTH * (s + 1)] for s in range(SAMP)], axis=1) for h in hs]
    hs = [relu(dot(streams[i][2], hs[i])).astype(bf16) for i in range(count)]
    hs = [relu(dot(streams[i][3], hs[i])).astype(bf16) for i in range(count)]
    outs = [dot(streams[i][4], hs[i]) for i in range(count)]
    results = []
    for out in outs:
        rays = out.shape[1] // SAMP
        raw = out[FEAT : FEAT + 1]
        optical = STEP * (jnp.maximum(raw, 0.0) + jnp.log(1.0 + jnp.exp(-jnp.abs(raw))))
        total = jnp.zeros((1, rays), f32)
        colour = jnp.zeros((FEAT, rays), f32)
        for s in range(SAMP):
            here = optical[:, s * rays : (s + 1) * rays]
            weight = jnp.exp(-total) * (1.0 - jnp.exp(-here))
            total = total + here
            colour = colour + weight * out[:FEAT, s * rays : (s + 1) * rays]
        results.append((total, colour))
    return results


def phase_source(phase, tap):
    return (phase + tap - 1) // 2


def put(ref, row, col, value):
    ref[row : row + value.shape[0], col : col + value.shape[1]] = value


def enlarge_weights(ref, w_conv, layer):
    taps = [[w_conv[layer, a, e].astype(f32) for e in range(3)] for a in range(3)]
    for pa in range(2):
        for pb in range(2):
            for dr in range(-1, 2):
                for dc in range(-1, 2):
                    hits = [taps[a][e] for a in range(3) for e in range(3)
                            if phase_source(pa, a) == dr and phase_source(pb, e) == dc]
                    value = sum(hits[1:], hits[0]) if hits else jnp.zeros((FEAT, FEAT), f32)
                    put(ref, (2 * pa + pb) * FEAT, ((dr + 1) * 3 + dc + 1) * FEAT, value.astype(bf16))


def dense_weights(ref, w_conv, layer):
    for qa in range(2):
        for qb in range(2):
            for s in range(-1, 3):
                for t in range(-1, 3):
                    a, e = s - qa + 1, t - qb + 1
                    inside = 0 <= a <= 2 and 0 <= e <= 2
                    value = w_conv[layer, a, e] if inside else jnp.zeros((FEAT, FEAT), bf16)
                    put(ref, (2 * qa + qb) * FEAT, ((s + 1) * 4 + t + 1) * FEAT, value)


def colour_weights(ref, w_conv, w_color, layer):
    ref[...] = jnp.zeros_like(ref)
    for a in range(3):
        for e in range(3):
            tint = dot(w_color[...], w_conv[layer, a, e])
            for i in range(4):
                for j in range(4):
                    group = (i - a + 2) * 6 + (j - e + 2)
                    cell = ((i // 2 * 2 + j // 2) * 2 + i % 2) * 2 + j % 2
                    put(ref, 8 * group, cell * FEAT, tint)


def moved(x, by):
    return pltpu.roll(x, (-by) % x.shape[1], 1)


def lines(x, first, count):
    return x[:, first * PITCH : (first + count) * PITCH]


def prepare(w_conv, w_color, k0, k1, k2, k3):
    enlarge_weights(k0, w_conv, 0)
    dense_weights(k1, w_conv, 1)
    enlarge_weights(k2, w_conv, 2)
    colour_weights(k3, w_conv, w_color, 3)


def decode(n_block, n_patch, seam, window, halo, link, out, k0, k1, k2, k3, res):
    me = lax.axis_index("block")
    place = lax.axis_index("patch")

    lane = iota((1, PITCH), 1)
    right_open = jnp.where(place < n_patch - 1, seam[0], 0).astype(f32)
    left_open = link[0:1].astype(f32)
    inner = jnp.where(lane < 2, left_open, jnp.where(lane < COLS + 2, 1.0, jnp.where(lane < COLS + 4, right_open, 0.0)))
    top = inner * jnp.where(me > 0, 1.0, 0.0)
    bottom = inner * jnp.where(me < n_block - 1, 1.0, 0.0)
    mask = jnp.concatenate([top] + [inner] * 4 + [bottom], axis=1)

    source = iota((128, 256), 0)
    move = (iota((128, 256), 1) == source // COLS * PITCH + source % COLS + 2).astype(f32).astype(bf16)
    body = dot(window[...].reshape(4 * FEAT, 128), move)
    image = jnp.concatenate([body[FEAT * t : FEAT * (t + 1)] for t in range(4)], axis=1)
    source = iota((32, 8 * PITCH), 0)
    target = source // 4 * PITCH + source % 2 + source // 2 % 2 * (COLS + 2)
    halo_move = (iota((32, 8 * PITCH), 1) == target).astype(f32).astype(bf16)
    image = image + dot(halo[...].astype(f32).T[:FEAT].astype(bf16), halo_move)
    image = image * jnp.concatenate([inner] * 8, axis=1)

    views = {-1: moved(image, -1).astype(bf16), 0: image.astype(bf16), 1: moved(image, 1).astype(bf16)}
    patches = jnp.concatenate([lines(views[dc], 1 + dr, 6) for dr in range(-1, 2) for dc in range(-1, 2)], axis=0)
    first = relu(dot(k0[...], patches)) * mask

    def column_views(maps):
        cell = lambda a, b: maps[(2 * a + b) * FEAT : (2 * a + b + 1) * FEAT]
        return [{-1: moved(cell(a, 1), -1).astype(bf16), 0: cell(a, 0).astype(bf16), 1: cell(a, 1).astype(bf16),
                 2: moved(cell(a, 0), 1).astype(bf16)} for a in range(2)]

    views = column_views(first)
    empty = jnp.zeros((FEAT, PITCH), bf16)
    parts = []
    for s in range(-1, 3):
        for t in range(-1, 3):
            view = views[s % 2][t]
            if s == -1:
                view = jnp.concatenate([empty, lines(view, 0, 5)], axis=1)
            if s == 2:
                view = jnp.concatenate([lines(view, 1, 5), empty], axis=1)
            parts.append(view)
    second = relu(dot(k1[...], jnp.concatenate(parts, axis=0))) * mask

    views = column_views(second)
    parts = []
    for qa in range(2):
        for qb in range(2):
            cells = []
            for s in range(qa - 1, qa + 2):
                for t in range(qb - 1, qb + 2):
                    start = s // 2 + 1 - qa
                    cells.append(lines(views[s % 2][t], start, 5))
            third = relu(dot(k2[...], jnp.concatenate(cells, axis=0))) * lines(mask, 1 - qa, 5)
            third = third.astype(bf16)
            blank = jnp.zeros((4 * FEAT, PITCH), bf16)
            parts.append(jnp.concatenate([third, blank] if qa else [blank, third], axis=1))
    spread = dot(k3[...].astype(bf16), jnp.concatenate(parts, axis=0))

    def cell(i, j):
        group = (i + 1) * 6 + j + 1
        return spread[8 * group : 8 * group + 8]

    def row(i, j):
        value = lines(cell(i, j), 1, 4)
        if i == 0:
            value = value + lines(cell(4, j), 0, 4)
        if i == 3:
            value = value + lines(cell(-1, j), 2, 4)
        return value

    stack = []
    for i in range(4):
        cols = [row(i, j) for j in range(-1, 5)]
        middle = cols[1:5]
        middle[0] = middle[0] + moved(cols[5], -1)
        middle[3] = middle[3] + moved(cols[0], 1)
        stack.append(middle)
    wide = jnp.concatenate(
        [jnp.concatenate([lines(stack[i][j], r, 1) for j in range(4)], axis=1) for r in range(4) for i in range(4)], axis=0
    )
    source = iota((4 * PITCH, 256), 0)
    at = source % PITCH - 2
    target = jnp.where((at >= 0) & (at < COLS), 4 * at + source // PITCH, -1)
    weave = (iota((4 * PITCH, 256), 1) == target).astype(f32).astype(bf16)
    high = wide.astype(bf16)
    low = (wide - high.astype(f32)).astype(bf16)
    woven = dot(high, weave) + dot(low, weave)
    for half in range(2):
        lanes = slice(128 * half, 128 * (half + 1))
        res[half] = woven[:, lanes]
        for k in range(3):
            out[k, :, lanes] = res[half, pl.ds(k, 16, stride=8), :]


def last_tile(device):
    return ((device + 1) // 2 + 3) % 4


def field_kernel(
    n_block, n_patch, order, seam, x, w_in, w_mid, w_feat, w_dens, w_conv, w_color, out,
    window_out, halo_out, k0, k1, k2, k3, res,
    spread, w1, w2, w3, head, rays_out, rays_in, meta, meta_in, depth_rows, tiles, tiles_in, last_in, passed, passed_in,
    halo, halo_in, halo_depth, halo_depth_in, lines16, shares,
    rays_send, rays_recv, meta_send, meta_recv, tile_send, tile_recv, last_send, last_recv, pass_send, pass_recv,
    halo_send, halo_recv,
):
    me = lax.axis_index("block")
    place = lax.axis_index("patch")
    sides = ((place - 1, place > 0), (place + 1, place < n_patch - 1))
    rays_in[...] = jnp.zeros_like(rays_in)
    meta_in[...] = jnp.zeros_like(meta_in)
    barrier = pltpu.get_barrier_semaphore()
    for k in range(1, n_block):
        pl.semaphore_signal(barrier, inc=1, device_id=((me + k) % n_block, place), device_id_type=MESH)
    for side, there in sides:

        @pl.when(there)
        def _():
            pl.semaphore_signal(barrier, inc=1, device_id=(me, side), device_id_type=MESH)

    line = iota((16, 256), 0)
    wanted = line % 8 // 2 * COLS + line % 2 + jnp.where(line >= 8, COLS - 2, 0)
    pick = (iota((16, 256), 1) == wanted).astype(f32).astype(bf16)
    for m in range(2):
        found = [dot(pick, x[m, 2 * g : 2 * g + 2].reshape(256, 128)) for g in range(8)]
        for side in range(2):
            rows = jnp.concatenate([f[8 * side : 8 * side + 8] for f in found], axis=0)
            rays_out[side, m] = rows.astype(bf16)
    slot = iota((16, 128), 0)
    member = 2 * ((me + n_block - slot // 2) % n_block) + slot % 2
    rank = jnp.zeros((16, 128), jnp.int32)
    for k in range(16):
        rank = jnp.where(member == order[0, k], k, rank)
    meta[:16] = rank
    meta[16:] = jnp.full((8, 128), jnp.where(place < n_patch - 1, seam[0], 0), jnp.int32)

    spread[...] = jnp.zeros_like(spread)
    for m in range(2):
        for s in range(SAMP):
            spread[ENC * s : ENC * (s + 1), WIDTH * s : WIDTH * (s + 1)] = w_in[m]
        w1[m] = spread[...].T
        w2[m] = w_mid[m, 0].T
        w3[m] = w_mid[m, 1].T
        head[m, :FEAT] = w_feat[m]
        head[m, FEAT:] = jnp.broadcast_to(w_dens[pl.ds(m, 1), :], (16, WIDTH))
    depth_rows[...] = jnp.zeros_like(depth_rows)

    def side_copies(side):
        target = (me, sides[side][0])
        return [
            pltpu.make_async_remote_copy(
                src_ref=rays_out.at[side], dst_ref=rays_in.at[1 - side], send_sem=rays_send.at[side],
                recv_sem=rays_recv.at[1 - side], device_id=target, device_id_type=MESH,
            ),
            pltpu.make_async_remote_copy(
                src_ref=meta, dst_ref=meta_in.at[1 - side], send_sem=meta_send.at[side],
                recv_sem=meta_recv.at[1 - side], device_id=target, device_id_type=MESH,
            ),
        ]

    def weights(m):
        return w1[m], w2[m], w3[m], head[m]

    def depth_block(m, total):
        lanes = slice(0, total.shape[1])
        high = total.astype(bf16).astype(f32)
        depth_rows[m : m + 1, lanes] = high
        depth_rows[2 + m : 3 + m, lanes] = total - high

    def rays_of(unit, m):
        return jnp.concatenate([x[m, 4 * j + unit] for j in range(4)], axis=0)

    def keep(unit, m, tint):
        tint = tint.astype(bf16)
        for j in range(4):
            tiles[unit, j, FEAT * m : FEAT * (m + 1)] = tint[:, 128 * j : 128 * (j + 1)]

    def keep_depth(unit):
        rows = depth_rows[...].astype(bf16)
        for j in range(4):
            tiles[unit, j, 2 * FEAT :] = rows[:, 128 * j : 128 * (j + 1)]

    def store(unit, results):
        for m, (total, tint) in enumerate(results):
            keep(unit, m, tint)
            depth_block(m, total)
        keep_depth(unit)

    def send_owner(unit):
        for j in range(4):
            owner = 2 * j + unit // 2

            @pl.when(owner != me)
            def _():
                pltpu.make_async_remote_copy(
                    src_ref=tiles.at[unit, j], dst_ref=tiles_in.at[unit, (owner + n_block - me) % n_block - 1],
                    send_sem=tile_send.at[unit], recv_sem=tile_recv.at[unit],
                    device_id=(owner, place), device_id_type=MESH,
                ).start()

    results = field_chunks([(rays_of(unit, m), *weights(m)) for unit in range(2) for m in range(2)])
    store(0, results[:2])
    store(1, results[2:])
    count = (place > 0).astype(jnp.int32) + (place < n_patch - 1).astype(jnp.int32)
    pl.semaphore_wait(barrier, n_block - 1 + count)
    for side in range(2):
        for copy in side_copies(side):
            pl.when(sides[side][1])(copy.start)
    send_owner(0)
    send_owner(1)
    store(2, field_chunks([(rays_of(2, m), *weights(m)) for m in range(2)]))
    send_owner(2)

    for side in range(2):
        for copy in side_copies(side):
            pl.when(sides[1 - side][1])(copy.wait_recv)
    results = field_chunks(
        [(jnp.concatenate([rays_in[0, m], rays_in[1, m]], axis=0), *weights(m)) for m in range(2)]
        + [(rays_of(3, 0), *weights(0))]
    )
    ((last_total, last_tint),) = results[2:]
    results = results[:2]
    for m, (total, tint) in enumerate(results):
        depth_block(m, total)
    halo_depth[...] = depth_rows[:, :128].astype(bf16)
    ray = iota((144, 128), 0) - 8
    source = jnp.where((ray >= 0) & (ray < 128), ray // 2 % 2 * 64 + ray // 4 * 2 + ray % 2, -1)
    turn = (iota((144, 128), 1) == source).astype(f32).astype(bf16)
    both = jnp.concatenate([tint for total, tint in results], axis=0).astype(bf16)
    halo[...] = dot_nt(turn, both).astype(bf16)

    def halo_copies(k):
        peer = (me + k) % n_block
        return [
            pltpu.make_async_remote_copy(
                src_ref=halo.at[pl.ds(pl.multiple_of(16 * peer, 16), 32)], dst_ref=halo_in.at[k - 1],
                send_sem=halo_send.at[0, k - 1], recv_sem=halo_recv.at[0, k - 1],
                device_id=(peer, place), device_id_type=MESH,
            ),
            pltpu.make_async_remote_copy(
                src_ref=halo_depth, dst_ref=halo_depth_in.at[k - 1],
                send_sem=halo_send.at[1, k - 1], recv_sem=halo_recv.at[1, k - 1],
                device_id=(peer, place), device_id_type=MESH,
            ),
        ]

    for k in range(1, n_block):
        for copy in halo_copies(k):
            copy.start()

    def last_copy(k, m):
        peer = (me + k) % n_block
        rows = pl.ds(0, FEAT) if m == 0 else pl.ds(FEAT, FEAT + 8)
        return pltpu.make_async_remote_copy(
            src_ref=tiles.at[3, last_tile(peer), rows], dst_ref=last_in.at[k - 1, rows],
            send_sem=last_send.at[m, k - 1], recv_sem=last_recv.at[m, k - 1],
            device_id=(peer, place), device_id_type=MESH,
        )

    for m in range(2):
        total, tint = (last_total, last_tint) if m == 0 else field_chunks([(rays_of(3, 1), *weights(1))])[0]
        keep(3, m, tint)
        depth_block(m, total)
        if m == 1:
            keep_depth(3)
        for k in range(1, n_block):
            last_copy(k, m).start()

    def order_weights(blocks, ranks):
        for k, block in enumerate(blocks):
            block = block.astype(f32)
            lines16[2 * k : 2 * k + 2] = block[0:2] + block[2:4]
        depths = lines16[...]
        prefixes = [
            jnp.sum(jnp.where(ranks < ranks[i : i + 1], depths, 0.0), axis=0, keepdims=True) for i in range(16)
        ]
        return [jnp.exp(-prefix) for prefix in prefixes]

    def combine(own, got):
        slots = [own] + [got.at[k - 1] for k in range(1, n_block)]
        factors = order_weights([slot[2 * FEAT :] for slot in slots], meta[:16])
        mixed = jnp.zeros((FEAT, 128), f32)
        for i in range(16):
            tint = slots[i // 2][i % 2 * FEAT : (i % 2 + 1) * FEAT]
            mixed = mixed + factors[i] * tint.astype(f32)
        return mixed

    def pass_copy(unit):
        target = me - 1 if unit % 2 == 0 else me + 1
        return pltpu.make_async_remote_copy(
            src_ref=passed.at[unit], dst_ref=passed_in.at[unit], send_sem=pass_send.at[unit],
            recv_sem=pass_recv.at[unit], device_id=(target, place), device_id_type=MESH,
        )

    def mine(unit):
        return me % 2 == unit // 2

    def has_target(unit):
        return mine(unit) & ((me > 0) if unit % 2 == 0 else (me < n_block - 1))

    def has_source(unit):
        return (me % 2 != unit // 2) & ((me < n_block - 1) if unit % 2 == 0 else (me > 0))

    for unit in range(3):

        @pl.when(mine(unit))
        def _():
            pltpu.make_async_copy(tiles_in.at[unit], tiles_in.at[unit], tile_recv.at[unit]).wait()
            passed[unit] = combine(tiles.at[unit, me // 2], tiles_in.at[unit]).astype(bf16)

        pl.when(has_target(unit))(pass_copy(unit).start)

        @pl.when(mine(unit))
        def _():
            window_out[1 + unit % 2] = passed[unit]

    prepare(w_conv, w_color, k0, k1, k2, k3)

    for k in range(1, n_block):
        for copy in halo_copies(k):
            copy.wait_recv()
    ranks = jnp.where(iota((16, 128), 1) < 64, meta_in[0, :16], meta_in[1, :16])
    factors = order_weights([halo_depth[...]] + [halo_depth_in[k - 1] for k in range(1, n_block)], ranks)
    for i in range(16):
        shares[i : i + 1] = factors[i]
    line = iota((32, 128), 0)
    row = line // 4 + 4 * me - 2
    source = jnp.where((row >= 0) & (row < 32), line // 2 % 2 * 64 + row * 2 + line % 2, -1)
    turn = (iota((32, 128), 1) == source).astype(f32).astype(bf16)
    high = shares[...].astype(bf16)
    low = (shares[...] - high.astype(f32)).astype(bf16)
    share = dot_nt(turn, high) + dot_nt(turn, low)
    mixed = jnp.zeros((32, 128), f32)
    for k in range(n_block):
        tint = halo[pl.ds(pl.multiple_of(16 * me, 16), 32), :] if k == 0 else halo_in[k - 1]
        factor = jnp.where(iota((32, 128), 1) < 64, share[:, 2 * k : 2 * k + 1], share[:, 2 * k + 1 : 2 * k + 2])
        mixed = mixed + factor * tint.astype(f32)
    halo_out[...] = (mixed + pltpu.roll(mixed, 64, 1)).astype(bf16)

    for unit in range(3):

        @pl.when(has_source(unit))
        def _():
            pass_copy(unit).wait_recv()
            window_out[3 - unit % 2 * 3] = passed_in[unit]

    @pl.when(me == n_block - 1)
    def _():
        window_out[3] = jnp.zeros((FEAT, 128), bf16)

    for m in range(2):
        for k in range(1, n_block):
            last_copy(k, m).wait_recv()
    mixed = combine(tiles.at[3, last_tile(me)], last_in)
    window_out[me % 2 * 2] = (mixed * jnp.where(me > 0, 1.0, 0.0)).astype(bf16)
    decode(n_block, n_patch, seam, window_out, halo_out, meta_in.at[0, pl.ds(16, 8)], out, k0, k1, k2, k3, res)

    for side in range(2):
        for copy in side_copies(side):
            pl.when(sides[side][1])(copy.wait_send)
    for k in range(1, n_block):
        for copy in halo_copies(k) + [last_copy(k, 0), last_copy(k, 1)]:
            copy.wait_send()
    for unit in range(3):
        pl.when(has_target(unit))(pass_copy(unit).wait_send)
        sent = pltpu.make_async_copy(tiles_in.at[unit, pl.ds(0, 3)], tiles_in.at[unit, pl.ds(0, 3)], tile_send.at[unit])
        more = pltpu.make_async_copy(tiles_in.at[unit, 3], tiles_in.at[unit, 3], tile_send.at[unit])
        sent.wait()
        pl.when(me % 2 != unit // 2)(more.wait)


def render(order, seam, x, w_in, w_mid, w_feat, w_dens, w_conv, w_color, n_block, n_patch):
    vmem = pl.BlockSpec(memory_space=pltpu.VMEM)
    smem = pl.BlockSpec(memory_space=pltpu.SMEM)
    dma = pltpu.SemaphoreType.DMA
    peers = n_block - 1
    rows = 2 * FEAT + 8
    return pl.pallas_call(
        functools.partial(field_kernel, n_block, n_patch),
        out_shape=jax.ShapeDtypeStruct((3, 16, 256), f32),
        in_specs=[smem, smem] + [vmem] * 7,
        out_specs=vmem,
        scratch_shapes=[
            pltpu.VMEM((4, FEAT, 128), bf16),
            pltpu.VMEM((32, 128), bf16),
            pltpu.VMEM((256, 576), bf16),
            pltpu.VMEM((256, 1024), bf16),
            pltpu.VMEM((256, 576), bf16),
            pltpu.VMEM((288, 1024), f32),
            pltpu.VMEM((2, 128, 128), f32),
            pltpu.VMEM((128, 1024), bf16),
            pltpu.VMEM((2, 1024, 128), bf16),
            pltpu.VMEM((2, WIDTH, WIDTH), bf16),
            pltpu.VMEM((2, WIDTH, WIDTH), bf16),
            pltpu.VMEM((2, FEAT + 16, WIDTH), bf16),
            pltpu.VMEM((2, 2, 64, 128), bf16),
            pltpu.VMEM((2, 2, 64, 128), bf16),
            pltpu.VMEM((24, 128), jnp.int32),
            pltpu.VMEM((2, 24, 128), jnp.int32),
            pltpu.VMEM((8, 512), f32),
            pltpu.VMEM((4, 4, rows, 128), bf16),
            pltpu.VMEM((3, peers, rows, 128), bf16),
            pltpu.VMEM((peers, rows, 128), bf16),
            pltpu.VMEM((3, FEAT, 128), bf16),
            pltpu.VMEM((3, FEAT, 128), bf16),
            pltpu.VMEM((144, 128), bf16),
            pltpu.VMEM((peers, 32, 128), bf16),
            pltpu.VMEM((8, 128), bf16),
            pltpu.VMEM((peers, 8, 128), bf16),
            pltpu.VMEM((16, 128), f32),
            pltpu.VMEM((16, 128), f32),
            dma((2,)), dma((2,)), dma((2,)), dma((2,)), dma((3,)), dma((3,)), dma((2, peers)), dma((2, peers)),
            dma((3,)), dma((3,)), dma((2, peers)), dma((2, peers)),
        ],
        compiler_params=pltpu.CompilerParams(collective_id=0, has_side_effects=True),
        name="field",
    )(order, seam, x, w_in, w_mid, w_feat, w_dens, w_conv, w_color)


def body(samples_in, block_order, seam_link, w_in, w_mid, w_feat, w_density, w_conv, w_color):
    n_block, n_patch = lax.axis_size("block"), lax.axis_size("patch")
    x = samples_in.reshape(2, RAYS // 128, 128, SAMP * ENC)
    return render(
        block_order, seam_link, x, w_in, w_mid, jnp.swapaxes(w_feat, 1, 2), w_density, w_conv, w_color, n_block, n_patch
    )


def solution(mesh):
    return jax.shard_map(
        body,
        mesh=mesh,
        in_specs=(
            P("block", None, "patch", None),
            P("patch", None),
            P("patch"),
            P("block", None, None),
            P("block", None, None, None),
            P("block", None, None),
            P("block", None),
            P(),
            P(),
        ),
        out_specs=P(None, "block", "patch"),
        check_vma=False,
    )
```

```python
import functools

import jax
import jax.numpy as jnp
from jax import lax
from jax.experimental import pallas as pl
from jax.experimental.pallas import tpu as pltpu
from jax.sharding import PartitionSpec as P

f32, bf16 = jnp.float32, jnp.bfloat16
MESH = pl.DeviceIdType.MESH

ENC = 32
SAMP = 4
STEP = 0.03
FEAT = 64
WIDTH = 256
COLS = 64
RAYS = 2048
PITCH = 68
SPAN = 512
ROLL = bf16


def iota(shape, dim):
    return lax.broadcasted_iota(jnp.int32, shape, dim)


def relu(x):
    return jnp.maximum(x, 0.0)


def dot(a, b):
    return jnp.dot(a, b, preferred_element_type=f32)


def dot_nt(a, b):
    return lax.dot_general(a, b, (((1,), (1,)), ((), ())), preferred_element_type=f32)


def field_chunks(streams):
    count = len(streams)
    hs = [relu(dot_nt(w1, x)).astype(bf16) for x, w1, w2, w3, head in streams]
    hs = [jnp.concatenate([h[WIDTH * s : WIDTH * (s + 1)] for s in range(SAMP)], axis=1) for h in hs]
    hs = [relu(dot(streams[i][2], hs[i])).astype(bf16) for i in range(count)]
    hs = [relu(dot(streams[i][3], hs[i])).astype(bf16) for i in range(count)]
    outs = [dot(streams[i][4], hs[i]) for i in range(count)]
    results = []
    for out in outs:
        rays = out.shape[1] // SAMP
        raw = out[FEAT : FEAT + 1]
        optical = STEP * (jnp.maximum(raw, 0.0) + jnp.log(1.0 + jnp.exp(-jnp.abs(raw))))
        total = jnp.zeros((1, rays), f32)
        colour = jnp.zeros((FEAT, rays), f32)
        for s in range(SAMP):
            here = optical[:, s * rays : (s + 1) * rays]
            weight = jnp.exp(-total) * (1.0 - jnp.exp(-here))
            total = total + here
            colour = colour + weight * out[:FEAT, s * rays : (s + 1) * rays]
        results.append((total, colour))
    return results


def phase_source(phase, tap):
    return (phase + tap - 1) // 2


def put(ref, row, col, value):
    ref[row : row + value.shape[0], col : col + value.shape[1]] = value


def enlarge_weights(ref, w_conv, layer):
    taps = [[w_conv[layer, a, e].astype(f32) for e in range(3)] for a in range(3)]
    for pa in range(2):
        for pb in range(2):
            for dr in range(-1, 2):
                for dc in range(-1, 2):
                    hits = [taps[a][e] for a in range(3) for e in range(3)
                            if phase_source(pa, a) == dr and phase_source(pb, e) == dc]
                    value = sum(hits[1:], hits[0]) if hits else jnp.zeros((FEAT, FEAT), f32)
                    put(ref, (2 * pa + pb) * FEAT, ((dr + 1) * 3 + dc + 1) * FEAT, value.astype(bf16))


def dense_weights(ref, w_conv, layer):
    for qa in range(2):
        for qb in range(2):
            for s in range(-1, 3):
                for t in range(-1, 3):
                    a, e = s - qa + 1, t - qb + 1
                    inside = 0 <= a <= 2 and 0 <= e <= 2
                    value = w_conv[layer, a, e] if inside else jnp.zeros((FEAT, FEAT), bf16)
                    put(ref, (2 * qa + qb) * FEAT, ((s + 1) * 4 + t + 1) * FEAT, value)


def colour_weights(ref, w_conv, w_color, layer):
    ref[...] = jnp.zeros_like(ref)
    for a in range(3):
        for e in range(3):
            tint = dot(w_color[...], w_conv[layer, a, e])
            for i in range(4):
                for j in range(4):
                    group = (i - a + 2) * 6 + (j - e + 2)
                    cell = ((i // 2 * 2 + j // 2) * 2 + i % 2) * 2 + j % 2
                    put(ref, 8 * group, cell * FEAT, tint)


def moved(x, by):
    return pltpu.roll(x, (-by) % x.shape[1], 1) if by else x


def prepare(w_conv, w_color, k0, k1, k2, k3, k4, place, halo_place, weave):
    enlarge_weights(k0, w_conv, 0)
    dense_weights(k1, w_conv, 1)
    enlarge_weights(k2, w_conv, 2)
    colour_weights(k3, w_conv, w_color, 3)
    k4[...] = k3[...].astype(bf16)
    source = iota(place.shape, 0)
    place[...] = (iota(place.shape, 1) == source // COLS * PITCH + source % COLS + 2).astype(f32).astype(bf16)
    source = iota(halo_place.shape, 0)
    target = source // 4 * PITCH + source % 2 + source // 2 % 2 * (COLS + 2)
    halo_place[...] = (iota(halo_place.shape, 1) == target).astype(f32).astype(bf16)
    source = iota(weave.shape, 0)
    target = jnp.where(source % 128 < COLS, 4 * (source % 128) + source // 128, -1)
    weave[...] = (iota(weave.shape, 1) == target).astype(f32).astype(bf16)


def decode(n_block, n_patch, seam, window, halo, link, out, k0, k1, k2, k4, place, halo_place, weave, res):
    me = lax.axis_index("block")
    column = lax.axis_index("patch")
    right_open = jnp.where(column < n_patch - 1, seam[0], 0).astype(f32)
    left_open = link[0:1, 0:1].astype(f32)

    def open_sides(lanes):
        at = iota((1, lanes), 1) % PITCH
        return jnp.where(at < 2, left_open, jnp.where(at < COLS + 2, 1.0, right_open))

    line = iota((1, SPAN), 1) // PITCH
    top = jnp.where(me > 0, 1.0, 0.0)
    bottom = jnp.where(me < n_block - 1, 1.0, 0.0)
    mask = jnp.where(line == 0, top, jnp.where(line < 5, 1.0, jnp.where(line == 5, bottom, 0.0))) * open_sides(SPAN)

    image = dot(jnp.concatenate([window[t] for t in range(4)], axis=1), place[...])
    image = image + dot(halo[...].astype(f32).T[:FEAT].astype(bf16), halo_place[...])
    image = (image * open_sides(image.shape[1])).astype(ROLL)
    patches = [
        moved(image, (dr + 1) * PITCH + dc)[:, :SPAN].astype(bf16) for dr in range(-1, 2) for dc in range(-1, 2)
    ]
    first = (relu(dot(k0[...], jnp.concatenate(patches, axis=0))) * mask).astype(ROLL)

    def views(maps):
        found = {}
        for s in range(-1, 3):
            for t in range(-1, 3):
                phase = (s % 2 * 2 + t % 2) * FEAT
                found[s, t] = moved(maps[phase : phase + FEAT], s // 2 * PITCH + t // 2).astype(bf16)
        return found

    cells = views(first)
    second = relu(dot(k1[...], jnp.concatenate([cells[s, t] for s in range(-1, 3) for t in range(-1, 3)], axis=0)))
    cells = views((second * mask).astype(ROLL))
    parts = []
    for qa in range(2):
        for qb in range(2):
            near = [cells[s, t] for s in range(qa - 1, qa + 2) for t in range(qb - 1, qb + 2)]
            parts.append((relu(dot(k2[...], jnp.concatenate(near, axis=0))) * mask).astype(bf16))
    spread = dot(k4[...], jnp.concatenate(parts, axis=0))

    def cell(i, j):
        group = (i + 1) * 6 + j + 1
        return spread[8 * group : 8 * group + 8]

    def row(i, j):
        value = cell(i, j)
        if i == 0:
            value = value + moved(cell(4, j), -PITCH)
        if i == 3:
            value = value + moved(cell(-1, j), PITCH)
        return value

    stack = []
    for i in range(4):
        cols = [row(i, j) for j in range(-1, 5)]
        middle = cols[1:5]
        middle[0] = middle[0] + moved(cols[5], -1)
        middle[3] = middle[3] + moved(cols[0], 1)
        stack.append(jnp.concatenate(middle, axis=0))
    stack = jnp.concatenate(stack, axis=0)
    starts = [(r + 1) * PITCH + 2 for r in range(4)]
    lines = [moved(stack[:, a // 128 * 128 : a // 128 * 128 + 256], a % 128)[:, :128] for a in starts[:3]]
    lines.append(moved(stack, starts[3])[:, :128])
    wide = jnp.concatenate(
        [
            jnp.concatenate([lines[r][8 * (4 * i + j) : 8 * (4 * i + j) + 8] for j in range(4)], axis=1)
            for r in range(4) for i in range(4)
        ],
        axis=0,
    )
    high = wide.astype(bf16)
    low = (wide - high.astype(f32)).astype(bf16)
    woven = dot(high, weave[...]) + dot(low, weave[...])
    for half in range(2):
        lanes = slice(128 * half, 128 * (half + 1))
        res[half] = woven[:, lanes]
        for k in range(3):
            out[k, :, lanes] = res[half, pl.ds(k, 16, stride=8), :]


def last_tile(device):
    return ((device + 1) // 2 + 3) % 4


def field_kernel(
    n_block, n_patch, seam, order_far, x_far, w_in_far, w_mid_far, w_feat_far, w_dens_far, w_conv_far, w_color_far, out,
    order, x, w_in, w_mid, w_feat, w_dens, w_conv, w_color, fetched,
    window_out, halo_out, k0, k1, k2, k3, k4, place_rows, place_halo, weave, res,
    spread, w1, w2, w3, head, rays_out, rays_in, meta, meta_in, depth_rows, tiles, tiles_in, last_in, passed, passed_in,
    halo, halo_in, halo_depth, halo_depth_in, lines16, shares,
    rays_send, rays_recv, meta_send, meta_recv, tile_send, tile_recv, last_send, last_recv, pass_send, pass_recv,
    halo_send, halo_recv,
):
    me = lax.axis_index("block")
    place = lax.axis_index("patch")
    sides = ((place - 1, place > 0), (place + 1, place < n_patch - 1))
    pairs = (
        (w_in_far, w_in), (w_mid_far, w_mid), (w_feat_far, w_feat), (w_dens_far, w_dens), (x_far, x), (order_far, order),
        (w_conv_far, w_conv), (w_color_far, w_color),
    )
    fetches = [pltpu.make_async_copy(far, near, fetched.at[i]) for i, (far, near) in enumerate(pairs)]
    for fetch in fetches:
        fetch.start()
    rays_in[...] = jnp.zeros_like(rays_in)
    meta_in[...] = jnp.zeros_like(meta_in)
    barrier = pltpu.get_barrier_semaphore()
    for k in range(1, n_block):
        pl.semaphore_signal(barrier, inc=1, device_id=((me + k) % n_block, place), device_id_type=MESH)
    for side, there in sides:

        @pl.when(there)
        def _():
            pl.semaphore_signal(barrier, inc=1, device_id=(me, side), device_id_type=MESH)

    spread[...] = jnp.zeros_like(spread)
    for fetch in fetches[:4]:
        fetch.wait()
    for m in range(2):
        for s in range(SAMP):
            spread[ENC * s : ENC * (s + 1), WIDTH * s : WIDTH * (s + 1)] = w_in[m]
        w1[m] = spread[...].T
        w2[m] = w_mid[m, 0].T
        w3[m] = w_mid[m, 1].T
        head[m, :FEAT] = w_feat[m]
        head[m, FEAT:] = jnp.broadcast_to(w_dens[pl.ds(m, 1), :], (16, WIDTH))
    for fetch in fetches[4:6]:
        fetch.wait()
    line = iota((16, 256), 0)
    wanted = line % 8 // 2 * COLS + line % 2 + jnp.where(line >= 8, COLS - 2, 0)
    pick = (iota((16, 256), 1) == wanted).astype(f32).astype(bf16)
    for m in range(2):
        found = [dot(pick, x[m, 2 * g : 2 * g + 2].reshape(256, 128)) for g in range(8)]
        for side in range(2):
            rows = jnp.concatenate([f[8 * side : 8 * side + 8] for f in found], axis=0)
            rays_out[side, m] = rows.astype(bf16)
    slot = iota((16, 128), 0)
    member = 2 * ((me + n_block - slot // 2) % n_block) + slot % 2
    rank = jnp.zeros((16, 128), jnp.int32)
    for k in range(16):
        rank = jnp.where(member == order[0, k], k, rank)
    meta[:16] = rank
    meta[16:] = jnp.full((8, 128), jnp.where(place < n_patch - 1, seam[0], 0), jnp.int32)

    depth_rows[...] = jnp.zeros_like(depth_rows)

    def side_copies(side):
        target = (me, sides[side][0])
        return [
            pltpu.make_async_remote_copy(
                src_ref=rays_out.at[side], dst_ref=rays_in.at[1 - side], send_sem=rays_send.at[side],
                recv_sem=rays_recv.at[1 - side], device_id=target, device_id_type=MESH,
            ),
            pltpu.make_async_remote_copy(
                src_ref=meta, dst_ref=meta_in.at[1 - side], send_sem=meta_send.at[side],
                recv_sem=meta_recv.at[1 - side], device_id=target, device_id_type=MESH,
            ),
        ]

    count = (place > 0).astype(jnp.int32) + (place < n_patch - 1).astype(jnp.int32)
    pl.semaphore_wait(barrier, n_block - 1 + count)
    for side in range(2):
        for copy in side_copies(side):
            pl.when(sides[side][1])(copy.start)

    def weights(m):
        return w1[m], w2[m], w3[m], head[m]

    def depth_block(m, total):
        lanes = slice(0, total.shape[1])
        high = total.astype(bf16).astype(f32)
        depth_rows[m : m + 1, lanes] = high
        depth_rows[2 + m : 3 + m, lanes] = total - high

    def rays_of(unit, m):
        return jnp.concatenate([x[m, 4 * j + unit] for j in range(4)], axis=0)

    def keep(unit, m, tint):
        tint = tint.astype(bf16)
        for j in range(4):
            tiles[unit, j, FEAT * m : FEAT * (m + 1)] = tint[:, 128 * j : 128 * (j + 1)]

    def keep_depth(unit):
        rows = depth_rows[...].astype(bf16)
        for j in range(4):
            tiles[unit, j, 2 * FEAT :] = rows[:, 128 * j : 128 * (j + 1)]

    def store(unit, results):
        for m, (total, tint) in enumerate(results):
            keep(unit, m, tint)
            depth_block(m, total)
        keep_depth(unit)

    def send_owner(unit):
        for j in range(4):
            owner = 2 * j + unit // 2

            @pl.when(owner != me)
            def _():
                pltpu.make_async_remote_copy(
                    src_ref=tiles.at[unit, j], dst_ref=tiles_in.at[unit, (owner + n_block - me) % n_block - 1],
                    send_sem=tile_send.at[unit], recv_sem=tile_recv.at[unit],
                    device_id=(owner, place), device_id_type=MESH,
                ).start()

    results = field_chunks([(rays_of(unit, m), *weights(m)) for unit in range(2) for m in range(2)])
    store(0, results[:2])
    store(1, results[2:])
    send_owner(0)
    send_owner(1)
    store(2, field_chunks([(rays_of(2, m), *weights(m)) for m in range(2)]))
    send_owner(2)

    for side in range(2):
        for copy in side_copies(side):
            pl.when(sides[1 - side][1])(copy.wait_recv)
    results = field_chunks(
        [(jnp.concatenate([rays_in[0, m], rays_in[1, m]], axis=0), *weights(m)) for m in range(2)]
        + [(rays_of(3, 0), *weights(0))]
    )
    ((last_total, last_tint),) = results[2:]
    results = results[:2]
    for m, (total, tint) in enumerate(results):
        depth_block(m, total)
    halo_depth[...] = depth_rows[:, :128].astype(bf16)
    ray = iota((144, 128), 0) - 8
    source = jnp.where((ray >= 0) & (ray < 128), ray // 2 % 2 * 64 + ray // 4 * 2 + ray % 2, -1)
    turn = (iota((144, 128), 1) == source).astype(f32).astype(bf16)
    both = jnp.concatenate([tint for total, tint in results], axis=0).astype(bf16)
    halo[...] = dot_nt(turn, both).astype(bf16)

    def halo_copies(k):
        peer = (me + k) % n_block
        return [
            pltpu.make_async_remote_copy(
                src_ref=halo.at[pl.ds(pl.multiple_of(16 * peer, 16), 32)], dst_ref=halo_in.at[k - 1],
                send_sem=halo_send.at[0, k - 1], recv_sem=halo_recv.at[0, k - 1],
                device_id=(peer, place), device_id_type=MESH,
            ),
            pltpu.make_async_remote_copy(
                src_ref=halo_depth, dst_ref=halo_depth_in.at[k - 1],
                send_sem=halo_send.at[1, k - 1], recv_sem=halo_recv.at[1, k - 1],
                device_id=(peer, place), device_id_type=MESH,
            ),
        ]

    for k in range(1, n_block):
        for copy in halo_copies(k):
            copy.start()

    def last_copy(k, m):
        peer = (me + k) % n_block
        rows = pl.ds(0, FEAT) if m == 0 else pl.ds(FEAT, FEAT + 8)
        return pltpu.make_async_remote_copy(
            src_ref=tiles.at[3, last_tile(peer), rows], dst_ref=last_in.at[k - 1, rows],
            send_sem=last_send.at[m, k - 1], recv_sem=last_recv.at[m, k - 1],
            device_id=(peer, place), device_id_type=MESH,
        )

    for m in range(2):
        total, tint = (last_total, last_tint) if m == 0 else field_chunks([(rays_of(3, 1), *weights(1))])[0]
        keep(3, m, tint)
        depth_block(m, total)
        if m == 1:
            keep_depth(3)
        for k in range(1, n_block):
            last_copy(k, m).start()

    def order_weights(blocks, ranks):
        for k, block in enumerate(blocks):
            block = block.astype(f32)
            lines16[2 * k : 2 * k + 2] = block[0:2] + block[2:4]
        depths = lines16[...]
        prefixes = [
            jnp.sum(jnp.where(ranks < ranks[i : i + 1], depths, 0.0), axis=0, keepdims=True) for i in range(16)
        ]
        return [jnp.exp(-prefix) for prefix in prefixes]

    def combine(own, got):
        slots = [own] + [got.at[k - 1] for k in range(1, n_block)]
        factors = order_weights([slot[2 * FEAT :] for slot in slots], meta[:16])
        mixed = jnp.zeros((FEAT, 128), f32)
        for i in range(16):
            tint = slots[i // 2][i % 2 * FEAT : (i % 2 + 1) * FEAT]
            mixed = mixed + factors[i] * tint.astype(f32)
        return mixed

    def pass_copy(unit):
        target = me - 1 if unit % 2 == 0 else me + 1
        return pltpu.make_async_remote_copy(
            src_ref=passed.at[unit], dst_ref=passed_in.at[unit], send_sem=pass_send.at[unit],
            recv_sem=pass_recv.at[unit], device_id=(target, place), device_id_type=MESH,
        )

    def mine(unit):
        return me % 2 == unit // 2

    def has_target(unit):
        return mine(unit) & ((me > 0) if unit % 2 == 0 else (me < n_block - 1))

    def has_source(unit):
        return (me % 2 != unit // 2) & ((me < n_block - 1) if unit % 2 == 0 else (me > 0))

    for unit in range(3):

        @pl.when(mine(unit))
        def _():
            pltpu.make_async_copy(tiles_in.at[unit], tiles_in.at[unit], tile_recv.at[unit]).wait()
            passed[unit] = combine(tiles.at[unit, me // 2], tiles_in.at[unit]).astype(bf16)

        pl.when(has_target(unit))(pass_copy(unit).start)

        @pl.when(mine(unit))
        def _():
            window_out[1 + unit % 2] = passed[unit]

    for fetch in fetches[6:]:
        fetch.wait()
    prepare(w_conv, w_color, k0, k1, k2, k3, k4, place_rows, place_halo, weave)

    for k in range(1, n_block):
        for copy in halo_copies(k):
            copy.wait_recv()
    ranks = jnp.where(iota((16, 128), 1) < 64, meta_in[0, :16], meta_in[1, :16])
    factors = order_weights([halo_depth[...]] + [halo_depth_in[k - 1] for k in range(1, n_block)], ranks)
    for i in range(16):
        shares[i : i + 1] = factors[i]
    line = iota((32, 128), 0)
    row = line // 4 + 4 * me - 2
    source = jnp.where((row >= 0) & (row < 32), line // 2 % 2 * 64 + row * 2 + line % 2, -1)
    turn = (iota((32, 128), 1) == source).astype(f32).astype(bf16)
    high = shares[...].astype(bf16)
    low = (shares[...] - high.astype(f32)).astype(bf16)
    share = dot_nt(turn, high) + dot_nt(turn, low)
    mixed = jnp.zeros((32, 128), f32)
    for k in range(n_block):
        tint = halo[pl.ds(pl.multiple_of(16 * me, 16), 32), :] if k == 0 else halo_in[k - 1]
        factor = jnp.where(iota((32, 128), 1) < 64, share[:, 2 * k : 2 * k + 1], share[:, 2 * k + 1 : 2 * k + 2])
        mixed = mixed + factor * tint.astype(f32)
    halo_out[...] = (mixed + pltpu.roll(mixed, 64, 1)).astype(bf16)

    for unit in range(3):

        @pl.when(has_source(unit))
        def _():
            pass_copy(unit).wait_recv()
            window_out[3 - unit % 2 * 3] = passed_in[unit]

    @pl.when(me == n_block - 1)
    def _():
        window_out[3] = jnp.zeros((FEAT, 128), bf16)

    for m in range(2):
        for k in range(1, n_block):
            last_copy(k, m).wait_recv()
    mixed = combine(tiles.at[3, last_tile(me)], last_in)
    window_out[me % 2 * 2] = (mixed * jnp.where(me > 0, 1.0, 0.0)).astype(bf16)
    decode(
        n_block, n_patch, seam, window_out, halo_out, meta_in.at[0, pl.ds(16, 8)], out, k0, k1, k2, k4,
        place_rows, place_halo, weave, res,
    )

    for side in range(2):
        for copy in side_copies(side):
            pl.when(sides[side][1])(copy.wait_send)
    for k in range(1, n_block):
        for copy in halo_copies(k) + [last_copy(k, 0), last_copy(k, 1)]:
            copy.wait_send()
    for unit in range(3):
        pl.when(has_target(unit))(pass_copy(unit).wait_send)
        sent = pltpu.make_async_copy(tiles_in.at[unit, pl.ds(0, 3)], tiles_in.at[unit, pl.ds(0, 3)], tile_send.at[unit])
        more = pltpu.make_async_copy(tiles_in.at[unit, 3], tiles_in.at[unit, 3], tile_send.at[unit])
        sent.wait()
        pl.when(me % 2 != unit // 2)(more.wait)


def render(order, seam, x, w_in, w_mid, w_feat, w_dens, w_conv, w_color, n_block, n_patch):
    vmem = pl.BlockSpec(memory_space=pltpu.VMEM)
    smem = pl.BlockSpec(memory_space=pltpu.SMEM)
    dma = pltpu.SemaphoreType.DMA
    peers = n_block - 1
    rows = 2 * FEAT + 8
    return pl.pallas_call(
        functools.partial(field_kernel, n_block, n_patch),
        out_shape=jax.ShapeDtypeStruct((3, 16, 256), f32),
        in_specs=[smem] + [pl.BlockSpec(memory_space=pl.ANY)] * 8,
        out_specs=vmem,
        scratch_shapes=[
            pltpu.SMEM(order.shape, jnp.int32),
            *[pltpu.VMEM(array.shape, bf16) for array in (x, w_in, w_mid, w_feat, w_dens, w_conv, w_color)],
            dma((8,)),
            pltpu.VMEM((4, FEAT, 128), bf16),
            pltpu.VMEM((32, 128), bf16),
            pltpu.VMEM((256, 576), bf16),
            pltpu.VMEM((256, 1024), bf16),
            pltpu.VMEM((256, 576), bf16),
            pltpu.VMEM((288, 1024), f32),
            pltpu.VMEM((288, 1024), bf16),
            pltpu.VMEM((512, 640), bf16),
            pltpu.VMEM((32, 640), bf16),
            pltpu.VMEM((512, 256), bf16),
            pltpu.VMEM((2, 128, 128), f32),
            pltpu.VMEM((128, 1024), bf16),
            pltpu.VMEM((2, 1024, 128), bf16),
            pltpu.VMEM((2, WIDTH, WIDTH), bf16),
            pltpu.VMEM((2, WIDTH, WIDTH), bf16),
            pltpu.VMEM((2, FEAT + 16, WIDTH), bf16),
            pltpu.VMEM((2, 2, 64, 128), bf16),
            pltpu.VMEM((2, 2, 64, 128), bf16),
            pltpu.VMEM((24, 128), jnp.int32),
            pltpu.VMEM((2, 24, 128), jnp.int32),
            pltpu.VMEM((8, 512), f32),
            pltpu.VMEM((4, 4, rows, 128), bf16),
            pltpu.VMEM((3, peers, rows, 128), bf16),
            pltpu.VMEM((peers, rows, 128), bf16),
            pltpu.VMEM((3, FEAT, 128), bf16),
            pltpu.VMEM((3, FEAT, 128), bf16),
            pltpu.VMEM((144, 128), bf16),
            pltpu.VMEM((peers, 32, 128), bf16),
            pltpu.VMEM((8, 128), bf16),
            pltpu.VMEM((peers, 8, 128), bf16),
            pltpu.VMEM((16, 128), f32),
            pltpu.VMEM((16, 128), f32),
            dma((2,)), dma((2,)), dma((2,)), dma((2,)), dma((3,)), dma((3,)), dma((2, peers)), dma((2, peers)),
            dma((3,)), dma((3,)), dma((2, peers)), dma((2, peers)),
        ],
        compiler_params=pltpu.CompilerParams(collective_id=0, has_side_effects=True),
        name="field",
    )(seam, order, x, w_in, w_mid, w_feat, w_dens, w_conv, w_color)


def body(samples_in, block_order, seam_link, w_in, w_mid, w_feat, w_density, w_conv, w_color):
    n_block, n_patch = lax.axis_size("block"), lax.axis_size("patch")
    x = samples_in.reshape(2, RAYS // 128, 128, SAMP * ENC)
    return render(
        block_order, seam_link, x, w_in, w_mid, jnp.swapaxes(w_feat, 1, 2), w_density, w_conv, w_color, n_block, n_patch
    )


def solution(mesh):
    return jax.shard_map(
        body,
        mesh=mesh,
        in_specs=(
            P("block", None, "patch", None),
            P("patch", None),
            P("patch"),
            P("block", None, None),
            P("block", None, None, None),
            P("block", None, None),
            P("block", None),
            P(),
            P(),
        ),
        out_specs=P(None, "block", "patch"),
        check_vma=False,
    )
```

```python
import functools

import jax
import jax.numpy as jnp
from jax import lax
from jax.experimental import pallas as pl
from jax.experimental.pallas import tpu as pltpu
from jax.sharding import PartitionSpec as P

f32, bf16 = jnp.float32, jnp.bfloat16
MESH = pl.DeviceIdType.MESH

ENC = 32
SAMP = 4
STEP = 0.03
FEAT = 64
WIDTH = 256
COLS = 64
RAYS = 2048
PITCH = 68
SPAN = 512
ROLL = bf16


def iota(shape, dim):
    return lax.broadcasted_iota(jnp.int32, shape, dim)


def relu(x):
    return jnp.maximum(x, 0.0)


def dot(a, b):
    return jnp.dot(a, b, preferred_element_type=f32)


def dot_nt(a, b):
    return lax.dot_general(a, b, (((1,), (1,)), ((), ())), preferred_element_type=f32)


def field_chunks(streams):
    count = len(streams)
    hs = [relu(dot_nt(w1, x)).astype(bf16) for x, w1, w2, w3, head in streams]
    hs = [jnp.concatenate([h[WIDTH * s : WIDTH * (s + 1)] for s in range(SAMP)], axis=1) for h in hs]
    hs = [relu(dot(streams[i][2], hs[i])).astype(bf16) for i in range(count)]
    hs = [relu(dot(streams[i][3], hs[i])).astype(bf16) for i in range(count)]
    outs = [dot(streams[i][4], hs[i]) for i in range(count)]
    results = []
    for out in outs:
        rays = out.shape[1] // SAMP
        raw = out[FEAT : FEAT + 1]
        optical = STEP * (jnp.maximum(raw, 0.0) + jnp.log(1.0 + jnp.exp(-jnp.abs(raw))))
        total = jnp.zeros((1, rays), f32)
        colour = jnp.zeros((FEAT, rays), f32)
        for s in range(SAMP):
            here = optical[:, s * rays : (s + 1) * rays]
            weight = jnp.exp(-total) * (1.0 - jnp.exp(-here))
            total = total + here
            colour = colour + weight * out[:FEAT, s * rays : (s + 1) * rays]
        results.append((total, colour))
    return results


def phase_source(phase, tap):
    return (phase + tap - 1) // 2


def put(ref, row, col, value):
    ref[row : row + value.shape[0], col : col + value.shape[1]] = value


def enlarge_weights(ref, w_conv, layer):
    taps = [[w_conv[layer, a, e].astype(f32) for e in range(3)] for a in range(3)]
    for pa in range(2):
        for pb in range(2):
            for dr in range(-1, 2):
                for dc in range(-1, 2):
                    hits = [taps[a][e] for a in range(3) for e in range(3)
                            if phase_source(pa, a) == dr and phase_source(pb, e) == dc]
                    value = sum(hits[1:], hits[0]) if hits else jnp.zeros((FEAT, FEAT), f32)
                    put(ref, (2 * pa + pb) * FEAT, ((dr + 1) * 3 + dc + 1) * FEAT, value.astype(bf16))


def dense_weights(ref, w_conv, layer):
    for qa in range(2):
        for qb in range(2):
            for s in range(-1, 3):
                for t in range(-1, 3):
                    a, e = s - qa + 1, t - qb + 1
                    inside = 0 <= a <= 2 and 0 <= e <= 2
                    value = w_conv[layer, a, e] if inside else jnp.zeros((FEAT, FEAT), bf16)
                    put(ref, (2 * qa + qb) * FEAT, ((s + 1) * 4 + t + 1) * FEAT, value)


def colour_weights(ref, w_conv, w_color, layer):
    ref[...] = jnp.zeros_like(ref)
    for a in range(3):
        for e in range(3):
            tint = dot(w_color[...], w_conv[layer, a, e])
            for i in range(4):
                for j in range(4):
                    group = (i - a + 2) * 6 + (j - e + 2)
                    cell = ((i // 2 * 2 + j // 2) * 2 + i % 2) * 2 + j % 2
                    put(ref, 8 * group, cell * FEAT, tint)


def moved(x, by):
    return pltpu.roll(x, (-by) % x.shape[1], 1) if by else x


def prepare(w_conv, w_color, k0, k1, k2, k3, k4, place, halo_place, weave):
    enlarge_weights(k0, w_conv, 0)
    dense_weights(k1, w_conv, 1)
    enlarge_weights(k2, w_conv, 2)
    colour_weights(k3, w_conv, w_color, 3)
    k4[...] = k3[...].astype(bf16)
    source = iota(place.shape, 0)
    place[...] = (iota(place.shape, 1) == source // COLS * PITCH + source % COLS + 2).astype(f32).astype(bf16)
    source = iota(halo_place.shape, 0)
    target = source // 4 * PITCH + source % 2 + source // 2 % 2 * (COLS + 2)
    halo_place[...] = (iota(halo_place.shape, 1) == target).astype(f32).astype(bf16)
    source = iota(weave.shape, 0)
    target = jnp.where(source % 128 < COLS, 4 * (source % 128) + source // 128, -1)
    weave[...] = (iota(weave.shape, 1) == target).astype(f32).astype(bf16)


def decode(n_block, n_patch, seam, window, halo, link, out, k0, k1, k2, k4, place, halo_place, weave, res):
    me = lax.axis_index("block")
    column = lax.axis_index("patch")
    right_open = jnp.where(column < n_patch - 1, seam[0], 0).astype(f32)
    left_open = link[0:1, 0:1].astype(f32)

    def open_sides(lanes):
        at = iota((1, lanes), 1) % PITCH
        return jnp.where(at < 2, left_open, jnp.where(at < COLS + 2, 1.0, right_open))

    line = iota((1, SPAN), 1) // PITCH
    top = jnp.where(me > 0, 1.0, 0.0)
    bottom = jnp.where(me < n_block - 1, 1.0, 0.0)
    mask = jnp.where(line == 0, top, jnp.where(line < 5, 1.0, jnp.where(line == 5, bottom, 0.0))) * open_sides(SPAN)

    image = dot(jnp.concatenate([window[t] for t in range(4)], axis=1), place[...])
    image = image + dot(halo[...].astype(f32).T[:FEAT].astype(bf16), halo_place[...])
    image = (image * open_sides(image.shape[1])).astype(ROLL)
    patches = [
        moved(image, (dr + 1) * PITCH + dc)[:, :SPAN].astype(bf16) for dr in range(-1, 2) for dc in range(-1, 2)
    ]
    first = (relu(dot(k0[...], jnp.concatenate(patches, axis=0))) * mask).astype(ROLL)

    def views(maps):
        found = {}
        for s in range(-1, 3):
            for t in range(-1, 3):
                phase = (s % 2 * 2 + t % 2) * FEAT
                found[s, t] = moved(maps[phase : phase + FEAT], s // 2 * PITCH + t // 2).astype(bf16)
        return found

    cells = views(first)
    second = relu(dot(k1[...], jnp.concatenate([cells[s, t] for s in range(-1, 3) for t in range(-1, 3)], axis=0)))
    cells = views((second * mask).astype(ROLL))
    parts = []
    for qa in range(2):
        for qb in range(2):
            near = [cells[s, t] for s in range(qa - 1, qa + 2) for t in range(qb - 1, qb + 2)]
            parts.append((relu(dot(k2[...], jnp.concatenate(near, axis=0))) * mask).astype(bf16))
    spread = dot(k4[...], jnp.concatenate(parts, axis=0))

    def cell(i, j):
        group = (i + 1) * 6 + j + 1
        return spread[8 * group : 8 * group + 8]

    def row(i, j):
        value = cell(i, j)
        if i == 0:
            value = value + moved(cell(4, j), -PITCH)
        if i == 3:
            value = value + moved(cell(-1, j), PITCH)
        return value

    stack = []
    for i in range(4):
        cols = [row(i, j) for j in range(-1, 5)]
        middle = cols[1:5]
        middle[0] = middle[0] + moved(cols[5], -1)
        middle[3] = middle[3] + moved(cols[0], 1)
        stack.append(jnp.concatenate(middle, axis=0))
    stack = jnp.concatenate(stack, axis=0)
    starts = [(r + 1) * PITCH + 2 for r in range(4)]
    lines = [moved(stack[:, a // 128 * 128 : a // 128 * 128 + 256], a % 128)[:, :128] for a in starts[:3]]
    lines.append(moved(stack, starts[3])[:, :128])
    wide = jnp.concatenate(
        [
            jnp.concatenate([lines[r][8 * (4 * i + j) : 8 * (4 * i + j) + 8] for j in range(4)], axis=1)
            for r in range(4) for i in range(4)
        ],
        axis=0,
    )
    high = wide.astype(bf16)
    low = (wide - high.astype(f32)).astype(bf16)
    woven = dot(high, weave[...]) + dot(low, weave[...])
    for half in range(2):
        lanes = slice(128 * half, 128 * (half + 1))
        res[half] = woven[:, lanes]
        for k in range(3):
            out[k, :, lanes] = res[half, pl.ds(k, 16, stride=8), :]


def last_tile(device):
    return ((device + 1) // 2 + 3) % 4


def field_kernel(
    n_block, n_patch, seam, order_far, x_far, w_in_far, w_mid_far, w_feat_far, w_dens_far, w_conv_far, w_color_far, out,
    order, x, w_in, w_mid, w_feat, w_dens, w_conv, w_color, fetched,
    window_out, halo_out, k0, k1, k2, k3, k4, place_rows, place_halo, weave, res,
    spread, w1, w2, w3, head, rays_out, rays_in, meta, meta_in, depth_rows, tiles, tiles_in, last_in, passed, passed_in,
    halo, halo_in, halo_depth, halo_depth_in, lines16, shares,
    rays_send, rays_recv, meta_send, meta_recv, tile_send, tile_recv, last_send, last_recv, pass_send, pass_recv,
    halo_send, halo_recv,
):
    me = lax.axis_index("block")
    place = lax.axis_index("patch")
    sides = ((place - 1, place > 0), (place + 1, place < n_patch - 1))
    pairs = (
        (w_in_far, w_in), (w_mid_far, w_mid), (w_feat_far, w_feat), (w_dens_far, w_dens), (x_far, x), (order_far, order),
        (w_conv_far, w_conv), (w_color_far, w_color),
    )
    fetches = [pltpu.make_async_copy(far, near, fetched.at[i]) for i, (far, near) in enumerate(pairs)]
    for fetch in fetches:
        fetch.start()
    rays_in[...] = jnp.zeros_like(rays_in)
    meta_in[...] = jnp.zeros_like(meta_in)
    barrier = pltpu.get_barrier_semaphore()
    for k in range(1, n_block):
        pl.semaphore_signal(barrier, inc=1, device_id=((me + k) % n_block, place), device_id_type=MESH)
    for side, there in sides:

        @pl.when(there)
        def _():
            pl.semaphore_signal(barrier, inc=1, device_id=(me, side), device_id_type=MESH)

    spread[...] = jnp.zeros_like(spread)
    for fetch in fetches[:4]:
        fetch.wait()
    for m in range(2):
        for s in range(SAMP):
            spread[ENC * s : ENC * (s + 1), WIDTH * s : WIDTH * (s + 1)] = w_in[m]
        w1[m] = spread[...].T
        w2[m] = w_mid[m, 0].T
        w3[m] = w_mid[m, 1].T
        head[m, :FEAT] = w_feat[m]
        head[m, FEAT:] = jnp.broadcast_to(w_dens[pl.ds(m, 1), :], (16, WIDTH))
    for fetch in fetches[4:6]:
        fetch.wait()
    line = iota((16, 256), 0)
    wanted = line % 8 // 2 * COLS + line % 2 + jnp.where(line >= 8, COLS - 2, 0)
    pick = (iota((16, 256), 1) == wanted).astype(f32).astype(bf16)
    for m in range(2):
        found = [dot(pick, x[m, 2 * g : 2 * g + 2].reshape(256, 128)) for g in range(8)]
        for side in range(2):
            rows = jnp.concatenate([f[8 * side : 8 * side + 8] for f in found], axis=0)
            rays_out[side, m] = rows.astype(bf16)
    slot = iota((16, 128), 0)
    member = 2 * ((me + n_block - slot // 2) % n_block) + slot % 2
    rank = jnp.zeros((16, 128), jnp.int32)
    for k in range(16):
        rank = jnp.where(member == order[0, k], k, rank)
    meta[:16] = rank
    meta[16:] = jnp.full((8, 128), jnp.where(place < n_patch - 1, seam[0], 0), jnp.int32)

    depth_rows[...] = jnp.zeros_like(depth_rows)

    def side_copies(side):
        target = (me, sides[side][0])
        return [
            pltpu.make_async_remote_copy(
                src_ref=rays_out.at[side], dst_ref=rays_in.at[1 - side], send_sem=rays_send.at[side],
                recv_sem=rays_recv.at[1 - side], device_id=target, device_id_type=MESH,
            ),
            pltpu.make_async_remote_copy(
                src_ref=meta, dst_ref=meta_in.at[1 - side], send_sem=meta_send.at[side],
                recv_sem=meta_recv.at[1 - side], device_id=target, device_id_type=MESH,
            ),
        ]

    count = (place > 0).astype(jnp.int32) + (place < n_patch - 1).astype(jnp.int32)
    pl.semaphore_wait(barrier, n_block - 1 + count)
    for side in range(2):
        for copy in side_copies(side):
            pl.when(sides[side][1])(copy.start)

    def weights(m):
        return w1[m], w2[m], w3[m], head[m]

    def depth_block(m, total):
        lanes = slice(0, total.shape[1])
        high = total.astype(bf16).astype(f32)
        depth_rows[m : m + 1, lanes] = high
        depth_rows[2 + m : 3 + m, lanes] = total - high

    def rays_of(unit, m):
        return jnp.concatenate([x[m, 4 * j + unit] for j in range(4)], axis=0)

    def keep(unit, m, tint):
        tint = tint.astype(bf16)
        for j in range(4):
            tiles[unit, j, FEAT * m : FEAT * (m + 1)] = tint[:, 128 * j : 128 * (j + 1)]

    def keep_depth(unit):
        rows = depth_rows[...].astype(bf16)
        for j in range(4):
            tiles[unit, j, 2 * FEAT :] = rows[:, 128 * j : 128 * (j + 1)]

    def store(unit, results):
        for m, (total, tint) in enumerate(results):
            keep(unit, m, tint)
            depth_block(m, total)
        keep_depth(unit)

    def send_owner(unit):
        for j in range(4):
            owner = 2 * j + unit // 2

            @pl.when(owner != me)
            def _():
                pltpu.make_async_remote_copy(
                    src_ref=tiles.at[unit, j], dst_ref=tiles_in.at[unit, (owner + n_block - me) % n_block - 1],
                    send_sem=tile_send.at[unit], recv_sem=tile_recv.at[unit],
                    device_id=(owner, place), device_id_type=MESH,
                ).start()

    def loop(unit, carry):
        store(unit, field_chunks([(rays_of(unit, m), *weights(m)) for m in range(2)]))
        send_owner(unit)
        return carry

    lax.fori_loop(0, 3, loop, 0)

    for side in range(2):
        for copy in side_copies(side):
            pl.when(sides[1 - side][1])(copy.wait_recv)
    results = field_chunks(
        [(jnp.concatenate([rays_in[0, m], rays_in[1, m]], axis=0), *weights(m)) for m in range(2)]
        + [(rays_of(3, 0), *weights(0))]
    )
    ((last_total, last_tint),) = results[2:]
    results = results[:2]
    for m, (total, tint) in enumerate(results):
        depth_block(m, total)
    halo_depth[...] = depth_rows[:, :128].astype(bf16)
    ray = iota((144, 128), 0) - 8
    source = jnp.where((ray >= 0) & (ray < 128), ray // 2 % 2 * 64 + ray // 4 * 2 + ray % 2, -1)
    turn = (iota((144, 128), 1) == source).astype(f32).astype(bf16)
    both = jnp.concatenate([tint for total, tint in results], axis=0).astype(bf16)
    halo[...] = dot_nt(turn, both).astype(bf16)

    def halo_copies(k):
        peer = (me + k) % n_block
        return [
            pltpu.make_async_remote_copy(
                src_ref=halo.at[pl.ds(pl.multiple_of(16 * peer, 16), 32)], dst_ref=halo_in.at[k - 1],
                send_sem=halo_send.at[0, k - 1], recv_sem=halo_recv.at[0, k - 1],
                device_id=(peer, place), device_id_type=MESH,
            ),
            pltpu.make_async_remote_copy(
                src_ref=halo_depth, dst_ref=halo_depth_in.at[k - 1],
                send_sem=halo_send.at[1, k - 1], recv_sem=halo_recv.at[1, k - 1],
                device_id=(peer, place), device_id_type=MESH,
            ),
        ]

    for k in range(1, n_block):
        for copy in halo_copies(k):
            copy.start()

    def last_copy(k, m):
        peer = (me + k) % n_block
        rows = pl.ds(0, FEAT) if m == 0 else pl.ds(FEAT, FEAT + 8)
        return pltpu.make_async_remote_copy(
            src_ref=tiles.at[3, last_tile(peer), rows], dst_ref=last_in.at[k - 1, rows],
            send_sem=last_send.at[m, k - 1], recv_sem=last_recv.at[m, k - 1],
            device_id=(peer, place), device_id_type=MESH,
        )

    for m in range(2):
        total, tint = (last_total, last_tint) if m == 0 else field_chunks([(rays_of(3, 1), *weights(1))])[0]
        keep(3, m, tint)
        depth_block(m, total)
        if m == 1:
            keep_depth(3)
        for k in range(1, n_block):
            last_copy(k, m).start()

    def order_weights(blocks, ranks):
        for k, block in enumerate(blocks):
            block = block.astype(f32)
            lines16[2 * k : 2 * k + 2] = block[0:2] + block[2:4]
        depths = lines16[...]
        prefixes = [
            jnp.sum(jnp.where(ranks < ranks[i : i + 1], depths, 0.0), axis=0, keepdims=True) for i in range(16)
        ]
        return [jnp.exp(-prefix) for prefix in prefixes]

    def combine(own, got):
        slots = [own] + [got.at[k - 1] for k in range(1, n_block)]
        factors = order_weights([slot[2 * FEAT :] for slot in slots], meta[:16])
        mixed = jnp.zeros((FEAT, 128), f32)
        for i in range(16):
            tint = slots[i // 2][i % 2 * FEAT : (i % 2 + 1) * FEAT]
            mixed = mixed + factors[i] * tint.astype(f32)
        return mixed

    def pass_copy(unit):
        target = me - 1 if unit % 2 == 0 else me + 1
        return pltpu.make_async_remote_copy(
            src_ref=passed.at[unit], dst_ref=passed_in.at[unit], send_sem=pass_send.at[unit],
            recv_sem=pass_recv.at[unit], device_id=(target, place), device_id_type=MESH,
        )

    def mine(unit):
        return me % 2 == unit // 2

    def has_target(unit):
        return mine(unit) & ((me > 0) if unit % 2 == 0 else (me < n_block - 1))

    def has_source(unit):
        return (me % 2 != unit // 2) & ((me < n_block - 1) if unit % 2 == 0 else (me > 0))

    for unit in range(3):

        @pl.when(mine(unit))
        def _():
            pltpu.make_async_copy(tiles_in.at[unit], tiles_in.at[unit], tile_recv.at[unit]).wait()
            passed[unit] = combine(tiles.at[unit, me // 2], tiles_in.at[unit]).astype(bf16)

        pl.when(has_target(unit))(pass_copy(unit).start)

        @pl.when(mine(unit))
        def _():
            window_out[1 + unit % 2] = passed[unit]

    for fetch in fetches[6:]:
        fetch.wait()
    prepare(w_conv, w_color, k0, k1, k2, k3, k4, place_rows, place_halo, weave)

    for k in range(1, n_block):
        for copy in halo_copies(k):
            copy.wait_recv()
    ranks = jnp.where(iota((16, 128), 1) < 64, meta_in[0, :16], meta_in[1, :16])
    factors = order_weights([halo_depth[...]] + [halo_depth_in[k - 1] for k in range(1, n_block)], ranks)
    for i in range(16):
        shares[i : i + 1] = factors[i]
    line = iota((32, 128), 0)
    row = line // 4 + 4 * me - 2
    source = jnp.where((row >= 0) & (row < 32), line // 2 % 2 * 64 + row * 2 + line % 2, -1)
    turn = (iota((32, 128), 1) == source).astype(f32).astype(bf16)
    high = shares[...].astype(bf16)
    low = (shares[...] - high.astype(f32)).astype(bf16)
    share = dot_nt(turn, high) + dot_nt(turn, low)
    mixed = jnp.zeros((32, 128), f32)
    for k in range(n_block):
        tint = halo[pl.ds(pl.multiple_of(16 * me, 16), 32), :] if k == 0 else halo_in[k - 1]
        factor = jnp.where(iota((32, 128), 1) < 64, share[:, 2 * k : 2 * k + 1], share[:, 2 * k + 1 : 2 * k + 2])
        mixed = mixed + factor * tint.astype(f32)
    halo_out[...] = (mixed + pltpu.roll(mixed, 64, 1)).astype(bf16)

    for unit in range(3):

        @pl.when(has_source(unit))
        def _():
            pass_copy(unit).wait_recv()
            window_out[3 - unit % 2 * 3] = passed_in[unit]

    @pl.when(me == n_block - 1)
    def _():
        window_out[3] = jnp.zeros((FEAT, 128), bf16)

    for m in range(2):
        for k in range(1, n_block):
            last_copy(k, m).wait_recv()
    mixed = combine(tiles.at[3, last_tile(me)], last_in)
    window_out[me % 2 * 2] = (mixed * jnp.where(me > 0, 1.0, 0.0)).astype(bf16)
    decode(
        n_block, n_patch, seam, window_out, halo_out, meta_in.at[0, pl.ds(16, 8)], out, k0, k1, k2, k4,
        place_rows, place_halo, weave, res,
    )

    for side in range(2):
        for copy in side_copies(side):
            pl.when(sides[side][1])(copy.wait_send)
    for k in range(1, n_block):
        for copy in halo_copies(k) + [last_copy(k, 0), last_copy(k, 1)]:
            copy.wait_send()
    for unit in range(3):
        pl.when(has_target(unit))(pass_copy(unit).wait_send)
        sent = pltpu.make_async_copy(tiles_in.at[unit, pl.ds(0, 3)], tiles_in.at[unit, pl.ds(0, 3)], tile_send.at[unit])
        more = pltpu.make_async_copy(tiles_in.at[unit, 3], tiles_in.at[unit, 3], tile_send.at[unit])
        sent.wait()
        pl.when(me % 2 != unit // 2)(more.wait)


def render(order, seam, x, w_in, w_mid, w_feat, w_dens, w_conv, w_color, n_block, n_patch):
    vmem = pl.BlockSpec(memory_space=pltpu.VMEM)
    smem = pl.BlockSpec(memory_space=pltpu.SMEM)
    dma = pltpu.SemaphoreType.DMA
    peers = n_block - 1
    rows = 2 * FEAT + 8
    return pl.pallas_call(
        functools.partial(field_kernel, n_block, n_patch),
        out_shape=jax.ShapeDtypeStruct((3, 16, 256), f32),
        in_specs=[smem] + [pl.BlockSpec(memory_space=pl.ANY)] * 8,
        out_specs=vmem,
        scratch_shapes=[
            pltpu.SMEM(order.shape, jnp.int32),
            *[pltpu.VMEM(array.shape, bf16) for array in (x, w_in, w_mid, w_feat, w_dens, w_conv, w_color)],
            dma((8,)),
            pltpu.VMEM((4, FEAT, 128), bf16),
            pltpu.VMEM((32, 128), bf16),
            pltpu.VMEM((256, 576), bf16),
            pltpu.VMEM((256, 1024), bf16),
            pltpu.VMEM((256, 576), bf16),
            pltpu.VMEM((288, 1024), f32),
            pltpu.VMEM((288, 1024), bf16),
            pltpu.VMEM((512, 640), bf16),
            pltpu.VMEM((32, 640), bf16),
            pltpu.VMEM((512, 256), bf16),
            pltpu.VMEM((2, 128, 128), f32),
            pltpu.VMEM((128, 1024), bf16),
            pltpu.VMEM((2, 1024, 128), bf16),
            pltpu.VMEM((2, WIDTH, WIDTH), bf16),
            pltpu.VMEM((2, WIDTH, WIDTH), bf16),
            pltpu.VMEM((2, FEAT + 16, WIDTH), bf16),
            pltpu.VMEM((2, 2, 64, 128), bf16),
            pltpu.VMEM((2, 2, 64, 128), bf16),
            pltpu.VMEM((24, 128), jnp.int32),
            pltpu.VMEM((2, 24, 128), jnp.int32),
            pltpu.VMEM((8, 512), f32),
            pltpu.VMEM((4, 4, rows, 128), bf16),
            pltpu.VMEM((3, peers, rows, 128), bf16),
            pltpu.VMEM((peers, rows, 128), bf16),
            pltpu.VMEM((3, FEAT, 128), bf16),
            pltpu.VMEM((3, FEAT, 128), bf16),
            pltpu.VMEM((144, 128), bf16),
            pltpu.VMEM((peers, 32, 128), bf16),
            pltpu.VMEM((8, 128), bf16),
            pltpu.VMEM((peers, 8, 128), bf16),
            pltpu.VMEM((16, 128), f32),
            pltpu.VMEM((16, 128), f32),
            dma((2,)), dma((2,)), dma((2,)), dma((2,)), dma((3,)), dma((3,)), dma((2, peers)), dma((2, peers)),
            dma((3,)), dma((3,)), dma((2, peers)), dma((2, peers)),
        ],
        compiler_params=pltpu.CompilerParams(collective_id=0, has_side_effects=True),
        name="field",
    )(seam, order, x, w_in, w_mid, w_feat, w_dens, w_conv, w_color)


def body(samples_in, block_order, seam_link, w_in, w_mid, w_feat, w_density, w_conv, w_color):
    n_block, n_patch = lax.axis_size("block"), lax.axis_size("patch")
    x = samples_in.reshape(2, RAYS // 128, 128, SAMP * ENC)
    return render(
        block_order, seam_link, x, w_in, w_mid, jnp.swapaxes(w_feat, 1, 2), w_density, w_conv, w_color, n_block, n_patch
    )


def solution(mesh):
    return jax.shard_map(
        body,
        mesh=mesh,
        in_specs=(
            P("block", None, "patch", None),
            P("patch", None),
            P("patch"),
            P("block", None, None),
            P("block", None, None, None),
            P("block", None, None),
            P("block", None),
            P(),
            P(),
        ),
        out_specs=P(None, "block", "patch"),
        check_vma=False,
    )
```

```python
import functools

import jax
import jax.numpy as jnp
from jax import lax
from jax.experimental import pallas as pl
from jax.experimental.pallas import tpu as pltpu
from jax.sharding import PartitionSpec as P

f32, bf16 = jnp.float32, jnp.bfloat16
MESH = pl.DeviceIdType.MESH

ENC = 32
SAMP = 4
STEP = 0.03
FEAT = 64
WIDTH = 256
COLS = 64
RAYS = 2048
PITCH = 68
SPAN = 512
ROLL = bf16


def iota(shape, dim):
    return lax.broadcasted_iota(jnp.int32, shape, dim)


def relu(x):
    return jnp.maximum(x, 0.0)


def dot(a, b):
    return jnp.dot(a, b, preferred_element_type=f32)


def dot_nt(a, b):
    return lax.dot_general(a, b, (((1,), (1,)), ((), ())), preferred_element_type=f32)


def field_chunks(streams):
    count = len(streams)
    hs = [relu(dot_nt(w1, x)).astype(bf16) for x, w1, w2, w3, head in streams]
    hs = [jnp.concatenate([h[WIDTH * s : WIDTH * (s + 1)] for s in range(SAMP)], axis=1) for h in hs]
    hs = [relu(dot(streams[i][2], hs[i])).astype(bf16) for i in range(count)]
    hs = [relu(dot(streams[i][3], hs[i])).astype(bf16) for i in range(count)]
    outs = [dot(streams[i][4], hs[i]) for i in range(count)]
    results = []
    for out in outs:
        rays = out.shape[1] // SAMP
        raw = out[FEAT : FEAT + 1]
        optical = STEP * (jnp.maximum(raw, 0.0) + jnp.log(1.0 + jnp.exp(-jnp.abs(raw))))
        total = jnp.zeros((1, rays), f32)
        colour = jnp.zeros((FEAT, rays), f32)
        for s in range(SAMP):
            here = optical[:, s * rays : (s + 1) * rays]
            weight = jnp.exp(-total) * (1.0 - jnp.exp(-here))
            total = total + here
            colour = colour + weight * out[:FEAT, s * rays : (s + 1) * rays]
        results.append((total, colour))
    return results


def phase_source(phase, tap):
    return (phase + tap - 1) // 2


def put(ref, row, col, value):
    ref[row : row + value.shape[0], col : col + value.shape[1]] = value


def enlarge_weights(ref, w_conv, layer):
    taps = [[w_conv[layer, a, e].astype(f32) for e in range(3)] for a in range(3)]
    for pa in range(2):
        for pb in range(2):
            for dr in range(-1, 2):
                for dc in range(-1, 2):
                    hits = [taps[a][e] for a in range(3) for e in range(3)
                            if phase_source(pa, a) == dr and phase_source(pb, e) == dc]
                    value = sum(hits[1:], hits[0]) if hits else jnp.zeros((FEAT, FEAT), f32)
                    put(ref, (2 * pa + pb) * FEAT, ((dr + 1) * 3 + dc + 1) * FEAT, value.astype(bf16))


def dense_weights(ref, w_conv, layer):
    for qa in range(2):
        for qb in range(2):
            for s in range(-1, 3):
                for t in range(-1, 3):
                    a, e = s - qa + 1, t - qb + 1
                    inside = 0 <= a <= 2 and 0 <= e <= 2
                    value = w_conv[layer, a, e] if inside else jnp.zeros((FEAT, FEAT), bf16)
                    put(ref, (2 * qa + qb) * FEAT, ((s + 1) * 4 + t + 1) * FEAT, value)


def colour_weights(ref, w_conv, w_color, layer):
    ref[...] = jnp.zeros_like(ref)
    for a in range(3):
        for e in range(3):
            tint = dot(w_color[...], w_conv[layer, a, e])
            for i in range(4):
                for j in range(4):
                    group = (i - a + 2) * 6 + (j - e + 2)
                    cell = ((i // 2 * 2 + j // 2) * 2 + i % 2) * 2 + j % 2
                    put(ref, 8 * group, cell * FEAT, tint)


def moved(x, by):
    return pltpu.roll(x, (-by) % x.shape[1], 1) if by else x


def prepare(w_conv, w_color, k0, k1, k2, k3, k4, place, halo_place, weave):
    enlarge_weights(k0, w_conv, 0)
    dense_weights(k1, w_conv, 1)
    enlarge_weights(k2, w_conv, 2)
    colour_weights(k3, w_conv, w_color, 3)
    k4[...] = k3[...].astype(bf16)
    source = iota(place.shape, 0)
    place[...] = (iota(place.shape, 1) == source // COLS * PITCH + source % COLS + 2).astype(f32).astype(bf16)
    source = iota(halo_place.shape, 0)
    target = source // 4 * PITCH + source % 2 + source // 2 % 2 * (COLS + 2)
    halo_place[...] = (iota(halo_place.shape, 1) == target).astype(f32).astype(bf16)
    source = iota(weave.shape, 0)
    target = jnp.where(source % 128 < COLS, 4 * (source % 128) + source // 128, -1)
    weave[...] = (iota(weave.shape, 1) == target).astype(f32).astype(bf16)


def decode(n_block, n_patch, seam, window, halo, link, out, k0, k1, k2, k4, place, halo_place, weave, res):
    me = lax.axis_index("block")
    column = lax.axis_index("patch")
    right_open = jnp.where(column < n_patch - 1, seam[0], 0).astype(f32)
    left_open = link[0:1, 0:1].astype(f32)

    def open_sides(lanes):
        at = iota((1, lanes), 1) % PITCH
        return jnp.where(at < 2, left_open, jnp.where(at < COLS + 2, 1.0, right_open))

    line = iota((1, SPAN), 1) // PITCH
    top = jnp.where(me > 0, 1.0, 0.0)
    bottom = jnp.where(me < n_block - 1, 1.0, 0.0)
    mask = jnp.where(line == 0, top, jnp.where(line < 5, 1.0, jnp.where(line == 5, bottom, 0.0))) * open_sides(SPAN)

    image = dot(jnp.concatenate([window[t] for t in range(4)], axis=1), place[...])
    image = image + dot(halo[...].astype(f32).T[:FEAT].astype(bf16), halo_place[...])
    image = (image * open_sides(image.shape[1])).astype(ROLL)
    patches = [
        moved(image, (dr + 1) * PITCH + dc)[:, :SPAN].astype(bf16) for dr in range(-1, 2) for dc in range(-1, 2)
    ]
    first = (relu(dot(k0[...], jnp.concatenate(patches, axis=0))) * mask).astype(ROLL)

    def views(maps):
        found = {}
        for s in range(-1, 3):
            for t in range(-1, 3):
                phase = (s % 2 * 2 + t % 2) * FEAT
                found[s, t] = moved(maps[phase : phase + FEAT], s // 2 * PITCH + t // 2).astype(bf16)
        return found

    cells = views(first)
    second = relu(dot(k1[...], jnp.concatenate([cells[s, t] for s in range(-1, 3) for t in range(-1, 3)], axis=0)))
    cells = views((second * mask).astype(ROLL))
    parts = []
    for qa in range(2):
        for qb in range(2):
            near = [cells[s, t] for s in range(qa - 1, qa + 2) for t in range(qb - 1, qb + 2)]
            parts.append((relu(dot(k2[...], jnp.concatenate(near, axis=0))) * mask).astype(bf16))
    spread = dot(k4[...], jnp.concatenate(parts, axis=0))

    def cell(i, j):
        group = (i + 1) * 6 + j + 1
        return spread[8 * group : 8 * group + 8]

    def row(i, j):
        value = cell(i, j)
        if i == 0:
            value = value + moved(cell(4, j), -PITCH)
        if i == 3:
            value = value + moved(cell(-1, j), PITCH)
        return value

    stack = []
    for i in range(4):
        cols = [row(i, j) for j in range(-1, 5)]
        middle = cols[1:5]
        middle[0] = middle[0] + moved(cols[5], -1)
        middle[3] = middle[3] + moved(cols[0], 1)
        stack.append(jnp.concatenate(middle, axis=0))
    stack = jnp.concatenate(stack, axis=0)
    starts = [(r + 1) * PITCH + 2 for r in range(4)]
    lines = [moved(stack[:, a // 128 * 128 : a // 128 * 128 + 256], a % 128)[:, :128] for a in starts[:3]]
    lines.append(moved(stack, starts[3])[:, :128])
    wide = jnp.concatenate(
        [
            jnp.concatenate([lines[r][8 * (4 * i + j) : 8 * (4 * i + j) + 8] for j in range(4)], axis=1)
            for r in range(4) for i in range(4)
        ],
        axis=0,
    )
    high = wide.astype(bf16)
    low = (wide - high.astype(f32)).astype(bf16)
    woven = dot(high, weave[...]) + dot(low, weave[...])
    for half in range(2):
        lanes = slice(128 * half, 128 * (half + 1))
        res[half] = woven[:, lanes]
        for k in range(3):
            out[k, :, lanes] = res[half, pl.ds(k, 16, stride=8), :]


def last_tile(device):
    return ((device + 1) // 2 + 3) % 4


def field_kernel(
    n_block, n_patch, seam, order_far, x_far, w_in_far, w_mid_far, w_feat_far, w_dens_far, w_conv_far, w_color_far, out,
    order, x, w_in, w_mid, w_feat, w_dens, w_conv, w_color, fetched,
    window_out, halo_out, k0, k1, k2, k3, k4, place_rows, place_halo, weave, res,
    spread, w1, w2, w3, head, rays_out, rays_in, meta, meta_in, depth_rows, tiles, tiles_in, last_in, passed, passed_in,
    halo, halo_in, halo_depth, halo_depth_in, lines16, shares,
    rays_send, rays_recv, meta_send, meta_recv, tile_send, tile_recv, last_send, last_recv, pass_send, pass_recv,
    halo_send, halo_recv,
):
    me = lax.axis_index("block")
    place = lax.axis_index("patch")
    far_first = sorted(range(1, n_block), key=lambda k: abs(k - n_block // 2))
    sides = ((place - 1, place > 0), (place + 1, place < n_patch - 1))
    pairs = (
        (w_in_far, w_in), (w_mid_far, w_mid), (w_feat_far, w_feat), (w_dens_far, w_dens), (x_far, x), (order_far, order),
        (w_conv_far, w_conv), (w_color_far, w_color),
    )
    fetches = [pltpu.make_async_copy(far, near, fetched.at[i]) for i, (far, near) in enumerate(pairs)]
    for fetch in fetches:
        fetch.start()
    rays_in[...] = jnp.zeros_like(rays_in)
    meta_in[...] = jnp.zeros_like(meta_in)
    barrier = pltpu.get_barrier_semaphore()
    for k in range(1, n_block):
        pl.semaphore_signal(barrier, inc=1, device_id=((me + k) % n_block, place), device_id_type=MESH)
    for side, there in sides:

        @pl.when(there)
        def _():
            pl.semaphore_signal(barrier, inc=1, device_id=(me, side), device_id_type=MESH)

    spread[...] = jnp.zeros_like(spread)
    for fetch in fetches[:4]:
        fetch.wait()
    for m in range(2):
        for s in range(SAMP):
            spread[ENC * s : ENC * (s + 1), WIDTH * s : WIDTH * (s + 1)] = w_in[m]
        w1[m] = spread[...].T
        w2[m] = w_mid[m, 0].T
        w3[m] = w_mid[m, 1].T
        head[m, :FEAT] = w_feat[m]
        head[m, FEAT:] = jnp.broadcast_to(w_dens[pl.ds(m, 1), :], (16, WIDTH))
    for fetch in fetches[4:6]:
        fetch.wait()
    line = iota((16, 256), 0)
    wanted = line % 8 // 2 * COLS + line % 2 + jnp.where(line >= 8, COLS - 2, 0)
    pick = (iota((16, 256), 1) == wanted).astype(f32).astype(bf16)
    for m in range(2):
        found = [dot(pick, x[m, 2 * g : 2 * g + 2].reshape(256, 128)) for g in range(8)]
        for side in range(2):
            rows = jnp.concatenate([f[8 * side : 8 * side + 8] for f in found], axis=0)
            rays_out[side, m] = rows.astype(bf16)
    slot = iota((16, 128), 0)
    member = 2 * ((me + n_block - slot // 2) % n_block) + slot % 2
    rank = jnp.zeros((16, 128), jnp.int32)
    for k in range(16):
        rank = jnp.where(member == order[0, k], k, rank)
    meta[:16] = rank
    meta[16:] = jnp.full((8, 128), jnp.where(place < n_patch - 1, seam[0], 0), jnp.int32)

    depth_rows[...] = jnp.zeros_like(depth_rows)

    def side_copies(side):
        target = (me, sides[side][0])
        return [
            pltpu.make_async_remote_copy(
                src_ref=rays_out.at[side], dst_ref=rays_in.at[1 - side], send_sem=rays_send.at[side],
                recv_sem=rays_recv.at[1 - side], device_id=target, device_id_type=MESH,
            ),
            pltpu.make_async_remote_copy(
                src_ref=meta, dst_ref=meta_in.at[1 - side], send_sem=meta_send.at[side],
                recv_sem=meta_recv.at[1 - side], device_id=target, device_id_type=MESH,
            ),
        ]

    count = (place > 0).astype(jnp.int32) + (place < n_patch - 1).astype(jnp.int32)
    pl.semaphore_wait(barrier, n_block - 1 + count)
    for side in range(2):
        for copy in side_copies(side):
            pl.when(sides[side][1])(copy.start)

    def weights(m):
        return w1[m], w2[m], w3[m], head[m]

    def depth_block(m, total):
        lanes = slice(0, total.shape[1])
        high = total.astype(bf16).astype(f32)
        depth_rows[m : m + 1, lanes] = high
        depth_rows[2 + m : 3 + m, lanes] = total - high

    def rays_of(unit, m):
        return jnp.concatenate([x[m, 4 * j + unit] for j in range(4)], axis=0)

    def keep(unit, m, tint):
        tint = tint.astype(bf16)
        for j in range(4):
            tiles[unit, j, FEAT * m : FEAT * (m + 1)] = tint[:, 128 * j : 128 * (j + 1)]

    def keep_depth(unit):
        rows = depth_rows[...].astype(bf16)
        for j in range(4):
            tiles[unit, j, 2 * FEAT :] = rows[:, 128 * j : 128 * (j + 1)]

    def store(unit, results):
        for m, (total, tint) in enumerate(results):
            keep(unit, m, tint)
            depth_block(m, total)
        keep_depth(unit)

    def send_owner(unit):
        for j in range(4):
            owner = 2 * j + unit // 2

            @pl.when(owner != me)
            def _():
                pltpu.make_async_remote_copy(
                    src_ref=tiles.at[unit, j], dst_ref=tiles_in.at[unit, (owner + n_block - me) % n_block - 1],
                    send_sem=tile_send.at[unit], recv_sem=tile_recv.at[unit],
                    device_id=(owner, place), device_id_type=MESH,
                ).start()

    def loop(unit, carry):
        store(unit, field_chunks([(rays_of(unit, m), *weights(m)) for m in range(2)]))
        send_owner(unit)
        return carry

    lax.fori_loop(0, 3, loop, 0)

    for side in range(2):
        for copy in side_copies(side):
            pl.when(sides[1 - side][1])(copy.wait_recv)
    results = field_chunks(
        [(jnp.concatenate([rays_in[0, m], rays_in[1, m]], axis=0), *weights(m)) for m in range(2)]
        + [(rays_of(3, 0), *weights(0))]
    )
    ((last_total, last_tint),) = results[2:]
    results = results[:2]
    for m, (total, tint) in enumerate(results):
        depth_block(m, total)
    halo_depth[...] = depth_rows[:, :128].astype(bf16)
    ray = iota((144, 128), 0) - 8
    source = jnp.where((ray >= 0) & (ray < 128), ray // 2 % 2 * 64 + ray // 4 * 2 + ray % 2, -1)
    turn = (iota((144, 128), 1) == source).astype(f32).astype(bf16)
    both = jnp.concatenate([tint for total, tint in results], axis=0).astype(bf16)
    halo[...] = dot_nt(turn, both).astype(bf16)

    def halo_copies(k):
        peer = (me + k) % n_block
        return [
            pltpu.make_async_remote_copy(
                src_ref=halo.at[pl.ds(pl.multiple_of(16 * peer, 16), 32)], dst_ref=halo_in.at[k - 1],
                send_sem=halo_send.at[0, k - 1], recv_sem=halo_recv.at[0, k - 1],
                device_id=(peer, place), device_id_type=MESH,
            ),
            pltpu.make_async_remote_copy(
                src_ref=halo_depth, dst_ref=halo_depth_in.at[k - 1],
                send_sem=halo_send.at[1, k - 1], recv_sem=halo_recv.at[1, k - 1],
                device_id=(peer, place), device_id_type=MESH,
            ),
        ]

    for k in far_first:
        for copy in halo_copies(k):
            copy.start()

    def last_copy(k, m):
        peer = (me + k) % n_block
        rows = pl.ds(0, FEAT) if m == 0 else pl.ds(FEAT, FEAT + 8)
        return pltpu.make_async_remote_copy(
            src_ref=tiles.at[3, last_tile(peer), rows], dst_ref=last_in.at[k - 1, rows],
            send_sem=last_send.at[m, k - 1], recv_sem=last_recv.at[m, k - 1],
            device_id=(peer, place), device_id_type=MESH,
        )

    for m in range(2):
        total, tint = (last_total, last_tint) if m == 0 else field_chunks([(rays_of(3, 1), *weights(1))])[0]
        keep(3, m, tint)
        depth_block(m, total)
        if m == 1:
            keep_depth(3)
        for k in far_first:
            last_copy(k, m).start()

    def order_weights(blocks, ranks):
        for k, block in enumerate(blocks):
            block = block.astype(f32)
            lines16[2 * k : 2 * k + 2] = block[0:2] + block[2:4]
        depths = lines16[...]
        prefixes = [
            jnp.sum(jnp.where(ranks < ranks[i : i + 1], depths, 0.0), axis=0, keepdims=True) for i in range(16)
        ]
        return [jnp.exp(-prefix) for prefix in prefixes]

    def combine(own, got):
        slots = [own] + [got.at[k - 1] for k in range(1, n_block)]
        factors = order_weights([slot[2 * FEAT :] for slot in slots], meta[:16])
        mixed = jnp.zeros((FEAT, 128), f32)
        for i in range(16):
            tint = slots[i // 2][i % 2 * FEAT : (i % 2 + 1) * FEAT]
            mixed = mixed + factors[i] * tint.astype(f32)
        return mixed

    def pass_copy(unit):
        target = me - 1 if unit % 2 == 0 else me + 1
        return pltpu.make_async_remote_copy(
            src_ref=passed.at[unit], dst_ref=passed_in.at[unit], send_sem=pass_send.at[unit],
            recv_sem=pass_recv.at[unit], device_id=(target, place), device_id_type=MESH,
        )

    def mine(unit):
        return me % 2 == unit // 2

    def has_target(unit):
        return mine(unit) & ((me > 0) if unit % 2 == 0 else (me < n_block - 1))

    def has_source(unit):
        return (me % 2 != unit // 2) & ((me < n_block - 1) if unit % 2 == 0 else (me > 0))

    for unit in range(3):

        @pl.when(mine(unit))
        def _():
            pltpu.make_async_copy(tiles_in.at[unit], tiles_in.at[unit], tile_recv.at[unit]).wait()
            passed[unit] = combine(tiles.at[unit, me // 2], tiles_in.at[unit]).astype(bf16)

        pl.when(has_target(unit))(pass_copy(unit).start)

        @pl.when(mine(unit))
        def _():
            window_out[1 + unit % 2] = passed[unit]

    for fetch in fetches[6:]:
        fetch.wait()
    prepare(w_conv, w_color, k0, k1, k2, k3, k4, place_rows, place_halo, weave)

    for k in range(1, n_block):
        for copy in halo_copies(k):
            copy.wait_recv()
    ranks = jnp.where(iota((16, 128), 1) < 64, meta_in[0, :16], meta_in[1, :16])
    factors = order_weights([halo_depth[...]] + [halo_depth_in[k - 1] for k in range(1, n_block)], ranks)
    for i in range(16):
        shares[i : i + 1] = factors[i]
    line = iota((32, 128), 0)
    row = line // 4 + 4 * me - 2
    source = jnp.where((row >= 0) & (row < 32), line // 2 % 2 * 64 + row * 2 + line % 2, -1)
    turn = (iota((32, 128), 1) == source).astype(f32).astype(bf16)
    high = shares[...].astype(bf16)
    low = (shares[...] - high.astype(f32)).astype(bf16)
    share = dot_nt(turn, high) + dot_nt(turn, low)
    mixed = jnp.zeros((32, 128), f32)
    for k in range(n_block):
        tint = halo[pl.ds(pl.multiple_of(16 * me, 16), 32), :] if k == 0 else halo_in[k - 1]
        factor = jnp.where(iota((32, 128), 1) < 64, share[:, 2 * k : 2 * k + 1], share[:, 2 * k + 1 : 2 * k + 2])
        mixed = mixed + factor * tint.astype(f32)
    halo_out[...] = (mixed + pltpu.roll(mixed, 64, 1)).astype(bf16)

    for unit in range(3):

        @pl.when(has_source(unit))
        def _():
            pass_copy(unit).wait_recv()
            window_out[3 - unit % 2 * 3] = passed_in[unit]

    @pl.when(me == n_block - 1)
    def _():
        window_out[3] = jnp.zeros((FEAT, 128), bf16)

    for m in range(2):
        for k in range(1, n_block):
            last_copy(k, m).wait_recv()
    mixed = combine(tiles.at[3, last_tile(me)], last_in)
    window_out[me % 2 * 2] = (mixed * jnp.where(me > 0, 1.0, 0.0)).astype(bf16)
    decode(
        n_block, n_patch, seam, window_out, halo_out, meta_in.at[0, pl.ds(16, 8)], out, k0, k1, k2, k4,
        place_rows, place_halo, weave, res,
    )

    for side in range(2):
        for copy in side_copies(side):
            pl.when(sides[side][1])(copy.wait_send)
    for k in range(1, n_block):
        for copy in halo_copies(k) + [last_copy(k, 0), last_copy(k, 1)]:
            copy.wait_send()
    for unit in range(3):
        pl.when(has_target(unit))(pass_copy(unit).wait_send)
        sent = pltpu.make_async_copy(tiles_in.at[unit, pl.ds(0, 3)], tiles_in.at[unit, pl.ds(0, 3)], tile_send.at[unit])
        more = pltpu.make_async_copy(tiles_in.at[unit, 3], tiles_in.at[unit, 3], tile_send.at[unit])
        sent.wait()
        pl.when(me % 2 != unit // 2)(more.wait)


def render(order, seam, x, w_in, w_mid, w_feat, w_dens, w_conv, w_color, n_block, n_patch):
    vmem = pl.BlockSpec(memory_space=pltpu.VMEM)
    smem = pl.BlockSpec(memory_space=pltpu.SMEM)
    dma = pltpu.SemaphoreType.DMA
    peers = n_block - 1
    rows = 2 * FEAT + 8
    return pl.pallas_call(
        functools.partial(field_kernel, n_block, n_patch),
        out_shape=pltpu.VMEM((3, 16, 256), f32),
        in_specs=[smem] + [pl.BlockSpec(memory_space=pl.ANY)] * 8,
        out_specs=vmem,
        scratch_shapes=[
            pltpu.SMEM(order.shape, jnp.int32),
            *[pltpu.VMEM(array.shape, bf16) for array in (x, w_in, w_mid, w_feat, w_dens, w_conv, w_color)],
            dma((8,)),
            pltpu.VMEM((4, FEAT, 128), bf16),
            pltpu.VMEM((32, 128), bf16),
            pltpu.VMEM((256, 576), bf16),
            pltpu.VMEM((256, 1024), bf16),
            pltpu.VMEM((256, 576), bf16),
            pltpu.VMEM((288, 1024), f32),
            pltpu.VMEM((288, 1024), bf16),
            pltpu.VMEM((512, 640), bf16),
            pltpu.VMEM((32, 640), bf16),
            pltpu.VMEM((512, 256), bf16),
            pltpu.VMEM((2, 128, 128), f32),
            pltpu.VMEM((128, 1024), bf16),
            pltpu.VMEM((2, 1024, 128), bf16),
            pltpu.VMEM((2, WIDTH, WIDTH), bf16),
            pltpu.VMEM((2, WIDTH, WIDTH), bf16),
            pltpu.VMEM((2, FEAT + 16, WIDTH), bf16),
            pltpu.VMEM((2, 2, 64, 128), bf16),
            pltpu.VMEM((2, 2, 64, 128), bf16),
            pltpu.VMEM((24, 128), jnp.int32),
            pltpu.VMEM((2, 24, 128), jnp.int32),
            pltpu.VMEM((8, 512), f32),
            pltpu.VMEM((4, 4, rows, 128), bf16),
            pltpu.VMEM((3, peers, rows, 128), bf16),
            pltpu.VMEM((peers, rows, 128), bf16),
            pltpu.VMEM((3, FEAT, 128), bf16),
            pltpu.VMEM((3, FEAT, 128), bf16),
            pltpu.VMEM((144, 128), bf16),
            pltpu.VMEM((peers, 32, 128), bf16),
            pltpu.VMEM((8, 128), bf16),
            pltpu.VMEM((peers, 8, 128), bf16),
            pltpu.VMEM((16, 128), f32),
            pltpu.VMEM((16, 128), f32),
            dma((2,)), dma((2,)), dma((2,)), dma((2,)), dma((3,)), dma((3,)), dma((2, peers)), dma((2, peers)),
            dma((3,)), dma((3,)), dma((2, peers)), dma((2, peers)),
        ],
        compiler_params=pltpu.CompilerParams(collective_id=0, has_side_effects=True),
        name="field",
    )(seam, order, x, w_in, w_mid, w_feat, w_dens, w_conv, w_color)


def body(samples_in, block_order, seam_link, w_in, w_mid, w_feat, w_density, w_conv, w_color):
    n_block, n_patch = lax.axis_size("block"), lax.axis_size("patch")
    x = samples_in.reshape(2, RAYS // 128, 128, SAMP * ENC)
    return render(
        block_order, seam_link, x, w_in, w_mid, jnp.swapaxes(w_feat, 1, 2), w_density, w_conv, w_color, n_block, n_patch
    )


def solution(mesh):
    return jax.shard_map(
        body,
        mesh=mesh,
        in_specs=(
            P("block", None, "patch", None),
            P("patch", None),
            P("patch"),
            P("block", None, None),
            P("block", None, None, None),
            P("block", None, None),
            P("block", None),
            P(),
            P(),
        ),
        out_specs=P(None, "block", "patch"),
        check_vma=False,
    )
```

```python
import functools

import jax
import jax.numpy as jnp
from jax import lax
from jax.experimental import pallas as pl
from jax.experimental.pallas import tpu as pltpu
from jax.sharding import PartitionSpec as P

f32, bf16 = jnp.float32, jnp.bfloat16
MESH = pl.DeviceIdType.MESH

ENC = 32
SAMP = 4
STEP = 0.03
FEAT = 64
WIDTH = 256
COLS = 64
RAYS = 2048
PITCH = 68
SPAN = 512
ROLL = bf16


def iota(shape, dim):
    return lax.broadcasted_iota(jnp.int32, shape, dim)


def relu(x):
    return jnp.maximum(x, 0.0)


def dot(a, b):
    return jnp.dot(a, b, preferred_element_type=f32)


def dot_nt(a, b):
    return lax.dot_general(a, b, (((1,), (1,)), ((), ())), preferred_element_type=f32)


def field_chunks(streams):
    count = len(streams)
    hs = [relu(dot_nt(w1, x)).astype(bf16) for x, w1, w2, w3, head in streams]
    hs = [jnp.concatenate([h[WIDTH * s : WIDTH * (s + 1)] for s in range(SAMP)], axis=1) for h in hs]
    hs = [relu(dot(streams[i][2], hs[i])).astype(bf16) for i in range(count)]
    hs = [relu(dot(streams[i][3], hs[i])).astype(bf16) for i in range(count)]
    outs = [dot(streams[i][4], hs[i]) for i in range(count)]
    results = []
    for out in outs:
        rays = out.shape[1] // SAMP
        raw = out[FEAT : FEAT + 1]
        optical = STEP * (jnp.maximum(raw, 0.0) + jnp.log(1.0 + jnp.exp(-jnp.abs(raw))))
        total = jnp.zeros((1, rays), f32)
        colour = jnp.zeros((FEAT, rays), f32)
        for s in range(SAMP):
            here = optical[:, s * rays : (s + 1) * rays]
            weight = jnp.exp(-total) * (1.0 - jnp.exp(-here))
            total = total + here
            colour = colour + weight * out[:FEAT, s * rays : (s + 1) * rays]
        results.append((total, colour))
    return results


def phase_source(phase, tap):
    return (phase + tap - 1) // 2


def put(ref, row, col, value):
    ref[row : row + value.shape[0], col : col + value.shape[1]] = value


def enlarge_weights(ref, w_conv, layer):
    taps = [[w_conv[layer, a, e].astype(f32) for e in range(3)] for a in range(3)]
    for pa in range(2):
        for pb in range(2):
            for dr in range(-1, 2):
                for dc in range(-1, 2):
                    hits = [taps[a][e] for a in range(3) for e in range(3)
                            if phase_source(pa, a) == dr and phase_source(pb, e) == dc]
                    value = sum(hits[1:], hits[0]) if hits else jnp.zeros((FEAT, FEAT), f32)
                    put(ref, (2 * pa + pb) * FEAT, ((dr + 1) * 3 + dc + 1) * FEAT, value.astype(bf16))


def window_weights(ref, w_conv, layer):
    taps = [[w_conv[layer, a, e].astype(f32) for e in range(3)] for a in range(3)]
    for ua in range(2):
        for ub in range(2):
            for da in range(2):
                for db in range(2):
                    hits = [taps[a][e] for a in range(3) for e in range(3)
                            if phase_source(ua, a) == ua - 1 + da and phase_source(ub, e) == ub - 1 + db]
                    put(ref.at[2 * ua + ub], 0, (2 * da + db) * FEAT, sum(hits[1:], hits[0]).astype(bf16))


def dense_weights(ref, w_conv, layer):
    for qa in range(2):
        for qb in range(2):
            for s in range(-1, 3):
                for t in range(-1, 3):
                    a, e = s - qa + 1, t - qb + 1
                    inside = 0 <= a <= 2 and 0 <= e <= 2
                    value = w_conv[layer, a, e] if inside else jnp.zeros((FEAT, FEAT), bf16)
                    put(ref, (2 * qa + qb) * FEAT, ((s + 1) * 4 + t + 1) * FEAT, value)


def colour_weights(ref, w_conv, w_color, layer):
    ref[...] = jnp.zeros_like(ref)
    for a in range(3):
        for e in range(3):
            tint = dot(w_color[...], w_conv[layer, a, e])
            for i in range(4):
                for j in range(4):
                    group = (i - a + 2) * 6 + (j - e + 2)
                    cell = ((i // 2 * 2 + j // 2) * 2 + i % 2) * 2 + j % 2
                    put(ref, 8 * group, cell * FEAT, tint)


def moved(x, by):
    return pltpu.roll(x, (-by) % x.shape[1], 1) if by else x


def prepare(w_conv, w_color, k0, k1, k2, k3, k4, place, halo_place, weave):
    enlarge_weights(k0, w_conv, 0)
    dense_weights(k1, w_conv, 1)
    window_weights(k2, w_conv, 2)
    colour_weights(k3, w_conv, w_color, 3)
    k4[...] = k3[...].astype(bf16)
    source = iota(place.shape, 0)
    place[...] = (iota(place.shape, 1) == source // COLS * PITCH + source % COLS + 2).astype(f32).astype(bf16)
    source = iota(halo_place.shape, 0)
    target = source // 4 * PITCH + source % 2 + source // 2 % 2 * (COLS + 2)
    halo_place[...] = (iota(halo_place.shape, 1) == target).astype(f32).astype(bf16)
    source = iota(weave.shape, 0)
    target = jnp.where(source % 128 < COLS, 4 * (source % 128) + source // 128, -1)
    weave[...] = (iota(weave.shape, 1) == target).astype(f32).astype(bf16)


def decode(n_block, n_patch, seam, window, halo, link, out, k0, k1, k2, k4, place, halo_place, weave, res):
    me = lax.axis_index("block")
    column = lax.axis_index("patch")
    right_open = jnp.where(column < n_patch - 1, seam[0], 0).astype(f32)
    left_open = link[0:1, 0:1].astype(f32)

    def open_sides(lanes):
        at = iota((1, lanes), 1) % PITCH
        return jnp.where(at < 2, left_open, jnp.where(at < COLS + 2, 1.0, right_open))

    line = iota((1, SPAN), 1) // PITCH
    top = jnp.where(me > 0, 1.0, 0.0)
    bottom = jnp.where(me < n_block - 1, 1.0, 0.0)
    mask = jnp.where(line == 0, top, jnp.where(line < 5, 1.0, jnp.where(line == 5, bottom, 0.0))) * open_sides(SPAN)

    image = dot(jnp.concatenate([window[t] for t in range(4)], axis=1), place[...])
    image = image + dot(halo[...].astype(f32).T[:FEAT].astype(bf16), halo_place[...])
    image = (image * open_sides(image.shape[1])).astype(ROLL)
    patches = [
        moved(image, (dr + 1) * PITCH + dc)[:, :SPAN].astype(bf16) for dr in range(-1, 2) for dc in range(-1, 2)
    ]
    first = (relu(dot(k0[...], jnp.concatenate(patches, axis=0))) * mask).astype(ROLL)

    def views(maps):
        found = {}
        for s in range(-1, 3):
            for t in range(-1, 3):
                phase = (s % 2 * 2 + t % 2) * FEAT
                found[s, t] = moved(maps[phase : phase + FEAT], s // 2 * PITCH + t // 2).astype(bf16)
        return found

    cells = views(first)
    second = relu(dot(k1[...], jnp.concatenate([cells[s, t] for s in range(-1, 3) for t in range(-1, 3)], axis=0)))
    cells = views((second * mask).astype(ROLL))
    third = {}
    for wa in range(3):
        for wb in range(3):
            near = [cells[wa - 1 + da, wb - 1 + db] for da in range(2) for db in range(2)]
            users = [(ua, ub) for ua in range(2) for ub in range(2) if 0 <= wa - ua <= 1 and 0 <= wb - ub <= 1]
            kernels = jnp.concatenate([k2[2 * ua + ub] for ua, ub in users], axis=0)
            found = (relu(dot(kernels, jnp.concatenate(near, axis=0))) * mask).astype(bf16)
            for i, (ua, ub) in enumerate(users):
                third[wa - ua, wb - ub, ua, ub] = found[FEAT * i : FEAT * (i + 1)]
    parts = [third[key] for key in sorted(third)]
    spread = dot(k4[...], jnp.concatenate(parts, axis=0))

    def cell(i, j):
        group = (i + 1) * 6 + j + 1
        return spread[8 * group : 8 * group + 8]

    def row(i, j):
        value = cell(i, j)
        if i == 0:
            value = value + moved(cell(4, j), -PITCH)
        if i == 3:
            value = value + moved(cell(-1, j), PITCH)
        return value

    stack = []
    for i in range(4):
        cols = [row(i, j) for j in range(-1, 5)]
        middle = cols[1:5]
        middle[0] = middle[0] + moved(cols[5], -1)
        middle[3] = middle[3] + moved(cols[0], 1)
        stack.append(jnp.concatenate(middle, axis=0))
    stack = jnp.concatenate(stack, axis=0)
    starts = [(r + 1) * PITCH + 2 for r in range(4)]
    lines = [moved(stack[:, a // 128 * 128 : a // 128 * 128 + 256], a % 128)[:, :128] for a in starts[:3]]
    lines.append(moved(stack, starts[3])[:, :128])
    wide = jnp.concatenate(
        [
            jnp.concatenate([lines[r][8 * (4 * i + j) : 8 * (4 * i + j) + 8] for j in range(4)], axis=1)
            for r in range(4) for i in range(4)
        ],
        axis=0,
    )
    high = wide.astype(bf16)
    low = (wide - high.astype(f32)).astype(bf16)
    woven = dot(high, weave[...]) + dot(low, weave[...])
    for half in range(2):
        lanes = slice(128 * half, 128 * (half + 1))
        res[half] = woven[:, lanes]
        for k in range(3):
            out[k, :, lanes] = res[half, pl.ds(k, 16, stride=8), :]


def last_tile(device):
    return ((device + 1) // 2 + 3) % 4


def field_kernel(
    n_block, n_patch, seam, order_far, x_far, w_in_far, w_mid_far, w_feat_far, w_dens_far, w_conv_far, w_color_far, out,
    order, x, w_in, w_mid, w_feat, w_dens, w_conv, w_color, fetched,
    window_out, halo_out, k0, k1, k2, k3, k4, place_rows, place_halo, weave, res,
    spread, w1, w2, w3, head, rays_out, rays_in, meta, meta_in, depth_rows, tiles, tiles_in, last_in, passed, passed_in,
    halo, halo_in, halo_depth, halo_depth_in, lines16, shares,
    rays_send, rays_recv, meta_send, meta_recv, tile_send, tile_recv, last_send, last_recv, pass_send, pass_recv,
    halo_send, halo_recv,
):
    me = lax.axis_index("block")
    place = lax.axis_index("patch")
    far_first = sorted(range(1, n_block), key=lambda k: abs(k - n_block // 2))
    sides = ((place - 1, place > 0), (place + 1, place < n_patch - 1))
    pairs = (
        (w_in_far, w_in), (w_mid_far, w_mid), (w_feat_far, w_feat), (w_dens_far, w_dens), (x_far, x), (order_far, order),
        (w_conv_far, w_conv), (w_color_far, w_color),
    )
    fetches = [pltpu.make_async_copy(far, near, fetched.at[i]) for i, (far, near) in enumerate(pairs)]
    for fetch in fetches:
        fetch.start()
    rays_in[...] = jnp.zeros_like(rays_in)
    meta_in[...] = jnp.zeros_like(meta_in)
    barrier = pltpu.get_barrier_semaphore()
    for k in range(1, n_block):
        pl.semaphore_signal(barrier, inc=1, device_id=((me + k) % n_block, place), device_id_type=MESH)
    for side, there in sides:

        @pl.when(there)
        def _():
            pl.semaphore_signal(barrier, inc=1, device_id=(me, side), device_id_type=MESH)

    spread[...] = jnp.zeros_like(spread)
    for fetch in fetches[:4]:
        fetch.wait()
    for m in range(2):
        for s in range(SAMP):
            spread[ENC * s : ENC * (s + 1), WIDTH * s : WIDTH * (s + 1)] = w_in[m]
        w1[m] = spread[...].T
        w2[m] = w_mid[m, 0].T
        w3[m] = w_mid[m, 1].T
        head[m, :FEAT] = w_feat[m]
        head[m, FEAT:] = jnp.broadcast_to(w_dens[pl.ds(m, 1), :], (16, WIDTH))
    for fetch in fetches[4:6]:
        fetch.wait()
    line = iota((16, 256), 0)
    wanted = line % 8 // 2 * COLS + line % 2 + jnp.where(line >= 8, COLS - 2, 0)
    pick = (iota((16, 256), 1) == wanted).astype(f32).astype(bf16)
    for m in range(2):
        found = [dot(pick, x[m, 2 * g : 2 * g + 2].reshape(256, 128)) for g in range(8)]
        for side in range(2):
            rows = jnp.concatenate([f[8 * side : 8 * side + 8] for f in found], axis=0)
            rays_out[side, m] = rows.astype(bf16)
    slot = iota((16, 128), 0)
    member = 2 * ((me + n_block - slot // 2) % n_block) + slot % 2
    rank = jnp.zeros((16, 128), jnp.int32)
    for k in range(16):
        rank = jnp.where(member == order[0, k], k, rank)
    meta[:16] = rank
    meta[16:] = jnp.full((8, 128), jnp.where(place < n_patch - 1, seam[0], 0), jnp.int32)

    depth_rows[...] = jnp.zeros_like(depth_rows)

    def side_copies(side):
        target = (me, sides[side][0])
        return [
            pltpu.make_async_remote_copy(
                src_ref=rays_out.at[side], dst_ref=rays_in.at[1 - side], send_sem=rays_send.at[side],
                recv_sem=rays_recv.at[1 - side], device_id=target, device_id_type=MESH,
            ),
            pltpu.make_async_remote_copy(
                src_ref=meta, dst_ref=meta_in.at[1 - side], send_sem=meta_send.at[side],
                recv_sem=meta_recv.at[1 - side], device_id=target, device_id_type=MESH,
            ),
        ]

    count = (place > 0).astype(jnp.int32) + (place < n_patch - 1).astype(jnp.int32)
    pl.semaphore_wait(barrier, n_block - 1 + count)
    for side in range(2):
        for copy in side_copies(side):
            pl.when(sides[side][1])(copy.start)

    def weights(m):
        return w1[m], w2[m], w3[m], head[m]

    def depth_block(m, total):
        lanes = slice(0, total.shape[1])
        high = total.astype(bf16).astype(f32)
        depth_rows[m : m + 1, lanes] = high
        depth_rows[2 + m : 3 + m, lanes] = total - high

    def rays_of(unit, m):
        return jnp.concatenate([x[m, 4 * j + unit] for j in range(4)], axis=0)

    def keep(unit, m, tint):
        tint = tint.astype(bf16)
        for j in range(4):
            tiles[unit, j, FEAT * m : FEAT * (m + 1)] = tint[:, 128 * j : 128 * (j + 1)]

    def keep_depth(unit):
        rows = depth_rows[...].astype(bf16)
        for j in range(4):
            tiles[unit, j, 2 * FEAT :] = rows[:, 128 * j : 128 * (j + 1)]

    def store(unit, results):
        for m, (total, tint) in enumerate(results):
            keep(unit, m, tint)
            depth_block(m, total)
        keep_depth(unit)

    def send_owner(unit):
        for j in range(4):
            owner = 2 * j + unit // 2

            @pl.when(owner != me)
            def _():
                pltpu.make_async_remote_copy(
                    src_ref=tiles.at[unit, j], dst_ref=tiles_in.at[unit, (owner + n_block - me) % n_block - 1],
                    send_sem=tile_send.at[unit], recv_sem=tile_recv.at[unit],
                    device_id=(owner, place), device_id_type=MESH,
                ).start()

    def loop(unit, carry):
        store(unit, field_chunks([(rays_of(unit, m), *weights(m)) for m in range(2)]))
        send_owner(unit)
        return carry

    lax.fori_loop(0, 3, loop, 0)

    for side in range(2):
        for copy in side_copies(side):
            pl.when(sides[1 - side][1])(copy.wait_recv)
    results = field_chunks(
        [(jnp.concatenate([rays_in[0, m], rays_in[1, m]], axis=0), *weights(m)) for m in range(2)]
        + [(rays_of(3, 0), *weights(0))]
    )
    ((last_total, last_tint),) = results[2:]
    results = results[:2]
    for m, (total, tint) in enumerate(results):
        depth_block(m, total)
    halo_depth[...] = depth_rows[:, :128].astype(bf16)
    ray = iota((144, 128), 0) - 8
    source = jnp.where((ray >= 0) & (ray < 128), ray // 2 % 2 * 64 + ray // 4 * 2 + ray % 2, -1)
    turn = (iota((144, 128), 1) == source).astype(f32).astype(bf16)
    both = jnp.concatenate([tint for total, tint in results], axis=0).astype(bf16)
    halo[...] = dot_nt(turn, both).astype(bf16)

    def halo_copies(k):
        peer = (me + k) % n_block
        return [
            pltpu.make_async_remote_copy(
                src_ref=halo.at[pl.ds(pl.multiple_of(16 * peer, 16), 32)], dst_ref=halo_in.at[k - 1],
                send_sem=halo_send.at[0, k - 1], recv_sem=halo_recv.at[0, k - 1],
                device_id=(peer, place), device_id_type=MESH,
            ),
            pltpu.make_async_remote_copy(
                src_ref=halo_depth, dst_ref=halo_depth_in.at[k - 1],
                send_sem=halo_send.at[1, k - 1], recv_sem=halo_recv.at[1, k - 1],
                device_id=(peer, place), device_id_type=MESH,
            ),
        ]

    for k in far_first:
        for copy in halo_copies(k):
            copy.start()

    def last_copy(k, m):
        peer = (me + k) % n_block
        rows = pl.ds(0, FEAT) if m == 0 else pl.ds(FEAT, FEAT + 8)
        return pltpu.make_async_remote_copy(
            src_ref=tiles.at[3, last_tile(peer), rows], dst_ref=last_in.at[k - 1, rows],
            send_sem=last_send.at[m, k - 1], recv_sem=last_recv.at[m, k - 1],
            device_id=(peer, place), device_id_type=MESH,
        )

    for m in range(2):
        total, tint = (last_total, last_tint) if m == 0 else field_chunks([(rays_of(3, 1), *weights(1))])[0]
        keep(3, m, tint)
        depth_block(m, total)
        if m == 1:
            keep_depth(3)
        for k in far_first:
            last_copy(k, m).start()

    def order_weights(blocks, ranks):
        for k, block in enumerate(blocks):
            block = block.astype(f32)
            lines16[2 * k : 2 * k + 2] = block[0:2] + block[2:4]
        depths = lines16[...]
        prefixes = [
            jnp.sum(jnp.where(ranks < ranks[i : i + 1], depths, 0.0), axis=0, keepdims=True) for i in range(16)
        ]
        return [jnp.exp(-prefix) for prefix in prefixes]

    def combine(own, got):
        slots = [own] + [got.at[k - 1] for k in range(1, n_block)]
        factors = order_weights([slot[2 * FEAT :] for slot in slots], meta[:16])
        mixed = jnp.zeros((FEAT, 128), f32)
        for i in range(16):
            tint = slots[i // 2][i % 2 * FEAT : (i % 2 + 1) * FEAT]
            mixed = mixed + factors[i] * tint.astype(f32)
        return mixed

    def pass_copy(unit):
        target = me - 1 if unit % 2 == 0 else me + 1
        return pltpu.make_async_remote_copy(
            src_ref=passed.at[unit], dst_ref=passed_in.at[unit], send_sem=pass_send.at[unit],
            recv_sem=pass_recv.at[unit], device_id=(target, place), device_id_type=MESH,
        )

    def mine(unit):
        return me % 2 == unit // 2

    def has_target(unit):
        return mine(unit) & ((me > 0) if unit % 2 == 0 else (me < n_block - 1))

    def has_source(unit):
        return (me % 2 != unit // 2) & ((me < n_block - 1) if unit % 2 == 0 else (me > 0))

    for unit in range(3):

        @pl.when(mine(unit))
        def _():
            pltpu.make_async_copy(tiles_in.at[unit], tiles_in.at[unit], tile_recv.at[unit]).wait()
            passed[unit] = combine(tiles.at[unit, me // 2], tiles_in.at[unit]).astype(bf16)

        pl.when(has_target(unit))(pass_copy(unit).start)

        @pl.when(mine(unit))
        def _():
            window_out[1 + unit % 2] = passed[unit]

    for fetch in fetches[6:]:
        fetch.wait()
    prepare(w_conv, w_color, k0, k1, k2, k3, k4, place_rows, place_halo, weave)

    for k in range(1, n_block):
        for copy in halo_copies(k):
            copy.wait_recv()
    ranks = jnp.where(iota((16, 128), 1) < 64, meta_in[0, :16], meta_in[1, :16])
    factors = order_weights([halo_depth[...]] + [halo_depth_in[k - 1] for k in range(1, n_block)], ranks)
    for i in range(16):
        shares[i : i + 1] = factors[i]
    line = iota((32, 128), 0)
    row = line // 4 + 4 * me - 2
    source = jnp.where((row >= 0) & (row < 32), line // 2 % 2 * 64 + row * 2 + line % 2, -1)
    turn = (iota((32, 128), 1) == source).astype(f32).astype(bf16)
    high = shares[...].astype(bf16)
    low = (shares[...] - high.astype(f32)).astype(bf16)
    share = dot_nt(turn, high) + dot_nt(turn, low)
    mixed = jnp.zeros((32, 128), f32)
    for k in range(n_block):
        tint = halo[pl.ds(pl.multiple_of(16 * me, 16), 32), :] if k == 0 else halo_in[k - 1]
        factor = jnp.where(iota((32, 128), 1) < 64, share[:, 2 * k : 2 * k + 1], share[:, 2 * k + 1 : 2 * k + 2])
        mixed = mixed + factor * tint.astype(f32)
    halo_out[...] = (mixed + pltpu.roll(mixed, 64, 1)).astype(bf16)

    for unit in range(3):

        @pl.when(has_source(unit))
        def _():
            pass_copy(unit).wait_recv()
            window_out[3 - unit % 2 * 3] = passed_in[unit]

    @pl.when(me == n_block - 1)
    def _():
        window_out[3] = jnp.zeros((FEAT, 128), bf16)

    for m in range(2):
        for k in range(1, n_block):
            last_copy(k, m).wait_recv()
    mixed = combine(tiles.at[3, last_tile(me)], last_in)
    window_out[me % 2 * 2] = (mixed * jnp.where(me > 0, 1.0, 0.0)).astype(bf16)
    decode(
        n_block, n_patch, seam, window_out, halo_out, meta_in.at[0, pl.ds(16, 8)], out, k0, k1, k2, k4,
        place_rows, place_halo, weave, res,
    )

    for side in range(2):
        for copy in side_copies(side):
            pl.when(sides[side][1])(copy.wait_send)
    for k in range(1, n_block):
        for copy in halo_copies(k) + [last_copy(k, 0), last_copy(k, 1)]:
            copy.wait_send()
    for unit in range(3):
        pl.when(has_target(unit))(pass_copy(unit).wait_send)
        sent = pltpu.make_async_copy(tiles_in.at[unit, pl.ds(0, 3)], tiles_in.at[unit, pl.ds(0, 3)], tile_send.at[unit])
        more = pltpu.make_async_copy(tiles_in.at[unit, 3], tiles_in.at[unit, 3], tile_send.at[unit])
        sent.wait()
        pl.when(me % 2 != unit // 2)(more.wait)


def render(order, seam, x, w_in, w_mid, w_feat, w_dens, w_conv, w_color, n_block, n_patch):
    vmem = pl.BlockSpec(memory_space=pltpu.VMEM)
    smem = pl.BlockSpec(memory_space=pltpu.SMEM)
    dma = pltpu.SemaphoreType.DMA
    peers = n_block - 1
    rows = 2 * FEAT + 8
    return pl.pallas_call(
        functools.partial(field_kernel, n_block, n_patch),
        out_shape=pltpu.VMEM((3, 16, 256), f32),
        in_specs=[smem] + [pl.BlockSpec(memory_space=pl.ANY)] * 8,
        out_specs=vmem,
        scratch_shapes=[
            pltpu.SMEM(order.shape, jnp.int32),
            *[pltpu.VMEM(array.shape, bf16) for array in (x, w_in, w_mid, w_feat, w_dens, w_conv, w_color)],
            dma((8,)),
            pltpu.VMEM((4, FEAT, 128), bf16),
            pltpu.VMEM((32, 128), bf16),
            pltpu.VMEM((256, 576), bf16),
            pltpu.VMEM((256, 1024), bf16),
            pltpu.VMEM((4, FEAT, 256), bf16),
            pltpu.VMEM((288, 1024), f32),
            pltpu.VMEM((288, 1024), bf16),
            pltpu.VMEM((512, 640), bf16),
            pltpu.VMEM((32, 640), bf16),
            pltpu.VMEM((512, 256), bf16),
            pltpu.VMEM((2, 128, 128), f32),
            pltpu.VMEM((128, 1024), bf16),
            pltpu.VMEM((2, 1024, 128), bf16),
            pltpu.VMEM((2, WIDTH, WIDTH), bf16),
            pltpu.VMEM((2, WIDTH, WIDTH), bf16),
            pltpu.VMEM((2, FEAT + 16, WIDTH), bf16),
            pltpu.VMEM((2, 2, 64, 128), bf16),
            pltpu.VMEM((2, 2, 64, 128), bf16),
            pltpu.VMEM((24, 128), jnp.int32),
            pltpu.VMEM((2, 24, 128), jnp.int32),
            pltpu.VMEM((8, 512), f32),
            pltpu.VMEM((4, 4, rows, 128), bf16),
            pltpu.VMEM((3, peers, rows, 128), bf16),
            pltpu.VMEM((peers, rows, 128), bf16),
            pltpu.VMEM((3, FEAT, 128), bf16),
            pltpu.VMEM((3, FEAT, 128), bf16),
            pltpu.VMEM((144, 128), bf16),
            pltpu.VMEM((peers, 32, 128), bf16),
            pltpu.VMEM((8, 128), bf16),
            pltpu.VMEM((peers, 8, 128), bf16),
            pltpu.VMEM((16, 128), f32),
            pltpu.VMEM((16, 128), f32),
            dma((2,)), dma((2,)), dma((2,)), dma((2,)), dma((3,)), dma((3,)), dma((2, peers)), dma((2, peers)),
            dma((3,)), dma((3,)), dma((2, peers)), dma((2, peers)),
        ],
        compiler_params=pltpu.CompilerParams(collective_id=0, has_side_effects=True),
        name="field",
    )(seam, order, x, w_in, w_mid, w_feat, w_dens, w_conv, w_color)


def body(samples_in, block_order, seam_link, w_in, w_mid, w_feat, w_density, w_conv, w_color):
    n_block, n_patch = lax.axis_size("block"), lax.axis_size("patch")
    x = samples_in.reshape(2, RAYS // 128, 128, SAMP * ENC)
    return render(
        block_order, seam_link, x, w_in, w_mid, jnp.swapaxes(w_feat, 1, 2), w_density, w_conv, w_color, n_block, n_patch
    )


def solution(mesh):
    return jax.shard_map(
        body,
        mesh=mesh,
        in_specs=(
            P("block", None, "patch", None),
            P("patch", None),
            P("patch"),
            P("block", None, None),
            P("block", None, None, None),
            P("block", None, None),
            P("block", None),
            P(),
            P(),
        ),
        out_specs=P(None, "block", "patch"),
        check_vma=False,
    )
```

```python
import functools

import jax
import jax.numpy as jnp
from jax import lax
from jax.experimental import pallas as pl
from jax.experimental.pallas import tpu as pltpu
from jax.sharding import PartitionSpec as P

f32, bf16 = jnp.float32, jnp.bfloat16
MESH = pl.DeviceIdType.MESH

ENC = 32
SAMP = 4
STEP = 0.03
FEAT = 64
WIDTH = 256
COLS = 64
RAYS = 2048
PITCH = 68
SPAN = 512
ROLL = bf16


def iota(shape, dim):
    return lax.broadcasted_iota(jnp.int32, shape, dim)


def relu(x):
    return jnp.maximum(x, 0.0)


def dot(a, b):
    return jnp.dot(a, b, preferred_element_type=f32)


def dot_nt(a, b):
    return lax.dot_general(a, b, (((1,), (1,)), ((), ())), preferred_element_type=f32)


def field_chunks(streams):
    count = len(streams)
    hs = [relu(dot_nt(w1, x)).astype(bf16) for x, w1, w2, w3, head in streams]
    hs = [jnp.concatenate([h[WIDTH * s : WIDTH * (s + 1)] for s in range(SAMP)], axis=1) for h in hs]
    hs = [relu(dot(streams[i][2], hs[i])).astype(bf16) for i in range(count)]
    hs = [relu(dot(streams[i][3], hs[i])).astype(bf16) for i in range(count)]
    outs = [dot(streams[i][4], hs[i]) for i in range(count)]
    results = []
    for out in outs:
        rays = out.shape[1] // SAMP
        raw = out[FEAT : FEAT + 1]
        optical = STEP * (jnp.maximum(raw, 0.0) + jnp.log(1.0 + jnp.exp(-jnp.abs(raw))))
        total = jnp.zeros((1, rays), f32)
        colour = jnp.zeros((FEAT, rays), f32)
        for s in range(SAMP):
            here = optical[:, s * rays : (s + 1) * rays]
            weight = jnp.exp(-total) * (1.0 - jnp.exp(-here))
            total = total + here
            colour = colour + weight * out[:FEAT, s * rays : (s + 1) * rays]
        results.append((total, colour))
    return results


def phase_source(phase, tap):
    return (phase + tap - 1) // 2


def put(ref, row, col, value):
    ref[row : row + value.shape[0], col : col + value.shape[1]] = value


def enlarge_weights(ref, w_conv, layer):
    taps = [[w_conv[layer, a, e].astype(f32) for e in range(3)] for a in range(3)]
    for pa in range(2):
        for pb in range(2):
            for dr in range(-1, 2):
                for dc in range(-1, 2):
                    hits = [taps[a][e] for a in range(3) for e in range(3)
                            if phase_source(pa, a) == dr and phase_source(pb, e) == dc]
                    value = sum(hits[1:], hits[0]) if hits else jnp.zeros((FEAT, FEAT), f32)
                    put(ref, (2 * pa + pb) * FEAT, ((dr + 1) * 3 + dc + 1) * FEAT, value.astype(bf16))


def window_weights(ref, w_conv, layer):
    taps = [[w_conv[layer, a, e].astype(f32) for e in range(3)] for a in range(3)]
    for ua in range(2):
        for ub in range(2):
            for da in range(2):
                for db in range(2):
                    hits = [taps[a][e] for a in range(3) for e in range(3)
                            if phase_source(ua, a) == ua - 1 + da and phase_source(ub, e) == ub - 1 + db]
                    put(ref.at[2 * ua + ub], 0, (2 * da + db) * FEAT, sum(hits[1:], hits[0]).astype(bf16))


def dense_weights(ref, w_conv, layer):
    for qa in range(2):
        for qb in range(2):
            for s in range(-1, 3):
                for t in range(-1, 3):
                    a, e = s - qa + 1, t - qb + 1
                    inside = 0 <= a <= 2 and 0 <= e <= 2
                    value = w_conv[layer, a, e] if inside else jnp.zeros((FEAT, FEAT), bf16)
                    put(ref, (2 * qa + qb) * FEAT, ((s + 1) * 4 + t + 1) * FEAT, value)


def colour_weights(ref, w_conv, w_color, layer):
    ref[...] = jnp.zeros_like(ref)
    for a in range(3):
        for e in range(3):
            tint = dot(w_color[...], w_conv[layer, a, e])
            for i in range(4):
                for j in range(4):
                    group = (i - a + 2) * 6 + (j - e + 2)
                    cell = ((i // 2 * 2 + j // 2) * 2 + i % 2) * 2 + j % 2
                    put(ref, 8 * group, cell * FEAT, tint)


def moved(x, by):
    return pltpu.roll(x, (-by) % x.shape[1], 1) if by else x


def prepare(w_conv, w_color, k0, k1, k2, k3, k4, place, halo_place, weave):
    enlarge_weights(k0, w_conv, 0)
    dense_weights(k1, w_conv, 1)
    window_weights(k2, w_conv, 2)
    colour_weights(k3, w_conv, w_color, 3)
    k4[...] = k3[...].astype(bf16)
    source = iota(place.shape, 0)
    place[...] = (iota(place.shape, 1) == source // COLS * PITCH + source % COLS + 2).astype(f32).astype(bf16)
    source = iota(halo_place.shape, 0)
    target = source // 4 * PITCH + source % 2 + source // 2 % 2 * (COLS + 2)
    halo_place[...] = (iota(halo_place.shape, 1) == target).astype(f32).astype(bf16)
    source = iota(weave.shape, 0)
    target = jnp.where(source % 128 < COLS, 4 * (source % 128) + source // 128, -1)
    weave[...] = (iota(weave.shape, 1) == target).astype(f32).astype(bf16)


def decode(n_block, n_patch, seam, window, halo, link, out, k0, k1, k2, k4, place, halo_place, weave, res):
    me = lax.axis_index("block")
    column = lax.axis_index("patch")
    right_open = jnp.where(column < n_patch - 1, seam[0], 0).astype(f32)
    left_open = link[0:1, 0:1].astype(f32)

    def open_sides(lanes):
        at = iota((1, lanes), 1) % PITCH
        return jnp.where(at < 2, left_open, jnp.where(at < COLS + 2, 1.0, right_open))

    line = iota((1, SPAN), 1) // PITCH
    top = jnp.where(me > 0, 1.0, 0.0)
    bottom = jnp.where(me < n_block - 1, 1.0, 0.0)
    mask = jnp.where(line == 0, top, jnp.where(line < 5, 1.0, jnp.where(line == 5, bottom, 0.0))) * open_sides(SPAN)

    image = dot(jnp.concatenate([window[t] for t in range(4)], axis=1), place[...])
    image = image + dot(halo[...].astype(f32).T[:FEAT].astype(bf16), halo_place[...])
    image = (image * open_sides(image.shape[1])).astype(ROLL)
    patches = [
        moved(image, (dr + 1) * PITCH + dc)[:, :SPAN].astype(bf16) for dr in range(-1, 2) for dc in range(-1, 2)
    ]
    first = (relu(dot(k0[...], jnp.concatenate(patches, axis=0))) * mask).astype(ROLL)

    def views(maps):
        found = {}
        for s in range(-1, 3):
            for t in range(-1, 3):
                phase = (s % 2 * 2 + t % 2) * FEAT
                found[s, t] = moved(maps[phase : phase + FEAT], s // 2 * PITCH + t // 2).astype(bf16)
        return found

    cells = views(first)
    second = relu(dot(k1[...], jnp.concatenate([cells[s, t] for s in range(-1, 3) for t in range(-1, 3)], axis=0)))
    cells = views((second * mask).astype(ROLL))
    third = {}
    for wa in range(3):
        for wb in range(3):
            near = [cells[wa - 1 + da, wb - 1 + db] for da in range(2) for db in range(2)]
            users = [(ua, ub) for ua in range(2) for ub in range(2) if 0 <= wa - ua <= 1 and 0 <= wb - ub <= 1]
            kernels = jnp.concatenate([k2[2 * ua + ub] for ua, ub in users], axis=0)
            found = (relu(dot(kernels, jnp.concatenate(near, axis=0))) * mask).astype(bf16)
            for i, (ua, ub) in enumerate(users):
                third[wa - ua, wb - ub, ua, ub] = found[FEAT * i : FEAT * (i + 1)]
    parts = [third[key] for key in sorted(third)]
    spread = dot(k4[...], jnp.concatenate(parts, axis=0))

    def cell(i, j):
        group = (i + 1) * 6 + j + 1
        return spread[8 * group : 8 * group + 8]

    def row(i, j):
        value = cell(i, j)
        if i == 0:
            value = value + moved(cell(4, j), -PITCH)
        if i == 3:
            value = value + moved(cell(-1, j), PITCH)
        return value

    stack = []
    for i in range(4):
        cols = [row(i, j) for j in range(-1, 5)]
        middle = cols[1:5]
        middle[0] = middle[0] + moved(cols[5], -1)
        middle[3] = middle[3] + moved(cols[0], 1)
        stack.append(jnp.concatenate(middle, axis=0))
    stack = jnp.concatenate(stack, axis=0)
    starts = [(r + 1) * PITCH + 2 for r in range(4)]
    lines = [moved(stack[:, a // 128 * 128 : a // 128 * 128 + 256], a % 128)[:, :128] for a in starts[:3]]
    lines.append(moved(stack, starts[3])[:, :128])
    wide = jnp.concatenate(
        [
            jnp.concatenate([lines[r][8 * (4 * i + j) : 8 * (4 * i + j) + 8] for j in range(4)], axis=1)
            for r in range(4) for i in range(4)
        ],
        axis=0,
    )
    high = wide.astype(bf16)
    low = (wide - high.astype(f32)).astype(bf16)
    woven = dot(high, weave[...]) + dot(low, weave[...])
    for half in range(2):
        lanes = slice(128 * half, 128 * (half + 1))
        res[half] = woven[:, lanes]
        for k in range(3):
            out[k, :, lanes] = res[half, pl.ds(k, 16, stride=8), :]


def last_tile(device):
    return ((device + 1) // 2 + 3) % 4


def field_kernel(
    n_block, n_patch, seam, order_far, x_far, w_in_far, w_mid_far, w_feat_far, w_dens_far, w_conv_far, w_color_far, out,
    order, x, w_in, w_mid, w_feat, w_dens, w_conv, w_color, fetched,
    window_out, halo_out, k0, k1, k2, k3, k4, place_rows, place_halo, weave, res,
    spread, w1, w2, w3, head, rays_out, rays_in, meta, meta_in, depth_rows, tiles, tiles_in, last_in, passed, passed_in,
    halo, halo_in, halo_depth, halo_depth_in, lines16, shares,
    rays_send, rays_recv, meta_send, meta_recv, tile_send, tile_recv, last_send, last_recv, pass_send, pass_recv,
    halo_send, halo_recv,
):
    me = lax.axis_index("block")
    place = lax.axis_index("patch")
    far_first = sorted(range(1, n_block), key=lambda k: abs(k - n_block // 2))
    sides = ((place - 1, place > 0), (place + 1, place < n_patch - 1))
    pairs = (
        (w_in_far, w_in), (w_mid_far, w_mid), (w_feat_far, w_feat), (w_dens_far, w_dens), (x_far, x), (order_far, order),
        (w_conv_far, w_conv), (w_color_far, w_color),
    )
    fetches = [pltpu.make_async_copy(far, near, fetched.at[i]) for i, (far, near) in enumerate(pairs)]
    for fetch in fetches:
        fetch.start()
    rays_in[...] = jnp.zeros_like(rays_in)
    meta_in[...] = jnp.zeros_like(meta_in)
    barrier = pltpu.get_barrier_semaphore()
    for k in range(1, n_block):
        pl.semaphore_signal(barrier, inc=1, device_id=((me + k) % n_block, place), device_id_type=MESH)
    for side, there in sides:

        @pl.when(there)
        def _():
            pl.semaphore_signal(barrier, inc=1, device_id=(me, side), device_id_type=MESH)

    spread[...] = jnp.zeros_like(spread)
    for fetch in fetches[:4]:
        fetch.wait()
    for m in range(2):
        for s in range(SAMP):
            spread[ENC * s : ENC * (s + 1), WIDTH * s : WIDTH * (s + 1)] = w_in[m]
        w1[m] = spread[...].T
        w2[m] = w_mid[m, 0].T
        w3[m] = w_mid[m, 1].T
        head[m, :FEAT] = w_feat[m]
        head[m, FEAT:] = jnp.broadcast_to(w_dens[pl.ds(m, 1), :], (16, WIDTH))
    for fetch in fetches[4:6]:
        fetch.wait()
    line = iota((16, 256), 0)
    wanted = line % 8 // 2 * COLS + line % 2 + jnp.where(line >= 8, COLS - 2, 0)
    pick = (iota((16, 256), 1) == wanted).astype(f32).astype(bf16)
    for m in range(2):
        found = [dot(pick, x[m, 2 * g : 2 * g + 2].reshape(256, 128)) for g in range(8)]
        for side in range(2):
            rows = jnp.concatenate([f[8 * side : 8 * side + 8] for f in found], axis=0)
            rays_out[side, m] = rows.astype(bf16)
    slot = iota((16, 128), 0)
    member = 2 * ((me + n_block - slot // 2) % n_block) + slot % 2
    rank = jnp.zeros((16, 128), jnp.int32)
    for k in range(16):
        rank = jnp.where(member == order[0, k], k, rank)
    meta[:16] = rank
    meta[16:] = jnp.full((8, 128), jnp.where(place < n_patch - 1, seam[0], 0), jnp.int32)

    depth_rows[...] = jnp.zeros_like(depth_rows)

    def side_copies(side):
        target = (me, sides[side][0])
        return [
            pltpu.make_async_remote_copy(
                src_ref=rays_out.at[side], dst_ref=rays_in.at[1 - side], send_sem=rays_send.at[side],
                recv_sem=rays_recv.at[1 - side], device_id=target, device_id_type=MESH,
            ),
            pltpu.make_async_remote_copy(
                src_ref=meta, dst_ref=meta_in.at[1 - side], send_sem=meta_send.at[side],
                recv_sem=meta_recv.at[1 - side], device_id=target, device_id_type=MESH,
            ),
        ]

    count = (place > 0).astype(jnp.int32) + (place < n_patch - 1).astype(jnp.int32)
    pl.semaphore_wait(barrier, n_block - 1 + count)
    for side in range(2):
        for copy in side_copies(side):
            pl.when(sides[side][1])(copy.start)

    def weights(m):
        return w1[m], w2[m], w3[m], head[m]

    def depth_block(m, total):
        lanes = slice(0, total.shape[1])
        high = total.astype(bf16).astype(f32)
        depth_rows[m : m + 1, lanes] = high
        depth_rows[2 + m : 3 + m, lanes] = total - high

    def rays_of(unit, m):
        return jnp.concatenate([x[m, 4 * j + unit] for j in range(4)], axis=0)

    def keep(unit, m, tint):
        tint = tint.astype(bf16)
        for j in range(4):
            tiles[unit, j, FEAT * m : FEAT * (m + 1)] = tint[:, 128 * j : 128 * (j + 1)]

    def keep_depth(unit):
        rows = depth_rows[...].astype(bf16)
        for j in range(4):
            tiles[unit, j, 2 * FEAT :] = rows[:, 128 * j : 128 * (j + 1)]

    def store(unit, results):
        for m, (total, tint) in enumerate(results):
            keep(unit, m, tint)
            depth_block(m, total)
        keep_depth(unit)

    def send_owner(unit):
        for j in range(4):
            owner = 2 * j + unit // 2

            @pl.when(owner != me)
            def _():
                pltpu.make_async_remote_copy(
                    src_ref=tiles.at[unit, j], dst_ref=tiles_in.at[unit, (owner + n_block - me) % n_block - 1],
                    send_sem=tile_send.at[unit], recv_sem=tile_recv.at[unit],
                    device_id=(owner, place), device_id_type=MESH,
                ).start()

    def loop(unit, carry):
        store(unit, field_chunks([(rays_of(unit, m), *weights(m)) for m in range(2)]))
        send_owner(unit)
        return carry

    lax.fori_loop(0, 2, loop, 0)

    for side in range(2):
        for copy in side_copies(side):
            pl.when(sides[1 - side][1])(copy.wait_recv)
    results = field_chunks(
        [(rays_of(2, m), *weights(m)) for m in range(2)]
        + [(jnp.concatenate([rays_in[0, m], rays_in[1, m]], axis=0), *weights(m)) for m in range(2)]
    )
    store(2, results[:2])
    send_owner(2)
    results = results[2:]
    for m, (total, tint) in enumerate(results):
        depth_block(m, total)
    halo_depth[...] = depth_rows[:, :128].astype(bf16)
    ray = iota((144, 128), 0) - 8
    source = jnp.where((ray >= 0) & (ray < 128), ray // 2 % 2 * 64 + ray // 4 * 2 + ray % 2, -1)
    turn = (iota((144, 128), 1) == source).astype(f32).astype(bf16)
    both = jnp.concatenate([tint for total, tint in results], axis=0).astype(bf16)
    halo[...] = dot_nt(turn, both).astype(bf16)

    def halo_copies(k):
        peer = (me + k) % n_block
        return [
            pltpu.make_async_remote_copy(
                src_ref=halo.at[pl.ds(pl.multiple_of(16 * peer, 16), 32)], dst_ref=halo_in.at[k - 1],
                send_sem=halo_send.at[0, k - 1], recv_sem=halo_recv.at[0, k - 1],
                device_id=(peer, place), device_id_type=MESH,
            ),
            pltpu.make_async_remote_copy(
                src_ref=halo_depth, dst_ref=halo_depth_in.at[k - 1],
                send_sem=halo_send.at[1, k - 1], recv_sem=halo_recv.at[1, k - 1],
                device_id=(peer, place), device_id_type=MESH,
            ),
        ]

    for k in far_first:
        for copy in halo_copies(k):
            copy.start()

    def last_copy(k, m):
        peer = (me + k) % n_block
        rows = pl.ds(0, FEAT) if m == 0 else pl.ds(FEAT, FEAT + 8)
        return pltpu.make_async_remote_copy(
            src_ref=tiles.at[3, last_tile(peer), rows], dst_ref=last_in.at[k - 1, rows],
            send_sem=last_send.at[m, k - 1], recv_sem=last_recv.at[m, k - 1],
            device_id=(peer, place), device_id_type=MESH,
        )

    for m in range(2):
        ((total, tint),) = field_chunks([(rays_of(3, m), *weights(m))])
        keep(3, m, tint)
        depth_block(m, total)
        if m == 1:
            keep_depth(3)
        for k in far_first:
            last_copy(k, m).start()

    def order_weights(blocks, ranks):
        for k, block in enumerate(blocks):
            block = block.astype(f32)
            lines16[2 * k : 2 * k + 2] = block[0:2] + block[2:4]
        depths = lines16[...]
        prefixes = [
            jnp.sum(jnp.where(ranks < ranks[i : i + 1], depths, 0.0), axis=0, keepdims=True) for i in range(16)
        ]
        return [jnp.exp(-prefix) for prefix in prefixes]

    def combine(own, got):
        slots = [own] + [got.at[k - 1] for k in range(1, n_block)]
        factors = order_weights([slot[2 * FEAT :] for slot in slots], meta[:16])
        mixed = jnp.zeros((FEAT, 128), f32)
        for i in range(16):
            tint = slots[i // 2][i % 2 * FEAT : (i % 2 + 1) * FEAT]
            mixed = mixed + factors[i] * tint.astype(f32)
        return mixed

    def pass_copy(unit):
        target = me - 1 if unit % 2 == 0 else me + 1
        return pltpu.make_async_remote_copy(
            src_ref=passed.at[unit], dst_ref=passed_in.at[unit], send_sem=pass_send.at[unit],
            recv_sem=pass_recv.at[unit], device_id=(target, place), device_id_type=MESH,
        )

    def mine(unit):
        return me % 2 == unit // 2

    def has_target(unit):
        return mine(unit) & ((me > 0) if unit % 2 == 0 else (me < n_block - 1))

    def has_source(unit):
        return (me % 2 != unit // 2) & ((me < n_block - 1) if unit % 2 == 0 else (me > 0))

    for unit in range(3):

        @pl.when(mine(unit))
        def _():
            pltpu.make_async_copy(tiles_in.at[unit], tiles_in.at[unit], tile_recv.at[unit]).wait()
            passed[unit] = combine(tiles.at[unit, me // 2], tiles_in.at[unit]).astype(bf16)

        pl.when(has_target(unit))(pass_copy(unit).start)

        @pl.when(mine(unit))
        def _():
            window_out[1 + unit % 2] = passed[unit]

    for fetch in fetches[6:]:
        fetch.wait()
    prepare(w_conv, w_color, k0, k1, k2, k3, k4, place_rows, place_halo, weave)

    for k in range(1, n_block):
        for copy in halo_copies(k):
            copy.wait_recv()
    ranks = jnp.where(iota((16, 128), 1) < 64, meta_in[0, :16], meta_in[1, :16])
    factors = order_weights([halo_depth[...]] + [halo_depth_in[k - 1] for k in range(1, n_block)], ranks)
    for i in range(16):
        shares[i : i + 1] = factors[i]
    line = iota((32, 128), 0)
    row = line // 4 + 4 * me - 2
    source = jnp.where((row >= 0) & (row < 32), line // 2 % 2 * 64 + row * 2 + line % 2, -1)
    turn = (iota((32, 128), 1) == source).astype(f32).astype(bf16)
    high = shares[...].astype(bf16)
    low = (shares[...] - high.astype(f32)).astype(bf16)
    share = dot_nt(turn, high) + dot_nt(turn, low)
    mixed = jnp.zeros((32, 128), f32)
    for k in range(n_block):
        tint = halo[pl.ds(pl.multiple_of(16 * me, 16), 32), :] if k == 0 else halo_in[k - 1]
        factor = jnp.where(iota((32, 128), 1) < 64, share[:, 2 * k : 2 * k + 1], share[:, 2 * k + 1 : 2 * k + 2])
        mixed = mixed + factor * tint.astype(f32)
    halo_out[...] = (mixed + pltpu.roll(mixed, 64, 1)).astype(bf16)

    for unit in range(3):

        @pl.when(has_source(unit))
        def _():
            pass_copy(unit).wait_recv()
            window_out[3 - unit % 2 * 3] = passed_in[unit]

    @pl.when(me == n_block - 1)
    def _():
        window_out[3] = jnp.zeros((FEAT, 128), bf16)

    for m in range(2):
        for k in range(1, n_block):
            last_copy(k, m).wait_recv()
    mixed = combine(tiles.at[3, last_tile(me)], last_in)
    window_out[me % 2 * 2] = (mixed * jnp.where(me > 0, 1.0, 0.0)).astype(bf16)
    decode(
        n_block, n_patch, seam, window_out, halo_out, meta_in.at[0, pl.ds(16, 8)], out, k0, k1, k2, k4,
        place_rows, place_halo, weave, res,
    )

    for side in range(2):
        for copy in side_copies(side):
            pl.when(sides[side][1])(copy.wait_send)
    for k in range(1, n_block):
        for copy in halo_copies(k) + [last_copy(k, 0), last_copy(k, 1)]:
            copy.wait_send()
    for unit in range(3):
        pl.when(has_target(unit))(pass_copy(unit).wait_send)
        sent = pltpu.make_async_copy(tiles_in.at[unit, pl.ds(0, 3)], tiles_in.at[unit, pl.ds(0, 3)], tile_send.at[unit])
        more = pltpu.make_async_copy(tiles_in.at[unit, 3], tiles_in.at[unit, 3], tile_send.at[unit])
        sent.wait()
        pl.when(me % 2 != unit // 2)(more.wait)


def render(order, seam, x, w_in, w_mid, w_feat, w_dens, w_conv, w_color, n_block, n_patch):
    vmem = pl.BlockSpec(memory_space=pltpu.VMEM)
    smem = pl.BlockSpec(memory_space=pltpu.SMEM)
    dma = pltpu.SemaphoreType.DMA
    peers = n_block - 1
    rows = 2 * FEAT + 8
    return pl.pallas_call(
        functools.partial(field_kernel, n_block, n_patch),
        out_shape=pltpu.VMEM((3, 16, 256), f32),
        in_specs=[smem] + [pl.BlockSpec(memory_space=pl.ANY)] * 8,
        out_specs=vmem,
        scratch_shapes=[
            pltpu.SMEM(order.shape, jnp.int32),
            *[pltpu.VMEM(array.shape, bf16) for array in (x, w_in, w_mid, w_feat, w_dens, w_conv, w_color)],
            dma((8,)),
            pltpu.VMEM((4, FEAT, 128), bf16),
            pltpu.VMEM((32, 128), bf16),
            pltpu.VMEM((256, 576), bf16),
            pltpu.VMEM((256, 1024), bf16),
            pltpu.VMEM((4, FEAT, 256), bf16),
            pltpu.VMEM((288, 1024), f32),
            pltpu.VMEM((288, 1024), bf16),
            pltpu.VMEM((512, 640), bf16),
            pltpu.VMEM((32, 640), bf16),
            pltpu.VMEM((512, 256), bf16),
            pltpu.VMEM((2, 128, 128), f32),
            pltpu.VMEM((128, 1024), bf16),
            pltpu.VMEM((2, 1024, 128), bf16),
            pltpu.VMEM((2, WIDTH, WIDTH), bf16),
            pltpu.VMEM((2, WIDTH, WIDTH), bf16),
            pltpu.VMEM((2, FEAT + 16, WIDTH), bf16),
            pltpu.VMEM((2, 2, 64, 128), bf16),
            pltpu.VMEM((2, 2, 64, 128), bf16),
            pltpu.VMEM((24, 128), jnp.int32),
            pltpu.VMEM((2, 24, 128), jnp.int32),
            pltpu.VMEM((8, 512), f32),
            pltpu.VMEM((4, 4, rows, 128), bf16),
            pltpu.VMEM((3, peers, rows, 128), bf16),
            pltpu.VMEM((peers, rows, 128), bf16),
            pltpu.VMEM((3, FEAT, 128), bf16),
            pltpu.VMEM((3, FEAT, 128), bf16),
            pltpu.VMEM((144, 128), bf16),
            pltpu.VMEM((peers, 32, 128), bf16),
            pltpu.VMEM((8, 128), bf16),
            pltpu.VMEM((peers, 8, 128), bf16),
            pltpu.VMEM((16, 128), f32),
            pltpu.VMEM((16, 128), f32),
            dma((2,)), dma((2,)), dma((2,)), dma((2,)), dma((3,)), dma((3,)), dma((2, peers)), dma((2, peers)),
            dma((3,)), dma((3,)), dma((2, peers)), dma((2, peers)),
        ],
        compiler_params=pltpu.CompilerParams(collective_id=0, has_side_effects=True),
        name="field",
    )(seam, order, x, w_in, w_mid, w_feat, w_dens, w_conv, w_color)


def body(samples_in, block_order, seam_link, w_in, w_mid, w_feat, w_density, w_conv, w_color):
    n_block, n_patch = lax.axis_size("block"), lax.axis_size("patch")
    x = samples_in.reshape(2, RAYS // 128, 128, SAMP * ENC)
    return render(
        block_order, seam_link, x, w_in, w_mid, jnp.swapaxes(w_feat, 1, 2), w_density, w_conv, w_color, n_block, n_patch
    )


def solution(mesh):
    return jax.shard_map(
        body,
        mesh=mesh,
        in_specs=(
            P("block", None, "patch", None),
            P("patch", None),
            P("patch"),
            P("block", None, None),
            P("block", None, None, None),
            P("block", None, None),
            P("block", None),
            P(),
            P(),
        ),
        out_specs=P(None, "block", "patch"),
        check_vma=False,
    )
```

```python
import functools

import jax
import jax.numpy as jnp
from jax import lax
from jax.experimental import pallas as pl
from jax.experimental.pallas import tpu as pltpu
from jax.sharding import PartitionSpec as P

f32, bf16 = jnp.float32, jnp.bfloat16
MESH = pl.DeviceIdType.MESH

ENC = 32
SAMP = 4
STEP = 0.03
FEAT = 64
WIDTH = 256
COLS = 64
RAYS = 2048
PITCH = 68
SPAN = 512
ROLL = bf16


def iota(shape, dim):
    return lax.broadcasted_iota(jnp.int32, shape, dim)


def relu(x):
    return jnp.maximum(x, 0.0)


def dot(a, b):
    return jnp.dot(a, b, preferred_element_type=f32)


def dot_nt(a, b):
    return lax.dot_general(a, b, (((1,), (1,)), ((), ())), preferred_element_type=f32)


def field_chunks(streams):
    count = len(streams)
    hs = [relu(dot_nt(w1, x)).astype(bf16) for x, w1, w2, w3, head in streams]
    hs = [jnp.concatenate([h[WIDTH * s : WIDTH * (s + 1)] for s in range(SAMP)], axis=1) for h in hs]
    hs = [relu(dot(streams[i][2], hs[i])).astype(bf16) for i in range(count)]
    hs = [relu(dot(streams[i][3], hs[i])).astype(bf16) for i in range(count)]
    outs = [dot(streams[i][4], hs[i]) for i in range(count)]
    results = []
    for out in outs:
        rays = out.shape[1] // SAMP
        raw = out[FEAT : FEAT + 1]
        optical = STEP * (jnp.maximum(raw, 0.0) + jnp.log(1.0 + jnp.exp(-jnp.abs(raw))))
        total = jnp.zeros((1, rays), f32)
        colour = jnp.zeros((FEAT, rays), f32)
        for s in range(SAMP):
            here = optical[:, s * rays : (s + 1) * rays]
            weight = jnp.exp(-total) * (1.0 - jnp.exp(-here))
            total = total + here
            colour = colour + weight * out[:FEAT, s * rays : (s + 1) * rays]
        results.append((total, colour))
    return results


def phase_source(phase, tap):
    return (phase + tap - 1) // 2


def put(ref, row, col, value):
    ref[row : row + value.shape[0], col : col + value.shape[1]] = value


def enlarge_weights(ref, w_conv, layer):
    taps = [[w_conv[layer, a, e].astype(f32) for e in range(3)] for a in range(3)]
    for pa in range(2):
        for pb in range(2):
            for dr in range(-1, 2):
                for dc in range(-1, 2):
                    hits = [taps[a][e] for a in range(3) for e in range(3)
                            if phase_source(pa, a) == dr and phase_source(pb, e) == dc]
                    value = sum(hits[1:], hits[0]) if hits else jnp.zeros((FEAT, FEAT), f32)
                    put(ref, (2 * pa + pb) * FEAT, ((dr + 1) * 3 + dc + 1) * FEAT, value.astype(bf16))


def window_weights(ref, w_conv, layer):
    taps = [[w_conv[layer, a, e].astype(f32) for e in range(3)] for a in range(3)]
    for ua in range(2):
        for ub in range(2):
            for da in range(2):
                for db in range(2):
                    hits = [taps[a][e] for a in range(3) for e in range(3)
                            if phase_source(ua, a) == ua - 1 + da and phase_source(ub, e) == ub - 1 + db]
                    put(ref.at[2 * ua + ub], 0, (2 * da + db) * FEAT, sum(hits[1:], hits[0]).astype(bf16))


def dense_weights(ref, w_conv, layer):
    for qa in range(2):
        for qb in range(2):
            for s in range(-1, 3):
                for t in range(-1, 3):
                    a, e = s - qa + 1, t - qb + 1
                    inside = 0 <= a <= 2 and 0 <= e <= 2
                    value = w_conv[layer, a, e] if inside else jnp.zeros((FEAT, FEAT), bf16)
                    put(ref, (2 * qa + qb) * FEAT, ((s + 1) * 4 + t + 1) * FEAT, value)


def colour_weights(ref, w_conv, w_color, layer):
    ref[...] = jnp.zeros_like(ref)
    for a in range(3):
        for e in range(3):
            tint = dot(w_color[...], w_conv[layer, a, e])
            for i in range(4):
                for j in range(4):
                    group = (i - a + 2) * 6 + (j - e + 2)
                    cell = ((i // 2 * 2 + j // 2) * 2 + i % 2) * 2 + j % 2
                    put(ref, 8 * group, cell * FEAT, tint)


def moved(x, by):
    return pltpu.roll(x, (-by) % x.shape[1], 1) if by else x


def prepare(w_conv, w_color, k0, k1, k2, k3, k4, place, halo_place, weave):
    enlarge_weights(k0, w_conv, 0)
    dense_weights(k1, w_conv, 1)
    window_weights(k2, w_conv, 2)
    colour_weights(k3, w_conv, w_color, 3)
    k4[...] = k3[...].astype(bf16)
    source = iota(place.shape, 0)
    place[...] = (iota(place.shape, 1) == source // COLS * PITCH + source % COLS + 2).astype(f32).astype(bf16)
    source = iota(halo_place.shape, 0)
    target = source // 4 * PITCH + source % 2 + source // 2 % 2 * (COLS + 2)
    halo_place[...] = (iota(halo_place.shape, 1) == target).astype(f32).astype(bf16)
    source = iota(weave.shape, 0)
    target = jnp.where(source % 128 < COLS, 4 * (source % 128) + source // 128, -1)
    weave[...] = (iota(weave.shape, 1) == target).astype(f32).astype(bf16)


def decode(n_block, n_patch, seam, window, halo, link, out, k0, k1, k2, k4, place, halo_place, weave, res):
    me = lax.axis_index("block")
    column = lax.axis_index("patch")
    right_open = jnp.where(column < n_patch - 1, seam[0], 0).astype(f32)
    left_open = link[0:1, 0:1].astype(f32)

    def open_sides(lanes):
        at = iota((1, lanes), 1) % PITCH
        return jnp.where(at < 2, left_open, jnp.where(at < COLS + 2, 1.0, right_open))

    line = iota((1, SPAN), 1) // PITCH
    top = jnp.where(me > 0, 1.0, 0.0)
    bottom = jnp.where(me < n_block - 1, 1.0, 0.0)
    mask = jnp.where(line == 0, top, jnp.where(line < 5, 1.0, jnp.where(line == 5, bottom, 0.0))) * open_sides(SPAN)

    image = dot(jnp.concatenate([window[t] for t in range(4)], axis=1), place[...])
    image = image + dot(halo[...].astype(f32).T[:FEAT].astype(bf16), halo_place[...])
    image = (image * open_sides(image.shape[1])).astype(ROLL)
    patches = [
        moved(image, (dr + 1) * PITCH + dc)[:, :SPAN].astype(bf16) for dr in range(-1, 2) for dc in range(-1, 2)
    ]
    first = (relu(dot(k0[...], jnp.concatenate(patches, axis=0))) * mask).astype(ROLL)

    def views(maps):
        found = {}
        for s in range(-1, 3):
            for t in range(-1, 3):
                phase = (s % 2 * 2 + t % 2) * FEAT
                found[s, t] = moved(maps[phase : phase + FEAT], s // 2 * PITCH + t // 2).astype(bf16)
        return found

    cells = views(first)
    second = relu(dot(k1[...], jnp.concatenate([cells[s, t] for s in range(-1, 3) for t in range(-1, 3)], axis=0)))
    cells = views((second * mask).astype(ROLL))
    third = {}
    for wa in range(3):
        for wb in range(3):
            near = [cells[wa - 1 + da, wb - 1 + db] for da in range(2) for db in range(2)]
            users = [(ua, ub) for ua in range(2) for ub in range(2) if 0 <= wa - ua <= 1 and 0 <= wb - ub <= 1]
            kernels = jnp.concatenate([k2[2 * ua + ub] for ua, ub in users], axis=0)
            found = (relu(dot(kernels, jnp.concatenate(near, axis=0))) * mask).astype(bf16)
            for i, (ua, ub) in enumerate(users):
                third[wa - ua, wb - ub, ua, ub] = found[FEAT * i : FEAT * (i + 1)]
    parts = [third[key] for key in sorted(third)]
    spread = dot(k4[...], jnp.concatenate(parts, axis=0))

    def cell(i, j):
        group = (i + 1) * 6 + j + 1
        return spread[8 * group : 8 * group + 8]

    def row(i, j):
        value = cell(i, j)
        if i == 0:
            value = value + moved(cell(4, j), -PITCH)
        if i == 3:
            value = value + moved(cell(-1, j), PITCH)
        return value

    stack = []
    for i in range(4):
        cols = [row(i, j) for j in range(-1, 5)]
        middle = cols[1:5]
        middle[0] = middle[0] + moved(cols[5], -1)
        middle[3] = middle[3] + moved(cols[0], 1)
        stack.append(jnp.concatenate(middle, axis=0))
    stack = jnp.concatenate(stack, axis=0)
    starts = [(r + 1) * PITCH + 2 for r in range(4)]
    lines = [moved(stack[:, a // 128 * 128 : a // 128 * 128 + 256], a % 128)[:, :128] for a in starts[:3]]
    lines.append(moved(stack, starts[3])[:, :128])
    wide = jnp.concatenate(
        [
            jnp.concatenate([lines[r][8 * (4 * i + j) : 8 * (4 * i + j) + 8] for j in range(4)], axis=1)
            for r in range(4) for i in range(4)
        ],
        axis=0,
    )
    high = wide.astype(bf16)
    low = (wide - high.astype(f32)).astype(bf16)
    woven = dot(high, weave[...]) + dot(low, weave[...])
    for half in range(2):
        lanes = slice(128 * half, 128 * (half + 1))
        res[half] = woven[:, lanes]
        for k in range(3):
            out[k, :, lanes] = res[half, pl.ds(k, 16, stride=8), :]


def last_tile(device):
    return ((device + 1) // 2 + 3) % 4


def field_kernel(
    n_block, n_patch, seam, order_far, x_far, w_in_far, w_mid_far, w_feat_far, w_dens_far, w_conv_far, w_color_far, out,
    order, x, w_in, w_mid, w_feat, w_dens, w_conv, w_color, fetched,
    window_out, halo_out, k0, k1, k2, k3, k4, place_rows, place_halo, weave, res,
    spread, w1, w2, w3, head, rays_out, rays_in, meta, meta_in, depth_rows, tiles, tiles_in, last_in, passed, passed_in,
    halo, halo_in, halo_depth, halo_depth_in, lines16, shares,
    rays_send, rays_recv, meta_send, meta_recv, tile_send, tile_recv, last_send, last_recv, pass_send, pass_recv,
    halo_send, halo_recv,
):
    me = lax.axis_index("block")
    place = lax.axis_index("patch")
    far_first = sorted(range(1, n_block), key=lambda k: abs(k - n_block // 2))
    sides = ((place - 1, place > 0), (place + 1, place < n_patch - 1))
    pairs = (
        (w_in_far, w_in), (w_mid_far, w_mid), (w_feat_far, w_feat), (w_dens_far, w_dens), (x_far, x), (order_far, order),
        (w_conv_far, w_conv), (w_color_far, w_color),
    )
    fetches = [pltpu.make_async_copy(far, near, fetched.at[i]) for i, (far, near) in enumerate(pairs)]
    for fetch in fetches:
        fetch.start()
    rays_in[...] = jnp.zeros_like(rays_in)
    meta_in[...] = jnp.zeros_like(meta_in)
    barrier = pltpu.get_barrier_semaphore()
    for k in range(1, n_block):
        pl.semaphore_signal(barrier, inc=1, device_id=((me + k) % n_block, place), device_id_type=MESH)
    for side, there in sides:

        @pl.when(there)
        def _():
            pl.semaphore_signal(barrier, inc=1, device_id=(me, side), device_id_type=MESH)

    spread[...] = jnp.zeros_like(spread)
    for fetch in fetches[:4]:
        fetch.wait()
    for m in range(2):
        for s in range(SAMP):
            spread[ENC * s : ENC * (s + 1), WIDTH * s : WIDTH * (s + 1)] = w_in[m]
        w1[m] = spread[...].T
        w2[m] = w_mid[m, 0].T
        w3[m] = w_mid[m, 1].T
        head[m, :FEAT] = w_feat[m]
        head[m, FEAT:] = jnp.broadcast_to(w_dens[pl.ds(m, 1), :], (16, WIDTH))
    for fetch in fetches[4:6]:
        fetch.wait()
    line = iota((16, 256), 0)
    wanted = line % 8 // 2 * COLS + line % 2 + jnp.where(line >= 8, COLS - 2, 0)
    pick = (iota((16, 256), 1) == wanted).astype(f32).astype(bf16)
    for m in range(2):
        found = [dot(pick, x[m, 2 * g : 2 * g + 2].reshape(256, 128)) for g in range(8)]
        for side in range(2):
            rows = jnp.concatenate([f[8 * side : 8 * side + 8] for f in found], axis=0)
            rays_out[side, m] = rows.astype(bf16)
    slot = iota((16, 128), 0)
    member = 2 * ((me + n_block - slot // 2) % n_block) + slot % 2
    rank = jnp.zeros((16, 128), jnp.int32)
    for k in range(16):
        rank = jnp.where(member == order[0, k], k, rank)
    meta[:16] = rank
    meta[16:] = jnp.full((8, 128), jnp.where(place < n_patch - 1, seam[0], 0), jnp.int32)

    depth_rows[...] = jnp.zeros_like(depth_rows)

    def side_copies(side):
        target = (me, sides[side][0])
        return [
            pltpu.make_async_remote_copy(
                src_ref=rays_out.at[side], dst_ref=rays_in.at[1 - side], send_sem=rays_send.at[side],
                recv_sem=rays_recv.at[1 - side], device_id=target, device_id_type=MESH,
            ),
            pltpu.make_async_remote_copy(
                src_ref=meta, dst_ref=meta_in.at[1 - side], send_sem=meta_send.at[side],
                recv_sem=meta_recv.at[1 - side], device_id=target, device_id_type=MESH,
            ),
        ]

    count = (place > 0).astype(jnp.int32) + (place < n_patch - 1).astype(jnp.int32)
    pl.semaphore_wait(barrier, n_block - 1 + count)
    for side in range(2):
        for copy in side_copies(side):
            pl.when(sides[side][1])(copy.start)

    def weights(m):
        return w1[m], w2[m], w3[m], head[m]

    def depth_block(m, total):
        lanes = slice(0, total.shape[1])
        high = total.astype(bf16).astype(f32)
        depth_rows[m : m + 1, lanes] = high
        depth_rows[2 + m : 3 + m, lanes] = total - high

    def rays_of(unit, m):
        return jnp.concatenate([x[m, 4 * j + unit] for j in range(4)], axis=0)

    def keep(unit, m, tint):
        tint = tint.astype(bf16)
        for j in range(4):
            tiles[unit, j, FEAT * m : FEAT * (m + 1)] = tint[:, 128 * j : 128 * (j + 1)]

    def keep_depth(unit):
        rows = depth_rows[...].astype(bf16)
        for j in range(4):
            tiles[unit, j, 2 * FEAT :] = rows[:, 128 * j : 128 * (j + 1)]

    def store(unit, results):
        for m, (total, tint) in enumerate(results):
            keep(unit, m, tint)
            depth_block(m, total)
        keep_depth(unit)

    def send_owner(unit):
        for j in range(4):
            owner = 2 * j + unit // 2

            @pl.when(owner != me)
            def _():
                pltpu.make_async_remote_copy(
                    src_ref=tiles.at[unit, j], dst_ref=tiles_in.at[unit, (owner + n_block - me) % n_block - 1],
                    send_sem=tile_send.at[unit], recv_sem=tile_recv.at[unit],
                    device_id=(owner, place), device_id_type=MESH,
                ).start()

    def loop(unit, carry):
        store(unit, field_chunks([(rays_of(unit, m), *weights(m)) for m in range(2)]))
        send_owner(unit)
        return carry

    lax.fori_loop(0, 2, loop, 0)

    for side in range(2):
        for copy in side_copies(side):
            pl.when(sides[1 - side][1])(copy.wait_recv)
    results = field_chunks(
        [(rays_of(2, m), *weights(m)) for m in range(2)]
        + [(jnp.concatenate([rays_in[0, m], rays_in[1, m]], axis=0), *weights(m)) for m in range(2)]
    )
    store(2, results[:2])
    send_owner(2)
    results = results[2:]
    for m, (total, tint) in enumerate(results):
        depth_block(m, total)
    halo_depth[...] = depth_rows[:, :128].astype(bf16)
    ray = iota((144, 128), 0) - 8
    source = jnp.where((ray >= 0) & (ray < 128), ray // 2 % 2 * 64 + ray // 4 * 2 + ray % 2, -1)
    turn = (iota((144, 128), 1) == source).astype(f32).astype(bf16)
    both = jnp.concatenate([tint for total, tint in results], axis=0).astype(bf16)
    halo[...] = dot_nt(turn, both).astype(bf16)

    def halo_copies(k):
        peer = (me + k) % n_block
        return [
            pltpu.make_async_remote_copy(
                src_ref=halo.at[pl.ds(pl.multiple_of(16 * peer, 16), 32)], dst_ref=halo_in.at[k - 1],
                send_sem=halo_send.at[0, k - 1], recv_sem=halo_recv.at[0, k - 1],
                device_id=(peer, place), device_id_type=MESH,
            ),
            pltpu.make_async_remote_copy(
                src_ref=halo_depth, dst_ref=halo_depth_in.at[k - 1],
                send_sem=halo_send.at[1, k - 1], recv_sem=halo_recv.at[1, k - 1],
                device_id=(peer, place), device_id_type=MESH,
            ),
        ]

    for k in far_first:
        for copy in halo_copies(k):
            copy.start()

    def last_copy(k, m):
        peer = (me + k) % n_block
        rows = pl.ds(0, FEAT) if m == 0 else pl.ds(FEAT, FEAT + 8)
        return pltpu.make_async_remote_copy(
            src_ref=tiles.at[3, last_tile(peer), rows], dst_ref=last_in.at[k - 1, rows],
            send_sem=last_send.at[m, k - 1], recv_sem=last_recv.at[m, k - 1],
            device_id=(peer, place), device_id_type=MESH,
        )

    for m in range(2):
        ((total, tint),) = field_chunks([(rays_of(3, m), *weights(m))])
        keep(3, m, tint)
        depth_block(m, total)
        if m == 1:
            keep_depth(3)
        for k in far_first:
            last_copy(k, m).start()

    def order_weights(blocks, ranks):
        for k, block in enumerate(blocks):
            block = block.astype(f32)
            lines16[2 * k : 2 * k + 2] = block[0:2] + block[2:4]
        depths = lines16[...]
        prefixes = [
            jnp.sum(jnp.where(ranks < ranks[i : i + 1], depths, 0.0), axis=0, keepdims=True) for i in range(16)
        ]
        return [jnp.exp(-prefix) for prefix in prefixes]

    def combine(own, got):
        slots = [own] + [got.at[k - 1] for k in range(1, n_block)]
        factors = order_weights([slot[2 * FEAT :] for slot in slots], meta[:16])
        mixed = jnp.zeros((FEAT, 128), f32)
        for i in range(16):
            tint = slots[i // 2][i % 2 * FEAT : (i % 2 + 1) * FEAT]
            mixed = mixed + factors[i] * tint.astype(f32)
        return mixed

    def pass_copy(unit):
        target = me - 1 if unit % 2 == 0 else me + 1
        return pltpu.make_async_remote_copy(
            src_ref=passed.at[unit], dst_ref=passed_in.at[unit], send_sem=pass_send.at[unit],
            recv_sem=pass_recv.at[unit], device_id=(target, place), device_id_type=MESH,
        )

    def mine(unit):
        return me % 2 == unit // 2

    def has_target(unit):
        return mine(unit) & ((me > 0) if unit % 2 == 0 else (me < n_block - 1))

    def has_source(unit):
        return (me % 2 != unit // 2) & ((me < n_block - 1) if unit % 2 == 0 else (me > 0))

    for unit in range(3):

        @pl.when(mine(unit))
        def _():
            pltpu.make_async_copy(tiles_in.at[unit], tiles_in.at[unit], tile_recv.at[unit]).wait()
            passed[unit] = combine(tiles.at[unit, me // 2], tiles_in.at[unit]).astype(bf16)

        pl.when(has_target(unit))(pass_copy(unit).start)

        @pl.when(mine(unit))
        def _():
            window_out[1 + unit % 2] = passed[unit]

    for fetch in fetches[6:]:
        fetch.wait()
    prepare(w_conv, w_color, k0, k1, k2, k3, k4, place_rows, place_halo, weave)

    for k in range(1, n_block):
        for copy in halo_copies(k):
            copy.wait_recv()
    ranks = jnp.where(iota((16, 128), 1) < 64, meta_in[0, :16], meta_in[1, :16])
    factors = order_weights([halo_depth[...]] + [halo_depth_in[k - 1] for k in range(1, n_block)], ranks)
    for i in range(16):
        shares[i : i + 1] = factors[i]
    line = iota((32, 128), 0)
    row = line // 4 + 4 * me - 2
    source = jnp.where((row >= 0) & (row < 32), line // 2 % 2 * 64 + row * 2 + line % 2, -1)
    turn = (iota((32, 128), 1) == source).astype(f32).astype(bf16)
    high = shares[...].astype(bf16)
    low = (shares[...] - high.astype(f32)).astype(bf16)
    share = dot_nt(turn, high) + dot_nt(turn, low)
    mixed = jnp.zeros((32, 128), f32)
    for k in range(n_block):
        tint = halo[pl.ds(pl.multiple_of(16 * me, 16), 32), :] if k == 0 else halo_in[k - 1]
        factor = jnp.where(iota((32, 128), 1) < 64, share[:, 2 * k : 2 * k + 1], share[:, 2 * k + 1 : 2 * k + 2])
        mixed = mixed + factor * tint.astype(f32)
    halo_out[...] = (mixed + pltpu.roll(mixed, 64, 1)).astype(bf16)

    for unit in range(3):

        @pl.when(has_source(unit))
        def _():
            pass_copy(unit).wait_recv()
            window_out[3 - unit % 2 * 3] = passed_in[unit]

    @pl.when(me == n_block - 1)
    def _():
        window_out[3] = jnp.zeros((FEAT, 128), bf16)

    for side in range(2):
        for copy in side_copies(side):
            pl.when(sides[side][1])(copy.wait_send)
    for k in range(1, n_block):
        for copy in halo_copies(k) + [last_copy(k, 0), last_copy(k, 1)]:
            copy.wait_send()
    for unit in range(3):
        pl.when(has_target(unit))(pass_copy(unit).wait_send)
        sent = pltpu.make_async_copy(tiles_in.at[unit, pl.ds(0, 3)], tiles_in.at[unit, pl.ds(0, 3)], tile_send.at[unit])
        more = pltpu.make_async_copy(tiles_in.at[unit, 3], tiles_in.at[unit, 3], tile_send.at[unit])
        sent.wait()
        pl.when(me % 2 != unit // 2)(more.wait)

    for m in range(2):
        for k in range(1, n_block):
            last_copy(k, m).wait_recv()
    mixed = combine(tiles.at[3, last_tile(me)], last_in)
    window_out[me % 2 * 2] = (mixed * jnp.where(me > 0, 1.0, 0.0)).astype(bf16)
    decode(
        n_block, n_patch, seam, window_out, halo_out, meta_in.at[0, pl.ds(16, 8)], out, k0, k1, k2, k4,
        place_rows, place_halo, weave, res,
    )


def render(order, seam, x, w_in, w_mid, w_feat, w_dens, w_conv, w_color, n_block, n_patch):
    vmem = pl.BlockSpec(memory_space=pltpu.VMEM)
    smem = pl.BlockSpec(memory_space=pltpu.SMEM)
    dma = pltpu.SemaphoreType.DMA
    peers = n_block - 1
    rows = 2 * FEAT + 8
    return pl.pallas_call(
        functools.partial(field_kernel, n_block, n_patch),
        out_shape=pltpu.VMEM((3, 16, 256), f32),
        in_specs=[smem] + [pl.BlockSpec(memory_space=pl.ANY)] * 8,
        out_specs=vmem,
        scratch_shapes=[
            pltpu.SMEM(order.shape, jnp.int32),
            *[pltpu.VMEM(array.shape, bf16) for array in (x, w_in, w_mid, w_feat, w_dens, w_conv, w_color)],
            dma((8,)),
            pltpu.VMEM((4, FEAT, 128), bf16),
            pltpu.VMEM((32, 128), bf16),
            pltpu.VMEM((256, 576), bf16),
            pltpu.VMEM((256, 1024), bf16),
            pltpu.VMEM((4, FEAT, 256), bf16),
            pltpu.VMEM((288, 1024), f32),
            pltpu.VMEM((288, 1024), bf16),
            pltpu.VMEM((512, 640), bf16),
            pltpu.VMEM((32, 640), bf16),
            pltpu.VMEM((512, 256), bf16),
            pltpu.VMEM((2, 128, 128), f32),
            pltpu.VMEM((128, 1024), bf16),
            pltpu.VMEM((2, 1024, 128), bf16),
            pltpu.VMEM((2, WIDTH, WIDTH), bf16),
            pltpu.VMEM((2, WIDTH, WIDTH), bf16),
            pltpu.VMEM((2, FEAT + 16, WIDTH), bf16),
            pltpu.VMEM((2, 2, 64, 128), bf16),
            pltpu.VMEM((2, 2, 64, 128), bf16),
            pltpu.VMEM((24, 128), jnp.int32),
            pltpu.VMEM((2, 24, 128), jnp.int32),
            pltpu.VMEM((8, 512), f32),
            pltpu.VMEM((4, 4, rows, 128), bf16),
            pltpu.VMEM((3, peers, rows, 128), bf16),
            pltpu.VMEM((peers, rows, 128), bf16),
            pltpu.VMEM((3, FEAT, 128), bf16),
            pltpu.VMEM((3, FEAT, 128), bf16),
            pltpu.VMEM((144, 128), bf16),
            pltpu.VMEM((peers, 32, 128), bf16),
            pltpu.VMEM((8, 128), bf16),
            pltpu.VMEM((peers, 8, 128), bf16),
            pltpu.VMEM((16, 128), f32),
            pltpu.VMEM((16, 128), f32),
            dma((2,)), dma((2,)), dma((2,)), dma((2,)), dma((3,)), dma((3,)), dma((2, peers)), dma((2, peers)),
            dma((3,)), dma((3,)), dma((2, peers)), dma((2, peers)),
        ],
        compiler_params=pltpu.CompilerParams(collective_id=0, has_side_effects=True),
        name="field",
    )(seam, order, x, w_in, w_mid, w_feat, w_dens, w_conv, w_color)


def body(samples_in, block_order, seam_link, w_in, w_mid, w_feat, w_density, w_conv, w_color):
    n_block, n_patch = lax.axis_size("block"), lax.axis_size("patch")
    x = samples_in.reshape(2, RAYS // 128, 128, SAMP * ENC)
    return render(
        block_order, seam_link, x, w_in, w_mid, jnp.swapaxes(w_feat, 1, 2), w_density, w_conv, w_color, n_block, n_patch
    )


def solution(mesh):
    return jax.shard_map(
        body,
        mesh=mesh,
        in_specs=(
            P("block", None, "patch", None),
            P("patch", None),
            P("patch"),
            P("block", None, None),
            P("block", None, None, None),
            P("block", None, None),
            P("block", None),
            P(),
            P(),
        ),
        out_specs=P(None, "block", "patch"),
        check_vma=False,
    )
```

```python
import functools

import jax
import jax.numpy as jnp
from jax import lax
from jax.experimental import pallas as pl
from jax.experimental.pallas import tpu as pltpu
from jax.sharding import PartitionSpec as P

f32, bf16 = jnp.float32, jnp.bfloat16
MESH = pl.DeviceIdType.MESH

ENC = 32
SAMP = 4
STEP = 0.03
FEAT = 64
WIDTH = 256
COLS = 64
RAYS = 2048
PITCH = 68
SPAN = 512
ROLL = bf16


def iota(shape, dim):
    return lax.broadcasted_iota(jnp.int32, shape, dim)


def relu(x):
    return jnp.maximum(x, 0.0)


def dot(a, b):
    return jnp.dot(a, b, preferred_element_type=f32)


def dot_nt(a, b):
    return lax.dot_general(a, b, (((1,), (1,)), ((), ())), preferred_element_type=f32)


def field_chunks(streams):
    count = len(streams)
    hs = [relu(dot_nt(w1, x)).astype(bf16) for x, w1, w2, w3, head in streams]
    hs = [jnp.concatenate([h[WIDTH * s : WIDTH * (s + 1)] for s in range(SAMP)], axis=1) for h in hs]
    hs = [relu(dot(streams[i][2], hs[i])).astype(bf16) for i in range(count)]
    hs = [relu(dot(streams[i][3], hs[i])).astype(bf16) for i in range(count)]
    outs = [dot(streams[i][4], hs[i]) for i in range(count)]
    results = []
    for out in outs:
        rays = out.shape[1] // SAMP
        raw = out[FEAT : FEAT + 1]
        optical = STEP * (jnp.maximum(raw, 0.0) + jnp.log(1.0 + jnp.exp(-jnp.abs(raw))))
        total = jnp.zeros((1, rays), f32)
        colour = jnp.zeros((FEAT, rays), f32)
        for s in range(SAMP):
            here = optical[:, s * rays : (s + 1) * rays]
            weight = jnp.exp(-total) * (1.0 - jnp.exp(-here))
            total = total + here
            colour = colour + weight * out[:FEAT, s * rays : (s + 1) * rays]
        results.append((total, colour))
    return results


def phase_source(phase, tap):
    return (phase + tap - 1) // 2


def put(ref, row, col, value):
    ref[row : row + value.shape[0], col : col + value.shape[1]] = value


def enlarge_weights(ref, w_conv, layer):
    taps = [[w_conv[layer, a, e].astype(f32) for e in range(3)] for a in range(3)]
    for pa in range(2):
        for pb in range(2):
            for dr in range(-1, 2):
                for dc in range(-1, 2):
                    hits = [taps[a][e] for a in range(3) for e in range(3)
                            if phase_source(pa, a) == dr and phase_source(pb, e) == dc]
                    value = sum(hits[1:], hits[0]) if hits else jnp.zeros((FEAT, FEAT), f32)
                    put(ref, (2 * pa + pb) * FEAT, ((dr + 1) * 3 + dc + 1) * FEAT, value.astype(bf16))


def window_weights(ref, w_conv, layer):
    taps = [[w_conv[layer, a, e].astype(f32) for e in range(3)] for a in range(3)]
    for ua in range(2):
        for ub in range(2):
            for da in range(2):
                for db in range(2):
                    hits = [taps[a][e] for a in range(3) for e in range(3)
                            if phase_source(ua, a) == ua - 1 + da and phase_source(ub, e) == ub - 1 + db]
                    put(ref.at[2 * ua + ub], 0, (2 * da + db) * FEAT, sum(hits[1:], hits[0]).astype(bf16))


def dense_weights(ref, w_conv, layer):
    for qa in range(2):
        for qb in range(2):
            for s in range(-1, 3):
                for t in range(-1, 3):
                    a, e = s - qa + 1, t - qb + 1
                    inside = 0 <= a <= 2 and 0 <= e <= 2
                    value = w_conv[layer, a, e] if inside else jnp.zeros((FEAT, FEAT), bf16)
                    put(ref, (2 * qa + qb) * FEAT, ((s + 1) * 4 + t + 1) * FEAT, value)


def colour_weights(ref, w_conv, w_color, layer):
    ref[...] = jnp.zeros_like(ref)
    for a in range(3):
        for e in range(3):
            tint = dot(w_color[...], w_conv[layer, a, e])
            for i in range(4):
                for j in range(4):
                    group = (i - a + 2) * 6 + (j - e + 2)
                    cell = ((i // 2 * 2 + j // 2) * 2 + i % 2) * 2 + j % 2
                    put(ref, 8 * group, cell * FEAT, tint)


def moved(x, by):
    return pltpu.roll(x, (-by) % x.shape[1], 1) if by else x


def prepare(w_conv, w_color, k0, k1, k2, k3, k4, place, halo_place, weave):
    enlarge_weights(k0, w_conv, 0)
    dense_weights(k1, w_conv, 1)
    window_weights(k2, w_conv, 2)
    colour_weights(k3, w_conv, w_color, 3)
    k4[...] = k3[...].astype(bf16)
    source = iota(place.shape, 0)
    place[...] = (iota(place.shape, 1) == source // COLS * PITCH + source % COLS + 2).astype(f32).astype(bf16)
    source = iota(halo_place.shape, 0)
    target = source // 4 * PITCH + source % 2 + source // 2 % 2 * (COLS + 2)
    halo_place[...] = (iota(halo_place.shape, 1) == target).astype(f32).astype(bf16)
    source = iota(weave.shape, 0)
    target = jnp.where(source % 128 < COLS, 4 * (source % 128) + source // 128, -1)
    weave[...] = (iota(weave.shape, 1) == target).astype(f32).astype(bf16)


def decode(n_block, n_patch, seam, window, halo, link, out, k0, k1, k2, k4, place, halo_place, weave, res):
    me = lax.axis_index("block")
    column = lax.axis_index("patch")
    right_open = jnp.where(column < n_patch - 1, seam[0], 0).astype(f32)
    left_open = link[0:1, 0:1].astype(f32)

    def open_sides(lanes):
        at = iota((1, lanes), 1) % PITCH
        return jnp.where(at < 2, left_open, jnp.where(at < COLS + 2, 1.0, right_open))

    line = iota((1, SPAN), 1) // PITCH
    top = jnp.where(me > 0, 1.0, 0.0)
    bottom = jnp.where(me < n_block - 1, 1.0, 0.0)
    mask = jnp.where(line == 0, top, jnp.where(line < 5, 1.0, jnp.where(line == 5, bottom, 0.0))) * open_sides(SPAN)

    image = dot(jnp.concatenate([window[t] for t in range(4)], axis=1), place[...])
    image = image + dot(halo[...].astype(f32).T[:FEAT].astype(bf16), halo_place[...])
    image = (image * open_sides(image.shape[1])).astype(ROLL)
    patches = [
        moved(image, (dr + 1) * PITCH + dc)[:, :SPAN].astype(bf16) for dr in range(-1, 2) for dc in range(-1, 2)
    ]
    first = (relu(dot(k0[...], jnp.concatenate(patches, axis=0))) * mask).astype(ROLL)

    def views(maps):
        found = {}
        for s in range(-1, 3):
            for t in range(-1, 3):
                phase = (s % 2 * 2 + t % 2) * FEAT
                found[s, t] = moved(maps[phase : phase + FEAT], s // 2 * PITCH + t // 2).astype(bf16)
        return found

    cells = views(first)
    second = relu(dot(k1[...], jnp.concatenate([cells[s, t] for s in range(-1, 3) for t in range(-1, 3)], axis=0)))
    cells = views((second * mask).astype(ROLL))
    third = {}
    for wa in range(3):
        for wb in range(3):
            near = [cells[wa - 1 + da, wb - 1 + db] for da in range(2) for db in range(2)]
            users = [(ua, ub) for ua in range(2) for ub in range(2) if 0 <= wa - ua <= 1 and 0 <= wb - ub <= 1]
            kernels = jnp.concatenate([k2[2 * ua + ub] for ua, ub in users], axis=0)
            found = (relu(dot(kernels, jnp.concatenate(near, axis=0))) * mask).astype(bf16)
            for i, (ua, ub) in enumerate(users):
                third[wa - ua, wb - ub, ua, ub] = found[FEAT * i : FEAT * (i + 1)]
    parts = [third[key] for key in sorted(third)]
    spread = dot(k4[...], jnp.concatenate(parts, axis=0))

    def cell(i, j):
        group = (i + 1) * 6 + j + 1
        return spread[8 * group : 8 * group + 8]

    def row(i, j):
        value = cell(i, j)
        if i == 0:
            value = value + moved(cell(4, j), -PITCH)
        if i == 3:
            value = value + moved(cell(-1, j), PITCH)
        return value

    stack = []
    for i in range(4):
        cols = [row(i, j) for j in range(-1, 5)]
        middle = cols[1:5]
        middle[0] = middle[0] + moved(cols[5], -1)
        middle[3] = middle[3] + moved(cols[0], 1)
        stack.append(jnp.concatenate(middle, axis=0))
    stack = jnp.concatenate(stack, axis=0)
    starts = [(r + 1) * PITCH + 2 for r in range(4)]
    lines = [moved(stack[:, a // 128 * 128 : a // 128 * 128 + 256], a % 128)[:, :128] for a in starts[:3]]
    lines.append(moved(stack, starts[3])[:, :128])
    wide = jnp.concatenate(
        [
            jnp.concatenate([lines[r][8 * (4 * i + j) : 8 * (4 * i + j) + 8] for j in range(4)], axis=1)
            for r in range(4) for i in range(4)
        ],
        axis=0,
    )
    high = wide.astype(bf16)
    low = (wide - high.astype(f32)).astype(bf16)
    woven = dot(high, weave[...]) + dot(low, weave[...])
    for half in range(2):
        lanes = slice(128 * half, 128 * (half + 1))
        res[half] = woven[:, lanes]
        for k in range(3):
            out[k, :, lanes] = res[half, pl.ds(k, 16, stride=8), :]


def last_tile(device):
    return ((device + 1) // 2 + 3) % 4


def field_kernel(
    n_block, n_patch, seam, order_far, x_far, w_in_far, w_mid_far, w_feat_far, w_dens_far, w_conv_far, w_color_far, out,
    order, x, w_in, w_mid, w_feat, w_dens, w_conv, w_color, fetched,
    window_out, halo_out, k0, k1, k2, k3, k4, place_rows, place_halo, weave, res,
    spread, w1, w2, w3, head, rays_out, rays_in, meta, meta_in, depth_rows, tiles, tiles_in, last_in, passed, passed_in,
    halo, halo_in, halo_depth, halo_depth_in, lines16, shares,
    rays_send, rays_recv, meta_send, meta_recv, tile_send, tile_recv, last_send, last_recv, pass_send, pass_recv,
    halo_send, halo_recv,
):
    me = lax.axis_index("block")
    place = lax.axis_index("patch")
    far_first = sorted(range(1, n_block), key=lambda k: abs(k - n_block // 2))
    sides = ((place - 1, place > 0), (place + 1, place < n_patch - 1))
    pairs = (
        (w_in_far, w_in), (w_mid_far, w_mid), (w_feat_far, w_feat), (w_dens_far, w_dens), (x_far, x), (order_far, order),
        (w_conv_far, w_conv), (w_color_far, w_color),
    )
    fetches = [pltpu.make_async_copy(far, near, fetched.at[i]) for i, (far, near) in enumerate(pairs)]
    for fetch in fetches:
        fetch.start()
    rays_in[...] = jnp.zeros_like(rays_in)
    meta_in[...] = jnp.zeros_like(meta_in)
    barrier = pltpu.get_barrier_semaphore()
    for k in range(1, n_block):
        pl.semaphore_signal(barrier, inc=1, device_id=((me + k) % n_block, place), device_id_type=MESH)
    for side, there in sides:

        @pl.when(there)
        def _():
            pl.semaphore_signal(barrier, inc=1, device_id=(me, side), device_id_type=MESH)

    spread[...] = jnp.zeros_like(spread)
    for fetch in fetches[:4]:
        fetch.wait()
    for m in range(2):
        for s in range(SAMP):
            spread[ENC * s : ENC * (s + 1), WIDTH * s : WIDTH * (s + 1)] = w_in[m]
        w1[m] = spread[...].T
        w2[m] = w_mid[m, 0].T
        w3[m] = w_mid[m, 1].T
        head[m, :FEAT] = w_feat[m]
        head[m, FEAT:] = jnp.broadcast_to(w_dens[pl.ds(m, 1), :], (16, WIDTH))
    for fetch in fetches[4:6]:
        fetch.wait()
    line = iota((16, 256), 0)
    wanted = line % 8 // 2 * COLS + line % 2 + jnp.where(line >= 8, COLS - 2, 0)
    pick = (iota((16, 256), 1) == wanted).astype(f32).astype(bf16)
    for m in range(2):
        found = [dot(pick, x[m, 2 * g : 2 * g + 2].reshape(256, 128)) for g in range(8)]
        for side in range(2):
            rows = jnp.concatenate([f[8 * side : 8 * side + 8] for f in found], axis=0)
            rays_out[side, m] = rows.astype(bf16)
    slot = iota((16, 128), 0)
    member = 2 * ((me + n_block - slot // 2) % n_block) + slot % 2
    rank = jnp.zeros((16, 128), jnp.int32)
    for k in range(16):
        rank = jnp.where(member == order[0, k], k, rank)
    meta[:16] = rank
    meta[16:] = jnp.full((8, 128), jnp.where(place < n_patch - 1, seam[0], 0), jnp.int32)

    depth_rows[...] = jnp.zeros_like(depth_rows)

    def side_copies(side):
        target = (me, sides[side][0])
        return [
            pltpu.make_async_remote_copy(
                src_ref=rays_out.at[side], dst_ref=rays_in.at[1 - side], send_sem=rays_send.at[side],
                recv_sem=rays_recv.at[1 - side], device_id=target, device_id_type=MESH,
            ),
            pltpu.make_async_remote_copy(
                src_ref=meta, dst_ref=meta_in.at[1 - side], send_sem=meta_send.at[side],
                recv_sem=meta_recv.at[1 - side], device_id=target, device_id_type=MESH,
            ),
        ]

    count = (place > 0).astype(jnp.int32) + (place < n_patch - 1).astype(jnp.int32)
    pl.semaphore_wait(barrier, n_block - 1 + count)
    for side in range(2):
        for copy in side_copies(side):
            pl.when(sides[side][1])(copy.start)

    def weights(m):
        return w1[m], w2[m], w3[m], head[m]

    def depth_block(m, total):
        lanes = slice(0, total.shape[1])
        high = total.astype(bf16).astype(f32)
        depth_rows[m : m + 1, lanes] = high
        depth_rows[2 + m : 3 + m, lanes] = total - high

    def rays_of(unit, m):
        return jnp.concatenate([x[m, 4 * j + unit] for j in range(4)], axis=0)

    def keep(unit, m, tint):
        tint = tint.astype(bf16)
        for j in range(4):
            tiles[unit, j, FEAT * m : FEAT * (m + 1)] = tint[:, 128 * j : 128 * (j + 1)]

    def keep_depth(unit):
        rows = depth_rows[...].astype(bf16)
        for j in range(4):
            tiles[unit, j, 2 * FEAT :] = rows[:, 128 * j : 128 * (j + 1)]

    def store(unit, results):
        for m, (total, tint) in enumerate(results):
            keep(unit, m, tint)
            depth_block(m, total)
        keep_depth(unit)

    def send_owner(unit):
        for j in range(4):
            owner = 2 * j + unit // 2

            @pl.when(owner != me)
            def _():
                pltpu.make_async_remote_copy(
                    src_ref=tiles.at[unit, j], dst_ref=tiles_in.at[unit, (owner + n_block - me) % n_block - 1],
                    send_sem=tile_send.at[unit], recv_sem=tile_recv.at[unit],
                    device_id=(owner, place), device_id_type=MESH,
                ).start()

    def loop(unit, carry):
        store(unit, field_chunks([(rays_of(unit, m), *weights(m)) for m in range(2)]))
        send_owner(unit)
        return carry

    lax.fori_loop(0, 2, loop, 0)

    for side in range(2):
        for copy in side_copies(side):
            pl.when(sides[1 - side][1])(copy.wait_recv)
    results = field_chunks(
        [(rays_of(2, m), *weights(m)) for m in range(2)]
        + [(jnp.concatenate([rays_in[0, m], rays_in[1, m]], axis=0), *weights(m)) for m in range(2)]
    )
    store(2, results[:2])
    send_owner(2)
    results = results[2:]
    for m, (total, tint) in enumerate(results):
        depth_block(m, total)
    halo_depth[...] = depth_rows[:, :128].astype(bf16)
    ray = iota((144, 128), 0) - 8
    source = jnp.where((ray >= 0) & (ray < 128), ray // 2 % 2 * 64 + ray // 4 * 2 + ray % 2, -1)
    turn = (iota((144, 128), 1) == source).astype(f32).astype(bf16)
    both = jnp.concatenate([tint for total, tint in results], axis=0).astype(bf16)
    halo[...] = dot_nt(turn, both).astype(bf16)

    def halo_copies(k):
        peer = (me + k) % n_block
        return [
            pltpu.make_async_remote_copy(
                src_ref=halo.at[pl.ds(pl.multiple_of(16 * peer, 16), 32)], dst_ref=halo_in.at[k - 1],
                send_sem=halo_send.at[0, k - 1], recv_sem=halo_recv.at[0, k - 1],
                device_id=(peer, place), device_id_type=MESH,
            ),
            pltpu.make_async_remote_copy(
                src_ref=halo_depth, dst_ref=halo_depth_in.at[k - 1],
                send_sem=halo_send.at[1, k - 1], recv_sem=halo_recv.at[1, k - 1],
                device_id=(peer, place), device_id_type=MESH,
            ),
        ]

    for k in far_first:
        for copy in halo_copies(k):
            copy.start()

    def last_copy(k, m):
        peer = (me + k) % n_block
        rows = pl.ds(0, FEAT) if m == 0 else pl.ds(FEAT, FEAT + 8)
        return pltpu.make_async_remote_copy(
            src_ref=tiles.at[3, last_tile(peer), rows], dst_ref=last_in.at[k - 1, rows],
            send_sem=last_send.at[m, k - 1], recv_sem=last_recv.at[m, k - 1],
            device_id=(peer, place), device_id_type=MESH,
        )

    for m in range(2):
        ((total, tint),) = field_chunks([(rays_of(3, m), *weights(m))])
        keep(3, m, tint)
        depth_block(m, total)
        if m == 1:
            keep_depth(3)
        for k in far_first:
            last_copy(k, m).start()

    def order_weights(blocks, ranks):
        for k, block in enumerate(blocks):
            block = block.astype(f32)
            lines16[2 * k : 2 * k + 2] = block[0:2] + block[2:4]
        depths = lines16[...]
        prefixes = [
            jnp.sum(jnp.where(ranks < ranks[i : i + 1], depths, 0.0), axis=0, keepdims=True) for i in range(16)
        ]
        return [jnp.exp(-prefix) for prefix in prefixes]

    def combine(own, got):
        slots = [own] + [got.at[k - 1] for k in range(1, n_block)]
        factors = order_weights([slot[2 * FEAT :] for slot in slots], meta[:16])
        mixed = jnp.zeros((FEAT, 128), f32)
        for i in range(16):
            tint = slots[i // 2][i % 2 * FEAT : (i % 2 + 1) * FEAT]
            mixed = mixed + factors[i] * tint.astype(f32)
        return mixed

    def pass_copy(unit):
        target = me - 1 if unit % 2 == 0 else me + 1
        return pltpu.make_async_remote_copy(
            src_ref=passed.at[unit], dst_ref=passed_in.at[unit], send_sem=pass_send.at[unit],
            recv_sem=pass_recv.at[unit], device_id=(target, place), device_id_type=MESH,
        )

    def mine(unit):
        return me % 2 == unit // 2

    def has_target(unit):
        return mine(unit) & ((me > 0) if unit % 2 == 0 else (me < n_block - 1))

    def has_source(unit):
        return (me % 2 != unit // 2) & ((me < n_block - 1) if unit % 2 == 0 else (me > 0))

    for unit in range(3):
        if unit == 2:
            for fetch in fetches[6:]:
                fetch.wait()
            prepare(w_conv, w_color, k0, k1, k2, k3, k4, place_rows, place_halo, weave)

        @pl.when(mine(unit))
        def _():
            pltpu.make_async_copy(tiles_in.at[unit], tiles_in.at[unit], tile_recv.at[unit]).wait()
            passed[unit] = combine(tiles.at[unit, me // 2], tiles_in.at[unit]).astype(bf16)

        pl.when(has_target(unit))(pass_copy(unit).start)

        @pl.when(mine(unit))
        def _():
            window_out[1 + unit % 2] = passed[unit]


    for k in range(1, n_block):
        for copy in halo_copies(k):
            copy.wait_recv()
    ranks = jnp.where(iota((16, 128), 1) < 64, meta_in[0, :16], meta_in[1, :16])
    factors = order_weights([halo_depth[...]] + [halo_depth_in[k - 1] for k in range(1, n_block)], ranks)
    for i in range(16):
        shares[i : i + 1] = factors[i]
    line = iota((32, 128), 0)
    row = line // 4 + 4 * me - 2
    source = jnp.where((row >= 0) & (row < 32), line // 2 % 2 * 64 + row * 2 + line % 2, -1)
    turn = (iota((32, 128), 1) == source).astype(f32).astype(bf16)
    high = shares[...].astype(bf16)
    low = (shares[...] - high.astype(f32)).astype(bf16)
    share = dot_nt(turn, high) + dot_nt(turn, low)
    mixed = jnp.zeros((32, 128), f32)
    for k in range(n_block):
        tint = halo[pl.ds(pl.multiple_of(16 * me, 16), 32), :] if k == 0 else halo_in[k - 1]
        factor = jnp.where(iota((32, 128), 1) < 64, share[:, 2 * k : 2 * k + 1], share[:, 2 * k + 1 : 2 * k + 2])
        mixed = mixed + factor * tint.astype(f32)
    halo_out[...] = (mixed + pltpu.roll(mixed, 64, 1)).astype(bf16)

    for unit in range(3):

        @pl.when(has_source(unit))
        def _():
            pass_copy(unit).wait_recv()
            window_out[3 - unit % 2 * 3] = passed_in[unit]

    @pl.when(me == n_block - 1)
    def _():
        window_out[3] = jnp.zeros((FEAT, 128), bf16)

    for side in range(2):
        for copy in side_copies(side):
            pl.when(sides[side][1])(copy.wait_send)
    for k in range(1, n_block):
        for copy in halo_copies(k) + [last_copy(k, 0), last_copy(k, 1)]:
            copy.wait_send()
    for unit in range(3):
        pl.when(has_target(unit))(pass_copy(unit).wait_send)
        sent = pltpu.make_async_copy(tiles_in.at[unit, pl.ds(0, 3)], tiles_in.at[unit, pl.ds(0, 3)], tile_send.at[unit])
        more = pltpu.make_async_copy(tiles_in.at[unit, 3], tiles_in.at[unit, 3], tile_send.at[unit])
        sent.wait()
        pl.when(me % 2 != unit // 2)(more.wait)

    for m in range(2):
        for k in range(1, n_block):
            last_copy(k, m).wait_recv()
    mixed = combine(tiles.at[3, last_tile(me)], last_in)
    window_out[me % 2 * 2] = (mixed * jnp.where(me > 0, 1.0, 0.0)).astype(bf16)
    decode(
        n_block, n_patch, seam, window_out, halo_out, meta_in.at[0, pl.ds(16, 8)], out, k0, k1, k2, k4,
        place_rows, place_halo, weave, res,
    )


def render(order, seam, x, w_in, w_mid, w_feat, w_dens, w_conv, w_color, n_block, n_patch):
    vmem = pl.BlockSpec(memory_space=pltpu.VMEM)
    smem = pl.BlockSpec(memory_space=pltpu.SMEM)
    dma = pltpu.SemaphoreType.DMA
    peers = n_block - 1
    rows = 2 * FEAT + 8
    return pl.pallas_call(
        functools.partial(field_kernel, n_block, n_patch),
        out_shape=pltpu.VMEM((3, 16, 256), f32),
        in_specs=[smem] + [pl.BlockSpec(memory_space=pl.ANY)] * 8,
        out_specs=vmem,
        scratch_shapes=[
            pltpu.SMEM(order.shape, jnp.int32),
            *[pltpu.VMEM(array.shape, bf16) for array in (x, w_in, w_mid, w_feat, w_dens, w_conv, w_color)],
            dma((8,)),
            pltpu.VMEM((4, FEAT, 128), bf16),
            pltpu.VMEM((32, 128), bf16),
            pltpu.VMEM((256, 576), bf16),
            pltpu.VMEM((256, 1024), bf16),
            pltpu.VMEM((4, FEAT, 256), bf16),
            pltpu.VMEM((288, 1024), f32),
            pltpu.VMEM((288, 1024), bf16),
            pltpu.VMEM((512, 640), bf16),
            pltpu.VMEM((32, 640), bf16),
            pltpu.VMEM((512, 256), bf16),
            pltpu.VMEM((2, 128, 128), f32),
            pltpu.VMEM((128, 1024), bf16),
            pltpu.VMEM((2, 1024, 128), bf16),
            pltpu.VMEM((2, WIDTH, WIDTH), bf16),
            pltpu.VMEM((2, WIDTH, WIDTH), bf16),
            pltpu.VMEM((2, FEAT + 16, WIDTH), bf16),
            pltpu.VMEM((2, 2, 64, 128), bf16),
            pltpu.VMEM((2, 2, 64, 128), bf16),
            pltpu.VMEM((24, 128), jnp.int32),
            pltpu.VMEM((2, 24, 128), jnp.int32),
            pltpu.VMEM((8, 512), f32),
            pltpu.VMEM((4, 4, rows, 128), bf16),
            pltpu.VMEM((3, peers, rows, 128), bf16),
            pltpu.VMEM((peers, rows, 128), bf16),
            pltpu.VMEM((3, FEAT, 128), bf16),
            pltpu.VMEM((3, FEAT, 128), bf16),
            pltpu.VMEM((144, 128), bf16),
            pltpu.VMEM((peers, 32, 128), bf16),
            pltpu.VMEM((8, 128), bf16),
            pltpu.VMEM((peers, 8, 128), bf16),
            pltpu.VMEM((16, 128), f32),
            pltpu.VMEM((16, 128), f32),
            dma((2,)), dma((2,)), dma((2,)), dma((2,)), dma((3,)), dma((3,)), dma((2, peers)), dma((2, peers)),
            dma((3,)), dma((3,)), dma((2, peers)), dma((2, peers)),
        ],
        compiler_params=pltpu.CompilerParams(collective_id=0, has_side_effects=True),
        name="field",
    )(seam, order, x, w_in, w_mid, w_feat, w_dens, w_conv, w_color)


def body(samples_in, block_order, seam_link, w_in, w_mid, w_feat, w_density, w_conv, w_color):
    n_block, n_patch = lax.axis_size("block"), lax.axis_size("patch")
    x = samples_in.reshape(2, RAYS // 128, 128, SAMP * ENC)
    return render(
        block_order, seam_link, x, w_in, w_mid, jnp.swapaxes(w_feat, 1, 2), w_density, w_conv, w_color, n_block, n_patch
    )


def solution(mesh):
    return jax.shard_map(
        body,
        mesh=mesh,
        in_specs=(
            P("block", None, "patch", None),
            P("patch", None),
            P("patch"),
            P("block", None, None),
            P("block", None, None, None),
            P("block", None, None),
            P("block", None),
            P(),
            P(),
        ),
        out_specs=P(None, "block", "patch"),
        check_vma=False,
    )
```
